32 devices in a mesh: kv: 8 (over z, x), mlp: 4 (over y, core).
Axes of the slice: x: 2, y: 2, z: 4, core: 2. Of those that a mesh axis runs over, the one named last changes fastest.
Arguments:
- queries: bfloat16 [384, 4096], P('kv', 'mlp')
- root_cache: bfloat16 [8, 4096, 2048], P('kv', None, 'mlp')
- mid_cache: bfloat16 [16, 2048, 2048], P('kv', None, 'mlp')
- leaf_cache: bfloat16 [32, 1024, 2048], P('kv', None, 'mlp')
- token_leaf: int32 [384], replicated, may hold values from 0 to 31, as said below
- leaf_parent: int32 [32], replicated, may hold values from 0 to 15, as said below
- mid_parent: int32 [16], replicated, may hold values from 0 to 7, as said below
- root_len: int32 [8], replicated, may hold values from 256 to 4096, as said below
- mid_len: int32 [16], replicated, may hold values from 128 to 2048, as said below
- leaf_len: int32 [32], replicated, may hold values from 64 to 1024, as said below
- root_slot: int32 [8], replicated, may hold values from 0 to 7, each once
- mid_slot: int32 [16], replicated, may hold values from 0 to 15, each once
- leaf_slot: int32 [32], replicated, may hold values from 0 to 31, each once
- stream: bfloat16 [384, 4096], P('kv', 'mlp')
- out_weight: bfloat16 [4096, 4096], P('mlp'), may hold values from -0.09375 to 0.09375
- norm_gain: float32 [4096], P('mlp'), may hold values from 0.1 to 1.9
- gate_weight: bfloat16 [4096, 14336], P('mlp', 'kv'), may hold values from -0.09375 to 0.09375
- up_weight: bfloat16 [4096, 14336], P('mlp', 'kv'), may hold values from -0.09375 to 0.09375
- down_weight: bfloat16 [14336, 4096], P('kv', 'mlp'), may hold values from -0.046875 to 0.046875
Outputs:
- attended: bfloat16 [384, 4096], P('kv', 'mlp')
- mixed: bfloat16 [384, 4096], P('kv', 'mlp')
The draws below stay inside these ranges and needn't reach their ends.
Inputs may be any that keep to these rules, and one draw needn't show every extreme that they name: `token_leaf`: never falls; the tokens of one leaf are contiguous, 8 to 16 of them, and some leaf has exactly 16. `leaf_parent`: never falls; every mid node has 1 to 3 leaves; no mid node has more than 48 tokens beneath it, and one has exactly 48. `mid_parent`: never falls; every root has 1 to 3 mid nodes; no root has more than 144 tokens beneath it, and one has exactly 144. `root_len`: some root has exactly 4096. `mid_len`: some mid node has exactly 2048. `leaf_len`: some leaf has exactly 1024.
All inputs are finite; a program needn't handle non-finite values.
Results may differ from the reference program's by a relative error of at most 0.022.
Values may be sent and summed in bfloat16 or wider, within the bound.
No kernel may reach another device: no remote copies, remote signals or barrier semaphores. Data moves between devices by JAX's collectives and lax.ppermute only.
A program may use at most 128 MiB of HBM per device.

```python
import math
import jax
import jax.numpy as jnp
from jax import lax

D = 4096
HEADS = 32
KV_HEADS = 8
HEAD = 128
FF = 14336
QLEAF = 16
QMID = 48
QROOT = 144
LROOT = 4096
LMID = 2048
LLEAF = 1024
ROOTS = 8
MIDS = 16
LEAVES = 32
TOKENS = 384


def expand_sizes(sizes, total):
    ends = jnp.cumsum(sizes)
    return jnp.sum((ends[None, :] <= jnp.arange(total)[:, None]).astype(jnp.int32), axis=1).astype(jnp.int32)


def tree_shape(key):
    base = jax.random.fold_in(key, 11)
    first_key, second_key, third_key, fourth_key, fifth_key = jax.random.split(base, 5)
    half_leaves = LEAVES // 2
    leaf_shift = jax.random.randint(first_key, (half_leaves,), 0, 5)
    leaf_shift = jnp.where(jnp.arange(half_leaves) < 9, 4, leaf_shift)
    leaf_size = jnp.concatenate([12 + leaf_shift, 12 - leaf_shift]).astype(jnp.int32)
    half_mids = MIDS // 2
    mid_shift = jax.random.randint(second_key, (half_mids,), 0, 2)
    mid_shift = jnp.where(jnp.arange(half_mids) < 3, 1, mid_shift)
    mid_fan = jnp.concatenate([2 + mid_shift, 2 - mid_shift]).astype(jnp.int32)
    half_roots = ROOTS // 2
    root_shift = jax.random.randint(third_key, (half_roots,), 0, 2)
    root_shift = jnp.where(jnp.arange(half_roots) < 1, 1, root_shift)
    root_fan = jnp.concatenate([2 + root_shift, 2 - root_shift]).astype(jnp.int32)
    order = jax.random.permutation(fifth_key, ROOTS - 1) + 1
    order = jnp.concatenate([jnp.zeros((1,), jnp.int32), order.astype(jnp.int32)])
    root_fan = root_fan[order].astype(jnp.int32)
    token_leaf = expand_sizes(leaf_size, TOKENS)
    leaf_parent = expand_sizes(mid_fan, LEAVES)
    mid_parent = expand_sizes(root_fan, MIDS)
    rotate = jax.random.randint(fourth_key, (), 0, ROOTS)
    root_tail = jnp.arange(ROOTS) >= ROOTS - rotate
    mid_rotate = jnp.sum(jnp.where(root_tail, root_fan, 0))
    mid_tail = jnp.arange(MIDS) >= MIDS - mid_rotate
    leaf_rotate = jnp.sum(jnp.where(mid_tail, mid_fan, 0))
    leaf_tail = jnp.arange(LEAVES) >= LEAVES - leaf_rotate
    token_rotate = jnp.sum(jnp.where(leaf_tail, leaf_size, 0))
    token_leaf = jnp.roll((token_leaf + leaf_rotate) % LEAVES, token_rotate)
    leaf_parent = jnp.roll((leaf_parent + mid_rotate) % MIDS, leaf_rotate)
    mid_parent = jnp.roll((mid_parent + rotate) % ROOTS, mid_rotate)
    return (token_leaf.astype(jnp.int32), leaf_parent.astype(jnp.int32), mid_parent.astype(jnp.int32))


def draw_token_leaf(key, part):
    return tree_shape(key)[0]


def draw_leaf_parent(key, part):
    return tree_shape(key)[1]


def draw_mid_parent(key, part):
    return tree_shape(key)[2]


def node_lengths(key, count, capacity):
    first_key, second_key, third_key = jax.random.split(key, 3)
    level = jax.random.randint(first_key, (count,), 0, 4)
    top_len = jnp.right_shift(jnp.full((count,), capacity, jnp.int32), level)
    trimmed = jax.random.randint(second_key, (count,), 0, top_len // 2 + 1)
    lengths = top_len - trimmed
    chosen = jax.random.randint(third_key, (), 0, count)
    return jnp.where(jnp.arange(count) == chosen, capacity, lengths).astype(jnp.int32)


def draw_root_len(key, part):
    return node_lengths(jax.random.fold_in(key, 21), ROOTS, LROOT)


def draw_mid_len(key, part):
    return node_lengths(jax.random.fold_in(key, 22), MIDS, LMID)


def draw_leaf_len(key, part):
    return node_lengths(jax.random.fold_in(key, 23), LEAVES, LLEAF)


def draw_queries(key, part):
    base = jax.random.fold_in(key, 31)
    values = 2.0 * jax.random.truncated_normal(base, -4.0, 4.0, (TOKENS, HEADS, HEAD), jnp.float32)
    return values.reshape(TOKENS, HEADS * HEAD).astype(jnp.bfloat16)


def cache_values(key, salt, count, key_span):
    base = jax.random.fold_in(key, salt)
    shape = (count, key_span, KV_HEADS, 2, HEAD)
    values = jax.random.truncated_normal(base, -5.0, 5.0, shape, jnp.float32)
    return values.reshape(count, key_span, KV_HEADS * 2 * HEAD).astype(jnp.bfloat16)


def draw_root_cache(key, part):
    return cache_values(key, 61, ROOTS, LROOT)


def draw_mid_cache(key, part):
    return cache_values(key, 62, MIDS, LMID)


def draw_leaf_cache(key, part):
    return cache_values(key, 63, LEAVES, LLEAF)


def draw_stream(key, part):
    first_key, second_key, third_key = jax.random.split(jax.random.fold_in(key, 51), 3)
    column = jnp.arange(D, dtype=jnp.float32) / D
    column_rough = jax.random.uniform(second_key, (D,), jnp.float32)
    row_scale = 10.0 ** (0.5 - jax.random.uniform(third_key, (TOKENS,), jnp.float32))
    values = jax.random.truncated_normal(first_key, -6.0, 6.0, (TOKENS, D), jnp.float32)
    column_scale = 10.0 ** (0.5 * column + 0.5 * column_rough)
    return (values * row_scale[:, None] * column_scale[None, :]).astype(jnp.bfloat16)


def level_of(own_key, shape, pieces, low, largest):
    gain = 1.0
    for dim, parts in pieces:
        steps = jax.random.uniform(jax.random.fold_in(jax.random.fold_in(own_key, 6), dim), (parts,), jnp.float32, low / len(pieces), largest / len(pieces))
        gain = gain * jnp.repeat(jnp.exp(steps), shape[dim] // parts).reshape((-1,) + (1,) * (len(shape) - 1 - dim))
    return gain


def bell_draw(rng, shape, scale, most, shards=(), kind=jnp.bfloat16):
    drawn = jax.random.normal(rng, shape, jnp.float32) * scale
    if len(shards) > 0:
        drawn = level_of(rng, shape, shards, -0.22, 0.18) * drawn
    return jnp.clip(drawn, min=-most, max=most).astype(kind)


def setup_inputs(seed: int = 0) -> dict:
    key_of = jax.random.split(jax.random.key(seed), 20)
    queries = draw_queries(jax.random.fold_in(key_of[19], 71), 0)
    root_cache = draw_root_cache(jax.random.fold_in(key_of[19], 71), 0)
    mid_cache = draw_mid_cache(jax.random.fold_in(key_of[19], 71), 0)
    leaf_cache = draw_leaf_cache(jax.random.fold_in(key_of[19], 71), 0)
    token_leaf = draw_token_leaf(jax.random.fold_in(key_of[19], 71), 0)
    leaf_parent = draw_leaf_parent(jax.random.fold_in(key_of[19], 71), 0)
    mid_parent = draw_mid_parent(jax.random.fold_in(key_of[19], 71), 0)
    root_len = draw_root_len(jax.random.fold_in(key_of[19], 71), 0)
    mid_len = draw_mid_len(jax.random.fold_in(key_of[19], 71), 0)
    leaf_len = draw_leaf_len(jax.random.fold_in(key_of[19], 71), 0)
    root_slot = jax.random.permutation(key_of[10], ROOTS).astype(jnp.int32)
    mid_slot = jax.random.permutation(key_of[11], MIDS).astype(jnp.int32)
    leaf_slot = jax.random.permutation(key_of[12], LEAVES).astype(jnp.int32)
    stream = draw_stream(jax.random.fold_in(key_of[19], 71), 0)
    out_weight = bell_draw(key_of[14], (HEADS * HEAD, D), (HEADS * HEAD) ** -0.5, 0.09375, ((0, 4),))
    norm_gain = jnp.clip(1.0 + 0.18 * jax.random.normal(key_of[15], (D,), jnp.float32), 0.1, 1.9)
    gate_weight = bell_draw(key_of[16], (D, FF), D ** -0.5, 0.09375, ((0, 4), (1, 8)))
    up_weight = bell_draw(key_of[17], (D, FF), D ** -0.5, 0.09375, ((0, 4), (1, 8)))
    down_weight = bell_draw(key_of[18], (FF, D), FF ** -0.5, 0.046875, ((0, 8), (1, 4)))
    return {"queries": queries, "root_cache": root_cache, "mid_cache": mid_cache, "leaf_cache": leaf_cache, "token_leaf": token_leaf, "leaf_parent": leaf_parent, "mid_parent": mid_parent, "root_len": root_len, "mid_len": mid_len, "leaf_len": leaf_len, "root_slot": root_slot, "mid_slot": mid_slot, "leaf_slot": leaf_slot, "stream": stream, "out_weight": out_weight, "norm_gain": norm_gain, "gate_weight": gate_weight, "up_weight": up_weight, "down_weight": down_weight}


LOWEST = -1e+30
EPSILON = 1e-05

def tree_counts(token_leaf, leaf_parent, mid_parent, root_total):
    leaf_ids = jnp.arange(leaf_parent.shape[0], dtype=jnp.int32)
    leaf_count = lax.optimization_barrier(jnp.sum((token_leaf[None, :] == leaf_ids[:, None]).astype(jnp.int32), axis=1)).astype(jnp.int32)
    mid_ids = jnp.arange(mid_parent.shape[0], dtype=jnp.int32)
    mid_count = lax.optimization_barrier(jnp.sum(jnp.where(leaf_parent[None, :] == mid_ids[:, None], leaf_count[None, :], 0), axis=1)).astype(jnp.int32)
    root_ids = jnp.arange(root_total, dtype=jnp.int32)
    root_count = lax.optimization_barrier(jnp.sum(jnp.where(mid_parent[None, :] == root_ids[:, None], mid_count[None, :], 0), axis=1)).astype(jnp.int32)
    counts = (root_count, mid_count, leaf_count)
    starts = tuple(((jnp.cumsum(level_count) - level_count).astype(jnp.int32) for level_count in counts))
    return (starts, counts)

def node_attention(query_rows, key_values, length):
    row_count = query_rows.shape[0]
    key_span = key_values.shape[0]
    group_size = HEADS // KV_HEADS
    grouped = query_rows.astype(jnp.float32).reshape(row_count, KV_HEADS, group_size, HEAD)
    paired = key_values.reshape(key_span, KV_HEADS, 2, HEAD).astype(jnp.float32)
    scores = jnp.einsum('rkgd,jkd->rkgj', grouped, paired[:, :, 0, :]) * (1.0 / math.sqrt(HEAD))
    live_keys = jnp.arange(key_span, dtype=jnp.int32) < length
    scores = jnp.where(live_keys, scores, LOWEST)
    peak_score = lax.optimization_barrier(jnp.max(scores, axis=-1))
    weights = jnp.where(live_keys, jnp.exp(scores - peak_score[..., None]), 0.0)
    weight_sum = lax.optimization_barrier(jnp.sum(weights, axis=-1))
    rounded = lax.optimization_barrier(weights.astype(jnp.bfloat16)).astype(jnp.float32)
    partial_out = jnp.einsum('rkgj,jkd->rkgd', rounded, paired[:, :, 1, :])
    return (peak_score.reshape(row_count, HEADS), weight_sum.reshape(row_count, HEADS), partial_out.reshape(row_count, HEADS, HEAD))

def merge_into(running, part, first_row, row_count, capacity):
    run_peak, run_sum, run_out = running
    part_peak, part_sum, part_out = part
    window = jnp.minimum(first_row, run_peak.shape[0] - capacity).astype(jnp.int32)
    positions = window + jnp.arange(capacity, dtype=jnp.int32)
    live_rows = ((positions >= first_row) & (positions < first_row + row_count))[:, None]
    old_peak = lax.dynamic_slice_in_dim(run_peak, window, capacity, 0)
    old_sum = lax.dynamic_slice_in_dim(run_sum, window, capacity, 0)
    old_out = lax.dynamic_slice_in_dim(run_out, window, capacity, 0)
    new_peak = jnp.where(live_rows, jnp.maximum(old_peak, part_peak), old_peak)
    carry_factor = jnp.exp(old_peak - new_peak)
    take_factor = jnp.where(live_rows, jnp.exp(part_peak - new_peak), 0.0)
    new_sum = old_sum * carry_factor + part_sum * take_factor
    new_out = old_out * carry_factor[..., None] + part_out * take_factor[..., None]
    return (lax.dynamic_update_slice_in_dim(run_peak, new_peak, window, 0), lax.dynamic_update_slice_in_dim(run_sum, new_sum, window, 0), lax.dynamic_update_slice_in_dim(run_out, new_out, window, 0))

def level_pass(running, queries, cache, slot_map, lengths, starts, counts, capacity):

    def step_node(carry, node_index):
        first_row = starts[node_index]
        window = jnp.minimum(first_row, TOKENS - capacity).astype(jnp.int32)
        query_rows = lax.dynamic_slice_in_dim(queries, window, capacity, 0)
        key_values = lax.dynamic_index_in_dim(cache, slot_map[node_index], 0, keepdims=False)
        part = node_attention(query_rows, key_values, lengths[node_index])
        return (merge_into(carry, part, first_row, counts[node_index], capacity), None)
    return lax.scan(step_node, running, jnp.arange(slot_map.shape[0], dtype=jnp.int32))[0]

def reference(queries, root_cache, mid_cache, leaf_cache, token_leaf, leaf_parent, mid_parent, root_len, mid_len, leaf_len, root_slot, mid_slot, leaf_slot, stream, out_weight, norm_gain, gate_weight, up_weight, down_weight):
    starts, counts = tree_counts(token_leaf, leaf_parent, mid_parent, ROOTS)
    running = (jnp.full((TOKENS, HEADS), LOWEST, jnp.float32), jnp.zeros((TOKENS, HEADS), jnp.float32), jnp.zeros((TOKENS, HEADS, HEAD), jnp.float32))
    running = level_pass(running, queries, root_cache, root_slot, root_len, starts[0], counts[0], QROOT)
    running = level_pass(running, queries, mid_cache, mid_slot, mid_len, starts[1], counts[1], QMID)
    running = level_pass(running, queries, leaf_cache, leaf_slot, leaf_len, starts[2], counts[2], QLEAF)
    attended = (running[2] / running[1][..., None]).reshape(TOKENS, HEADS * HEAD).astype(jnp.bfloat16)
    projected = jnp.dot(attended, out_weight, preferred_element_type=jnp.float32)
    residual = (stream.astype(jnp.float32) + projected).astype(jnp.bfloat16)
    widened = lax.optimization_barrier(residual).astype(jnp.float32)
    mean_square = lax.optimization_barrier(jnp.mean(widened * widened, axis=1, keepdims=True))
    normed = (widened * lax.rsqrt(mean_square + EPSILON) * norm_gain).astype(jnp.bfloat16)
    gate = jnp.dot(normed, gate_weight, preferred_element_type=jnp.float32)
    upward = jnp.dot(normed, up_weight, preferred_element_type=jnp.float32)
    hidden = (jax.nn.silu(gate) * upward).astype(jnp.bfloat16)
    mixed = jnp.dot(hidden, down_weight, preferred_element_type=jnp.float32).astype(jnp.bfloat16)
    return (attended, mixed)
```

```python
import math

import jax
import jax.numpy as jnp
from jax import lax
from jax.sharding import PartitionSpec as P

D = 4096
HEAD = 128
QLEAF = 16
QMID = 48
QROOT = 144


LOWEST = -1e30
EPSILON = 1e-05


def tree_counts(token_leaf, leaf_parent, mid_parent, root_total):
    leaf_ids = jnp.arange(leaf_parent.shape[0], dtype=jnp.int32)
    leaf_count = jnp.sum((token_leaf[None, :] == leaf_ids[:, None]).astype(jnp.int32), axis=1)
    mid_ids = jnp.arange(mid_parent.shape[0], dtype=jnp.int32)
    mid_count = jnp.sum(
        jnp.where(leaf_parent[None, :] == mid_ids[:, None], leaf_count[None, :], 0), axis=1
    )
    root_ids = jnp.arange(root_total, dtype=jnp.int32)
    root_count = jnp.sum(
        jnp.where(mid_parent[None, :] == root_ids[:, None], mid_count[None, :], 0), axis=1
    )
    counts = (root_count, mid_count, leaf_count)
    return (tuple(before(level_count) for level_count in counts), counts)


def before(level_count):
    ids = jnp.arange(level_count.shape[0], dtype=jnp.int32)
    return jnp.sum(jnp.where(ids[None, :] < ids[:, None], level_count[None, :], 0), axis=1)


def slot_nodes(slot_map, wanted):
    node_ids = jnp.arange(slot_map.shape[0], dtype=jnp.int32)
    matches = slot_map[None, :] == wanted[:, None]
    return jnp.sum(jnp.where(matches, node_ids[None, :], 0), axis=1)


def lookup(values, wanted):
    table_ids = jnp.arange(values.shape[0], dtype=jnp.int32)
    matches = table_ids[None, :] == wanted[:, None]
    return jnp.sum(jnp.where(matches, values[None, :], 0), axis=1)


def attend(query_rows, cache, lengths):
    slot_total, row_count, row_width = query_rows.shape
    key_span = cache.shape[1]
    kv_count = cache.shape[2] // (2 * HEAD)
    group_size = row_width // (kv_count * HEAD)
    grouped = query_rows.reshape(slot_total, row_count, kv_count, group_size, HEAD)
    paired = cache.reshape(slot_total, key_span, kv_count, 2, HEAD)
    block_len = min(512, key_span)
    block_total = (jnp.max(lengths) + block_len - 1) // block_len
    score_scale = 1.0 / math.sqrt(HEAD)

    def visit_block(block_index, carry):
        peak_score, weight_sum, partial_out = carry
        key_piece = lax.dynamic_slice_in_dim(paired, block_index * block_len, block_len, 1)
        scores = (
            jnp.einsum(
                "srkgd,sjkd->srkgj",
                grouped,
                key_piece[:, :, :, 0, :],
                preferred_element_type=jnp.float32,
            )
            * score_scale
        )
        position = block_index * block_len + jnp.arange(block_len, dtype=jnp.int32)
        live_keys = (position[None, :] < lengths[:, None])[:, None, None, None, :]
        scores = jnp.where(live_keys, scores, LOWEST)
        new_peak = jnp.maximum(peak_score, jnp.max(scores, axis=-1))
        weights = jnp.where(live_keys, jnp.exp(scores - new_peak[..., None]), 0.0)
        carry_factor = jnp.exp(peak_score - new_peak)
        weight_sum = weight_sum * carry_factor + jnp.sum(weights, axis=-1)
        partial_out = partial_out * carry_factor[..., None] + jnp.einsum(
            "srkgj,sjkd->srkgd",
            weights.astype(jnp.bfloat16),
            key_piece[:, :, :, 1, :],
            preferred_element_type=jnp.float32,
        )
        return (new_peak, weight_sum, partial_out)

    initial = (
        jnp.full((slot_total, row_count, kv_count, group_size), LOWEST, jnp.float32),
        jnp.zeros((slot_total, row_count, kv_count, group_size), jnp.float32),
        jnp.zeros((slot_total, row_count, kv_count, group_size, HEAD), jnp.float32),
    )
    peak_score, weight_sum, partial_out = lax.fori_loop(0, block_total, visit_block, initial)
    head_count = kv_count * group_size
    return (
        peak_score.reshape(slot_total, row_count, head_count),
        weight_sum.reshape(slot_total, row_count, head_count),
        partial_out.reshape(slot_total, row_count, head_count, HEAD),
    )


def merge_into(running, part, first_row, row_count, capacity):
    run_peak, run_sum, run_out = running
    part_peak, part_sum, part_out = part
    window = jnp.minimum(first_row, run_peak.shape[0] - capacity)
    positions = window + jnp.arange(capacity, dtype=jnp.int32)
    live_rows = ((positions >= first_row) & (positions < first_row + row_count))[:, None]
    old_peak = lax.dynamic_slice_in_dim(run_peak, window, capacity, 0)
    old_sum = lax.dynamic_slice_in_dim(run_sum, window, capacity, 0)
    old_out = lax.dynamic_slice_in_dim(run_out, window, capacity, 0)
    new_peak = jnp.where(live_rows, jnp.maximum(old_peak, part_peak), old_peak)
    carry_factor = jnp.exp(old_peak - new_peak)
    take_factor = jnp.where(live_rows, jnp.exp(part_peak - new_peak), 0.0)
    new_sum = old_sum * carry_factor + part_sum * take_factor
    new_out = old_out * carry_factor[..., None] + part_out * take_factor[..., None]
    return (
        lax.dynamic_update_slice_in_dim(run_peak, new_peak, window, 0),
        lax.dynamic_update_slice_in_dim(run_sum, new_sum, window, 0),
        lax.dynamic_update_slice_in_dim(run_out, new_out, window, 0),
    )


def run_slots(running, everyone, cache_stack, lengths, node_starts, node_counts, capacity):
    slot_total = cache_stack.shape[0]
    windows = jnp.minimum(node_starts, everyone.shape[0] - capacity)
    query_rows = jnp.stack(
        [
            lax.dynamic_slice_in_dim(everyone, windows[member], capacity, 0)
            for member in range(slot_total)
        ]
    )
    part_peak, part_sum, part_out = attend(query_rows, cache_stack, lengths)
    for member in range(slot_total):
        running = merge_into(
            running,
            (part_peak[member], part_sum[member], part_out[member]),
            node_starts[member],
            node_counts[member],
            capacity,
        )
    return running


def shards(
    queries,
    root_cache,
    mid_cache,
    leaf_cache,
    token_leaf,
    leaf_parent,
    mid_parent,
    root_len,
    mid_len,
    leaf_len,
    root_slot,
    mid_slot,
    leaf_slot,
    stream,
    out_weight,
    norm_gain,
    gate_weight,
    up_weight,
    down_weight,
):
    own_rows = queries.shape[0]
    owner_index = lax.axis_index("kv")
    everyone = lax.all_gather(queries, "kv", axis=0, tiled=True)
    total_rows = everyone.shape[0]
    head_count = queries.shape[1] // HEAD
    starts, counts = tree_counts(token_leaf, leaf_parent, mid_parent, root_len.shape[0])
    running = (
        jnp.full((total_rows, head_count), LOWEST, jnp.float32),
        jnp.zeros((total_rows, head_count), jnp.float32),
        jnp.zeros((total_rows, head_count, HEAD), jnp.float32),
    )
    node_ids = slot_nodes(root_slot, owner_index[None])
    running = run_slots(
        running,
        everyone,
        root_cache,
        lookup(root_len, node_ids),
        lookup(starts[0], node_ids),
        lookup(counts[0], node_ids),
        QROOT,
    )
    mid_local = mid_cache.shape[0]
    mid_wanted = owner_index * mid_local + jnp.arange(mid_local, dtype=jnp.int32)
    mid_nodes = slot_nodes(mid_slot, mid_wanted)
    running = run_slots(
        running,
        everyone,
        mid_cache,
        lookup(mid_len, mid_nodes),
        lookup(starts[1], mid_nodes),
        lookup(counts[1], mid_nodes),
        QMID,
    )
    leaf_local = leaf_cache.shape[0]
    leaf_wanted = owner_index * leaf_local + jnp.arange(leaf_local, dtype=jnp.int32)
    leaf_nodes = slot_nodes(leaf_slot, leaf_wanted)
    running = run_slots(
        running,
        everyone,
        leaf_cache,
        lookup(leaf_len, leaf_nodes),
        lookup(starts[2], leaf_nodes),
        lookup(counts[2], leaf_nodes),
        QLEAF,
    )
    best_score = lax.pmax(running[0], "kv")
    factor = jnp.exp(running[0] - best_score)
    out_sum, weight_total = (
        lax.psum_scatter(
            (running[2] * factor[..., None]).astype(jnp.bfloat16),
            "kv",
            scatter_dimension=0,
            tiled=True,
        ).astype(jnp.float32),
        lax.psum_scatter(
            (running[1] * factor).astype(jnp.bfloat16), "kv", scatter_dimension=0, tiled=True
        ).astype(jnp.float32),
    )
    attended = (
        (out_sum / weight_total[..., None])
        .reshape(own_rows, head_count * HEAD)
        .astype(jnp.bfloat16)
    )
    projected = lax.psum_scatter(
        lax.dot_general(
            out_weight, attended, (((0,), (1,)), ((), ())), preferred_element_type=jnp.float32
        ).astype(jnp.bfloat16),
        "mlp",
        scatter_dimension=0,
        tiled=True,
    ).astype(jnp.float32)
    residual = (stream.astype(jnp.float32) + projected.T).astype(jnp.bfloat16)
    widened = lax.optimization_barrier(residual).astype(jnp.float32)
    square_sum = lax.psum(jnp.sum(widened * widened, axis=1), "mlp")
    normed = (widened * lax.rsqrt(square_sum / D + EPSILON)[:, None] * norm_gain).astype(
        jnp.bfloat16
    )
    gate_up = jnp.concatenate([gate_weight, up_weight], axis=1)
    unit_count = gate_weight.shape[1]
    gate_up_sum = jnp.dot(
        lax.all_gather(normed, "kv", axis=0, tiled=True),
        gate_up,
        preferred_element_type=jnp.float32,
    )
    share_rows = lax.psum_scatter(
        gate_up_sum.astype(jnp.bfloat16), "mlp", scatter_dimension=0, tiled=True
    ).astype(jnp.float32)
    hidden_share = (jax.nn.silu(share_rows[:, :unit_count]) * share_rows[:, unit_count:]).astype(
        jnp.bfloat16
    )
    hidden = lax.all_gather(hidden_share, "mlp", axis=0, tiled=True)
    mixed = lax.psum_scatter(
        jnp.dot(hidden, down_weight, preferred_element_type=jnp.float32).astype(jnp.bfloat16),
        "kv",
        scatter_dimension=0,
        tiled=True,
    )
    return (attended, mixed)


def solution(mesh):
    in_specs = (
        P("kv", "mlp"),
        P("kv", None, "mlp"),
        P("kv", None, "mlp"),
        P("kv", None, "mlp"),
        P(),
        P(),
        P(),
        P(),
        P(),
        P(),
        P(),
        P(),
        P(),
        P("kv", "mlp"),
        P("mlp", None),
        P("mlp"),
        P("mlp", "kv"),
        P("mlp", "kv"),
        P("kv", "mlp"),
    )
    out_specs = (P("kv", "mlp"), P("kv", "mlp"))
    return jax.shard_map(shards, mesh=mesh, in_specs=in_specs, out_specs=out_specs, check_vma=False)
```

```python
import math

import jax
import jax.numpy as jnp
from jax import lax
from jax.sharding import PartitionSpec as P

D = 4096
HEAD = 128
QLEAF = 16
QMID = 48
QROOT = 144


LOWEST = -1e30
EPSILON = 1e-05


def tree_counts(token_leaf, leaf_parent, mid_parent, root_total):
    leaf_ids = jnp.arange(leaf_parent.shape[0], dtype=jnp.int32)
    leaf_count = jnp.sum((token_leaf[None, :] == leaf_ids[:, None]).astype(jnp.int32), axis=1)
    mid_ids = jnp.arange(mid_parent.shape[0], dtype=jnp.int32)
    mid_count = jnp.sum(
        jnp.where(leaf_parent[None, :] == mid_ids[:, None], leaf_count[None, :], 0), axis=1
    )
    root_ids = jnp.arange(root_total, dtype=jnp.int32)
    root_count = jnp.sum(
        jnp.where(mid_parent[None, :] == root_ids[:, None], mid_count[None, :], 0), axis=1
    )
    counts = (root_count, mid_count, leaf_count)
    return (tuple(before(level_count) for level_count in counts), counts)


def before(level_count):
    ids = jnp.arange(level_count.shape[0], dtype=jnp.int32)
    return jnp.sum(jnp.where(ids[None, :] < ids[:, None], level_count[None, :], 0), axis=1)


def slot_nodes(slot_map, wanted):
    node_ids = jnp.arange(slot_map.shape[0], dtype=jnp.int32)
    matches = slot_map[None, :] == wanted[:, None]
    return jnp.sum(jnp.where(matches, node_ids[None, :], 0), axis=1)


def lookup(values, wanted):
    table_ids = jnp.arange(values.shape[0], dtype=jnp.int32)
    matches = table_ids[None, :] == wanted[:, None]
    return jnp.sum(jnp.where(matches, values[None, :], 0), axis=1)


def attend(query_rows, cache, lengths):
    slot_total, row_count, row_width = query_rows.shape
    key_span = cache.shape[1]
    kv_count = cache.shape[2] // (2 * HEAD)
    group_size = row_width // (kv_count * HEAD)
    grouped = query_rows.reshape(slot_total, row_count, kv_count, group_size, HEAD)
    paired = cache.reshape(slot_total, key_span, kv_count, 2, HEAD)
    block_len = min(512, key_span)
    block_total = (jnp.max(lengths) + block_len - 1) // block_len
    score_scale = 1.0 / math.sqrt(HEAD)

    def visit_block(block_index, carry):
        peak_score, weight_sum, partial_out = carry
        key_piece = lax.dynamic_slice_in_dim(paired, block_index * block_len, block_len, 1)
        scores = (
            jnp.einsum(
                "srkgd,sjkd->srkgj",
                grouped,
                key_piece[:, :, :, 0, :],
                preferred_element_type=jnp.float32,
            )
            * score_scale
        )
        position = block_index * block_len + jnp.arange(block_len, dtype=jnp.int32)
        live_keys = (position[None, :] < lengths[:, None])[:, None, None, None, :]
        scores = jnp.where(live_keys, scores, LOWEST)
        new_peak = jnp.maximum(peak_score, jnp.max(scores, axis=-1))
        weights = jnp.where(live_keys, jnp.exp(scores - new_peak[..., None]), 0.0)
        carry_factor = jnp.exp(peak_score - new_peak)
        weight_sum = weight_sum * carry_factor + jnp.sum(weights, axis=-1)
        partial_out = partial_out * carry_factor[..., None] + jnp.einsum(
            "srkgj,sjkd->srkgd",
            weights.astype(jnp.bfloat16),
            key_piece[:, :, :, 1, :],
            preferred_element_type=jnp.float32,
        )
        return (new_peak, weight_sum, partial_out)

    initial = (
        jnp.full((slot_total, row_count, kv_count, group_size), LOWEST, jnp.float32),
        jnp.zeros((slot_total, row_count, kv_count, group_size), jnp.float32),
        jnp.zeros((slot_total, row_count, kv_count, group_size, HEAD), jnp.float32),
    )
    peak_score, weight_sum, partial_out = lax.fori_loop(0, block_total, visit_block, initial)
    head_count = kv_count * group_size
    return (
        peak_score.reshape(slot_total, row_count, head_count),
        weight_sum.reshape(slot_total, row_count, head_count),
        partial_out.reshape(slot_total, row_count, head_count, HEAD),
    )


def merge_into(running, part, first_row, row_count, capacity):
    run_peak, run_sum, run_out = running
    part_peak, part_sum, part_out = part
    window = jnp.minimum(first_row, run_peak.shape[0] - capacity)
    positions = window + jnp.arange(capacity, dtype=jnp.int32)
    live_rows = ((positions >= first_row) & (positions < first_row + row_count))[:, None]
    old_peak = lax.dynamic_slice_in_dim(run_peak, window, capacity, 0)
    old_sum = lax.dynamic_slice_in_dim(run_sum, window, capacity, 0)
    old_out = lax.dynamic_slice_in_dim(run_out, window, capacity, 0)
    new_peak = jnp.where(live_rows, jnp.maximum(old_peak, part_peak), old_peak)
    carry_factor = jnp.exp(old_peak - new_peak)
    take_factor = jnp.where(live_rows, jnp.exp(part_peak - new_peak), 0.0)
    new_sum = old_sum * carry_factor + part_sum * take_factor
    new_out = old_out * carry_factor[..., None] + part_out * take_factor[..., None]
    return (
        lax.dynamic_update_slice_in_dim(run_peak, new_peak, window, 0),
        lax.dynamic_update_slice_in_dim(run_sum, new_sum, window, 0),
        lax.dynamic_update_slice_in_dim(run_out, new_out, window, 0),
    )


def run_slots(running, everyone, cache_stack, lengths, node_starts, node_counts, capacity):
    slot_total = cache_stack.shape[0]
    windows = jnp.minimum(node_starts, everyone.shape[0] - capacity)
    query_rows = jnp.stack(
        [
            lax.dynamic_slice_in_dim(everyone, windows[member], capacity, 0)
            for member in range(slot_total)
        ]
    )
    part_peak, part_sum, part_out = attend(query_rows, cache_stack, lengths)
    for member in range(slot_total):
        running = merge_into(
            running,
            (part_peak[member], part_sum[member], part_out[member]),
            node_starts[member],
            node_counts[member],
            capacity,
        )
    return running


def shards(
    queries,
    root_cache,
    mid_cache,
    leaf_cache,
    token_leaf,
    leaf_parent,
    mid_parent,
    root_len,
    mid_len,
    leaf_len,
    root_slot,
    mid_slot,
    leaf_slot,
    stream,
    out_weight,
    norm_gain,
    gate_weight,
    up_weight,
    down_weight,
):
    own_rows = queries.shape[0]
    owner_index = lax.axis_index("kv")
    everyone = lax.all_gather(queries, "kv", axis=0, tiled=True)
    total_rows = everyone.shape[0]
    head_count = queries.shape[1] // HEAD
    starts, counts = tree_counts(token_leaf, leaf_parent, mid_parent, root_len.shape[0])
    running = (
        jnp.full((total_rows, head_count), LOWEST, jnp.float32),
        jnp.zeros((total_rows, head_count), jnp.float32),
        jnp.zeros((total_rows, head_count, HEAD), jnp.float32),
    )
    node_ids = slot_nodes(root_slot, owner_index[None])
    running = run_slots(
        running,
        everyone,
        root_cache,
        lookup(root_len, node_ids),
        lookup(starts[0], node_ids),
        lookup(counts[0], node_ids),
        QROOT,
    )
    mid_local = mid_cache.shape[0]
    mid_wanted = owner_index * mid_local + jnp.arange(mid_local, dtype=jnp.int32)
    mid_nodes = slot_nodes(mid_slot, mid_wanted)
    running = run_slots(
        running,
        everyone,
        mid_cache,
        lookup(mid_len, mid_nodes),
        lookup(starts[1], mid_nodes),
        lookup(counts[1], mid_nodes),
        QMID,
    )
    leaf_local = leaf_cache.shape[0]
    leaf_wanted = owner_index * leaf_local + jnp.arange(leaf_local, dtype=jnp.int32)
    leaf_nodes = slot_nodes(leaf_slot, leaf_wanted)
    running = run_slots(
        running,
        everyone,
        leaf_cache,
        lookup(leaf_len, leaf_nodes),
        lookup(starts[2], leaf_nodes),
        lookup(counts[2], leaf_nodes),
        QLEAF,
    )
    kv_total = total_rows // own_rows
    filled = running[1] > 0.0
    safe_sum = jnp.where(filled, running[1], 1.0)
    part_out = (running[2] / safe_sum[..., None]).astype(jnp.bfloat16)
    part_lse = jnp.where(filled, running[0] + jnp.log(safe_sum), LOWEST)
    every_out = lax.all_to_all(
        part_out.reshape(kv_total, own_rows, head_count * HEAD), "kv", 0, 0
    ).reshape(kv_total, own_rows, head_count, HEAD)
    every_lse = lax.all_to_all(part_lse.reshape(kv_total, own_rows, head_count), "kv", 0, 0)
    share = jnp.exp(every_lse - jnp.max(every_lse, axis=0))
    attended = (
        (
            jnp.sum(every_out.astype(jnp.float32) * share[..., None], axis=0)
            / jnp.sum(share, axis=0)[..., None]
        )
        .reshape(own_rows, head_count * HEAD)
        .astype(jnp.bfloat16)
    )
    mlp_total = lax.axis_size("mlp")
    own_width = stream.shape[1]
    projected = lax.dot_general(
        attended, out_weight, (((1,), (0,)), ((), ())), preferred_element_type=jnp.float32
    ).astype(jnp.bfloat16)
    projected = projected.reshape(own_rows, mlp_total, own_width).transpose(1, 0, 2)
    projected = jnp.sum(lax.all_to_all(projected, "mlp", 0, 0).astype(jnp.float32), axis=0)
    residual = (stream.astype(jnp.float32) + projected).astype(jnp.bfloat16)
    widened = lax.optimization_barrier(residual).astype(jnp.float32)
    square_sum = lax.psum(jnp.sum(widened * widened, axis=1), "mlp")
    row_scale = lax.all_gather(lax.rsqrt(square_sum / D + EPSILON), "kv", axis=0, tiled=True)
    scaled = lax.all_gather((widened * norm_gain).astype(jnp.bfloat16), "kv", axis=0, tiled=True)
    gate_up = jnp.concatenate([gate_weight, up_weight], axis=1)
    unit_count = gate_weight.shape[1]
    gate_up_sum = jnp.dot(scaled, gate_up, preferred_element_type=jnp.float32)
    share_rows = halve(
        (gate_up_sum * row_scale[:, None]).astype(jnp.bfloat16), "mlp", mlp_total
    )
    share_rows = share_rows.astype(jnp.float32)
    hidden = (jax.nn.silu(share_rows[:, :unit_count]) * share_rows[:, unit_count:]).astype(
        jnp.bfloat16
    )
    hidden = double(hidden, "mlp", mlp_total)
    partial_mixed = jnp.dot(hidden, down_weight, preferred_element_type=jnp.float32)
    partial_mixed = partial_mixed.astype(jnp.bfloat16).reshape(kv_total, own_rows, own_width)
    mixed = jnp.sum(lax.all_to_all(partial_mixed, "kv", 0, 0).astype(jnp.float32), axis=0)
    return (attended, mixed.astype(jnp.bfloat16))


def halve(rows, axis_name, axis_total):
    place = lax.axis_index(axis_name)
    step = 1
    while step < axis_total:
        half = rows.shape[0] // 2
        side = (place // step) % 2
        keep = lax.dynamic_slice_in_dim(rows, side * half, half, 0)
        send = lax.dynamic_slice_in_dim(rows, (1 - side) * half, half, 0)
        got = lax.ppermute(send, axis_name, [(j, j ^ step) for j in range(axis_total)])
        rows = (keep.astype(jnp.float32) + got.astype(jnp.float32)).astype(jnp.bfloat16)
        step *= 2
    return rows


def double(rows, axis_name, axis_total):
    place = lax.axis_index(axis_name)
    step = axis_total // 2
    while step > 0:
        got = lax.ppermute(rows, axis_name, [(j, j ^ step) for j in range(axis_total)])
        low = (place // step) % 2 == 0
        rows = jnp.where(
            low, jnp.concatenate([rows, got], axis=0), jnp.concatenate([got, rows], axis=0)
        )
        step //= 2
    return rows


def solution(mesh):
    in_specs = (
        P("kv", "mlp"),
        P("kv", None, "mlp"),
        P("kv", None, "mlp"),
        P("kv", None, "mlp"),
        P(),
        P(),
        P(),
        P(),
        P(),
        P(),
        P(),
        P(),
        P(),
        P("kv", "mlp"),
        P("mlp", None),
        P("mlp"),
        P("mlp", "kv"),
        P("mlp", "kv"),
        P("kv", "mlp"),
    )
    out_specs = (P("kv", "mlp"), P("kv", "mlp"))
    return jax.shard_map(shards, mesh=mesh, in_specs=in_specs, out_specs=out_specs, check_vma=False)
```

```python
import math

import jax
import jax.numpy as jnp
from jax import lax
from jax.experimental import pallas as pl
from jax.experimental.pallas import tpu as pltpu
from jax.sharding import PartitionSpec as P

D = 4096
HEAD = 128
QLEAF = 16
QMID = 48
QROOT = 144


LOWEST = -1e30
EPSILON = 1e-05
ALIGN = 16
BLOCK = 512


def count_below(sorted_values, bounds):
    return jnp.sum((sorted_values[None, :] < bounds[:, None]).astype(jnp.int32), axis=1)


def slot_nodes(slot_map, lengths, wanted):
    node_ids = jnp.arange(slot_map.shape[0], dtype=jnp.int32)
    matches = slot_map[None, :] == wanted[:, None]
    nodes = jnp.sum(jnp.where(matches, node_ids[None, :], 0), axis=1)
    return nodes, jnp.sum(jnp.where(matches, lengths[None, :], 0), axis=1)


def own_nodes(owner, local_counts, tree, lengths, slots):
    token_leaf, leaf_parent, mid_parent = tree
    picked = [
        slot_nodes(slot_map, level_len, owner * local + jnp.arange(local, dtype=jnp.int32))
        for slot_map, level_len, local in zip(slots, lengths, local_counts)
    ]
    edges = jnp.concatenate([picked[0][0], picked[0][0] + 1])
    edges = jnp.concatenate([count_below(mid_parent, edges), picked[1][0], picked[1][0] + 1])
    edges = jnp.concatenate([count_below(leaf_parent, edges), picked[2][0], picked[2][0] + 1])
    edges = count_below(token_leaf, edges)
    first, last, place = [], [], 0
    for local in local_counts:
        first.append(edges[place : place + local])
        last.append(edges[place + local : place + 2 * local])
        place += 2 * local
    return jnp.stack(
        [
            jnp.concatenate(first),
            jnp.concatenate(last),
            jnp.concatenate([level_len for _, level_len in picked]),
        ]
    ).astype(jnp.int32)


def tree_attention(query_parts, caches, nodes, owner):
    part_total = len(query_parts)
    own_rows, width = query_parts[0].shape
    total_rows = part_total * own_rows
    kv_count = caches[0].shape[2] // (2 * HEAD)
    head_count = width // HEAD
    group_size = head_count // kv_count
    score_scale = 1.0 / math.sqrt(HEAD)
    levels = []
    for cache, capacity in zip(caches, (QROOT, QMID, QLEAF)):
        levels.append((cache.shape[0], cache.shape[1], min(capacity + ALIGN, total_rows)))

    def kernel(nodes_ref, owner_ref, *refs):
        query_refs = refs[:part_total]
        cache_refs = refs[part_total : part_total + 3]
        out_ref, all_rows, run_out, run_lse, acc, peak, total = refs[part_total + 3 :]
        me = owner_ref[0]
        for part in range(part_total):
            row = pl.multiple_of((me ^ part) * own_rows, ALIGN)
            all_rows[pl.ds(row, own_rows), :] = query_refs[part][...]
        run_out[...] = jnp.zeros_like(run_out)
        run_lse[...] = jnp.full_like(run_lse, LOWEST)
        node = 0
        for (slot_total, span, rows), cache_ref in zip(levels, cache_refs):
            lanes = rows * group_size
            block = min(BLOCK, span)
            for member in range(slot_total):
                low, high, length = nodes_ref[0, node], nodes_ref[1, node], nodes_ref[2, node]
                node += 1
                window = jnp.minimum(low - lax.rem(low, ALIGN), total_rows - rows)
                window = pl.multiple_of(window, ALIGN)
                for kv_head in range(kv_count):
                    columns = [
                        (kv_head * group_size + h) * HEAD for h in range(group_size)
                    ]
                    grouped = jnp.concatenate(
                        [all_rows[pl.ds(window, rows), c : c + HEAD] for c in columns], axis=0
                    )
                    acc[:, :lanes] = jnp.zeros((HEAD, lanes), jnp.float32)
                    peak[:, :lanes] = jnp.full((1, lanes), LOWEST, jnp.float32)
                    total[:, :lanes] = jnp.zeros((1, lanes), jnp.float32)

                    def visit(index, carry, masked):
                        at = pl.multiple_of(index * block, block)
                        keys = cache_ref[
                            member, pl.ds(at, block), 2 * kv_head * HEAD : (2 * kv_head + 1) * HEAD
                        ]
                        values = cache_ref[
                            member,
                            pl.ds(at, block),
                            (2 * kv_head + 1) * HEAD : (2 * kv_head + 2) * HEAD,
                        ]
                        scores = lax.dot_general(
                            keys,
                            grouped,
                            (((1,), (1,)), ((), ())),
                            preferred_element_type=jnp.float32,
                        )
                        if masked:
                            position = at + lax.broadcasted_iota(jnp.int32, (block, lanes), 0)
                            scores = jnp.where(position < length, scores, LOWEST)
                        old_peak = peak[:, :lanes]
                        new_peak = jnp.maximum(old_peak, jnp.max(scores, axis=0, keepdims=True))
                        weights = jnp.exp((scores - new_peak) * score_scale)
                        fade = jnp.exp((old_peak - new_peak) * score_scale)
                        peak[:, :lanes] = new_peak
                        total[:, :lanes] = total[:, :lanes] * fade + jnp.sum(
                            weights, axis=0, keepdims=True
                        )
                        acc[:, :lanes] = acc[:, :lanes] * fade + lax.dot_general(
                            values,
                            weights.astype(jnp.bfloat16),
                            (((0,), (0,)), ((), ())),
                            preferred_element_type=jnp.float32,
                        )
                        return carry

                    whole = lax.div(length, block)
                    lax.fori_loop(0, whole, lambda i, c: visit(i, c, False), 0)

                    @pl.when(whole * block < length)
                    def _():
                        visit(whole, 0, True)

                    weight_sum = total[:, :lanes]
                    part_out = (acc[:, :lanes] / weight_sum).T
                    part_lse = jnp.broadcast_to(
                        peak[:, :lanes] * score_scale + jnp.log(weight_sum), (HEAD, lanes)
                    ).T
                    position = window + lax.broadcasted_iota(jnp.int32, (rows, HEAD), 0)
                    live = (position >= low) & (position < high)
                    for h, c in enumerate(columns):
                        here = (pl.ds(window, rows), slice(c, c + HEAD))
                        old_lse, old_out = run_lse[here], run_out[here]
                        add_lse = part_lse[h * rows : (h + 1) * rows]
                        add_out = part_out[h * rows : (h + 1) * rows]
                        best = jnp.maximum(old_lse, add_lse)
                        old_share = jnp.exp(old_lse - best)
                        add_share = jnp.exp(add_lse - best)
                        share = old_share + add_share
                        run_out[here] = jnp.where(
                            live, (old_out * old_share + add_out * add_share) / share, old_out
                        )
                        run_lse[here] = jnp.where(live, best + jnp.log(share), old_lse)
        lane = lax.broadcasted_iota(jnp.int32, (own_rows, HEAD), 1)
        for part in range(part_total):
            at = part * own_rows
            out_ref[part, :, :width] = run_out[at : at + own_rows, :].astype(jnp.bfloat16)
            lse = jnp.zeros((own_rows, HEAD), jnp.float32)
            for h in range(head_count):
                piece = run_lse[at : at + own_rows, h * HEAD : (h + 1) * HEAD]
                lse = jnp.where(lax.rem(lane, head_count) == h, piece, lse)
            first = lse.astype(jnp.bfloat16)
            rest = lse - first.astype(jnp.float32)
            second = rest.astype(jnp.bfloat16)
            third = rest - second.astype(jnp.float32)
            field = lax.div(lane, head_count)
            packed = jnp.where(
                field == 0,
                first.astype(jnp.float32),
                jnp.where(
                    field == 1,
                    second.astype(jnp.float32),
                    jnp.where(field == 2, third, 0.0),
                ),
            )
            out_ref[part, :, width:] = packed.astype(jnp.bfloat16)

    most = max(rows for _, _, rows in levels) * group_size
    vmem = pl.BlockSpec(memory_space=pltpu.VMEM)
    smem = pl.BlockSpec(memory_space=pltpu.SMEM)
    return pl.pallas_call(
        kernel,
        out_shape=jax.ShapeDtypeStruct((part_total, own_rows, width + HEAD), jnp.bfloat16),
        in_specs=[smem, smem] + [vmem] * (part_total + 3),
        out_specs=vmem,
        scratch_shapes=[
            pltpu.VMEM((total_rows, width), jnp.bfloat16),
            pltpu.VMEM((total_rows, width), jnp.float32),
            pltpu.VMEM((total_rows, width), jnp.float32),
            pltpu.VMEM((HEAD, most), jnp.float32),
            pltpu.VMEM((1, most), jnp.float32),
            pltpu.VMEM((1, most), jnp.float32),
        ],
        compiler_params=pltpu.CompilerParams(vmem_limit_bytes=48 << 20),
        name="tree_attention",
    )(nodes, owner[None], *query_parts, *caches)


def swap(value, axis_name, mask):
    axis_total = lax.axis_size(axis_name)
    return lax.ppermute(value, axis_name, [(j, j ^ mask) for j in range(axis_total)])


def gather_parts(value, axis_name):
    parts = [value] * lax.axis_size(axis_name)
    for mask in range(len(parts) - 2, 0, -2):
        parts[mask] = swap(value, axis_name, mask)
    for mask in [0] + list(range(len(parts) - 2, 0, -2)):
        parts[mask + 1] = swap(parts[mask], axis_name, 1)
    return parts


def scatter_sum(parts, axis_name):
    wide = jnp.float32
    evens = list(range(len(parts) - 2, -1, -2))
    pairs = {
        mask: parts[mask].astype(wide) + swap(parts[mask + 1], axis_name, 1).astype(wide)
        for mask in evens
    }
    summed = pairs[0]
    for mask in evens[:-1]:
        summed = summed + swap(pairs[mask].astype(jnp.bfloat16), axis_name, mask).astype(wide)
    return summed


def shards(
    queries,
    root_cache,
    mid_cache,
    leaf_cache,
    token_leaf,
    leaf_parent,
    mid_parent,
    root_len,
    mid_len,
    leaf_len,
    root_slot,
    mid_slot,
    leaf_slot,
    stream,
    out_weight,
    norm_gain,
    gate_weight,
    up_weight,
    down_weight,
):
    own_rows, width = queries.shape
    head_count = width // HEAD
    owner = lax.axis_index("kv").astype(jnp.int32)
    caches = (root_cache, mid_cache, leaf_cache)
    nodes = own_nodes(
        owner,
        [cache.shape[0] for cache in caches],
        (token_leaf, leaf_parent, mid_parent),
        (root_len, mid_len, leaf_len),
        (root_slot, mid_slot, leaf_slot),
    )
    parts = tree_attention(gather_parts(queries, "kv"), caches, nodes, owner)
    every = lax.all_to_all(parts, "kv", 0, 0)
    fields = every[:, :, width : width + 3 * head_count].astype(jnp.float32)
    every_lse = (
        fields[:, :, :head_count]
        + fields[:, :, head_count : 2 * head_count]
        + fields[:, :, 2 * head_count :]
    )
    every_out = every[:, :, :width].reshape(-1, own_rows, head_count, HEAD)
    share = jnp.exp(every_lse - jnp.max(every_lse, axis=0))
    attended = (
        (
            jnp.sum(every_out.astype(jnp.float32) * share[..., None], axis=0)
            / jnp.sum(share, axis=0)[..., None]
        )
        .reshape(own_rows, width)
        .astype(jnp.bfloat16)
    )
    mlp_total = lax.axis_size("mlp")
    own_width = stream.shape[1]
    projected = lax.dot_general(
        attended, out_weight, (((1,), (0,)), ((), ())), preferred_element_type=jnp.float32
    ).astype(jnp.bfloat16)
    projected = projected.reshape(own_rows, mlp_total, own_width).transpose(1, 0, 2)
    projected = jnp.sum(lax.all_to_all(projected, "mlp", 0, 0).astype(jnp.float32), axis=0)
    residual = (stream.astype(jnp.float32) + projected).astype(jnp.bfloat16)
    widened = lax.optimization_barrier(residual).astype(jnp.float32)
    square_sum = jnp.sum(widened * widened, axis=1)
    square_parts = gather_parts(square_sum[None, :], "kv")
    scaled = jnp.concatenate(
        gather_parts((widened * norm_gain).astype(jnp.bfloat16), "kv"), axis=0
    )
    gate_up = jnp.concatenate([gate_weight, up_weight], axis=1)
    unit_count = gate_weight.shape[1]
    gate_up_sum = jnp.dot(scaled, gate_up, preferred_element_type=jnp.float32)
    share_rows = halve(gate_up_sum.astype(jnp.bfloat16), "mlp", mlp_total)
    every_square = jnp.concatenate(square_parts, axis=1).reshape(-1)
    every_square = jnp.sum(lax.all_gather(every_square, "mlp"), axis=0)
    row_scale = halve_place(lax.rsqrt(every_square / D + EPSILON), "mlp", mlp_total)
    share_rows = share_rows.astype(jnp.float32) * row_scale[:, None]
    hidden = (jax.nn.silu(share_rows[:, :unit_count]) * share_rows[:, unit_count:]).astype(
        jnp.bfloat16
    )
    hidden = double(hidden, "mlp", mlp_total)
    partial_mixed = jnp.dot(hidden, down_weight, preferred_element_type=jnp.float32)
    partial_mixed = partial_mixed.astype(jnp.bfloat16)
    mixed = scatter_sum(jnp.split(partial_mixed, lax.axis_size("kv"), axis=0), "kv")
    return (attended, mixed.astype(jnp.bfloat16))


def halve_place(rows, axis_name, axis_total):
    place = lax.axis_index(axis_name)
    step = 1
    while step < axis_total:
        half = rows.shape[0] // 2
        rows = lax.dynamic_slice_in_dim(rows, ((place // step) % 2) * half, half, 0)
        step *= 2
    return rows


def halve(rows, axis_name, axis_total):
    place = lax.axis_index(axis_name)
    step = 1
    while step < axis_total:
        half = rows.shape[0] // 2
        side = (place // step) % 2
        keep = lax.dynamic_slice_in_dim(rows, side * half, half, 0)
        send = lax.dynamic_slice_in_dim(rows, (1 - side) * half, half, 0)
        got = lax.ppermute(send, axis_name, [(j, j ^ step) for j in range(axis_total)])
        rows = (keep.astype(jnp.float32) + got.astype(jnp.float32)).astype(jnp.bfloat16)
        step *= 2
    return rows


def double(rows, axis_name, axis_total):
    place = lax.axis_index(axis_name)
    step = axis_total // 2
    while step > 0:
        got = lax.ppermute(rows, axis_name, [(j, j ^ step) for j in range(axis_total)])
        low = (place // step) % 2 == 0
        rows = jnp.where(
            low, jnp.concatenate([rows, got], axis=0), jnp.concatenate([got, rows], axis=0)
        )
        step //= 2
    return rows


def solution(mesh):
    in_specs = (
        P("kv", "mlp"),
        P("kv", None, "mlp"),
        P("kv", None, "mlp"),
        P("kv", None, "mlp"),
        P(),
        P(),
        P(),
        P(),
        P(),
        P(),
        P(),
        P(),
        P(),
        P("kv", "mlp"),
        P("mlp", None),
        P("mlp"),
        P("mlp", "kv"),
        P("mlp", "kv"),
        P("kv", "mlp"),
    )
    out_specs = (P("kv", "mlp"), P("kv", "mlp"))
    return jax.shard_map(shards, mesh=mesh, in_specs=in_specs, out_specs=out_specs, check_vma=False)
```

```python
import math

import jax
import jax.numpy as jnp
from jax import lax
from jax.experimental import pallas as pl
from jax.experimental.pallas import tpu as pltpu
from jax.sharding import PartitionSpec as P

D = 4096
HEAD = 128
QLEAF = 16
QMID = 48
QROOT = 144


LOWEST = -1e30
EPSILON = 1e-05
ALIGN = 16
BLOCK = 512


def own_nodes(owner, local_counts, tree, lengths, slots):
    token_leaf, leaf_parent, mid_parent = tree
    node_total = sum(local_counts)

    def kernel(owner_ref, token_ref, leaf_up, mid_up, *refs):
        len_refs, slot_refs, out_ref = refs[:3], refs[3:6], refs[6]

        def find(slot_ref, len_ref, local):
            base = owner_ref[0] * local

            def step(j, found):
                at, size = slot_ref[j] - base, len_ref[j]
                return tuple(
                    (jnp.where(at == k, j, node), jnp.where(at == k, size, length))
                    for k, (node, length) in enumerate(found)
                )

            zero = jnp.int32(0)
            return lax.fori_loop(0, slot_ref.shape[0], step, ((zero, zero),) * local)

        def below(parent_ref, edges):
            def step(j, counted):
                parent = parent_ref[j]
                return tuple(
                    c + jnp.where(parent < edge, 1, 0) for c, edge in zip(counted, edges)
                )

            return lax.fori_loop(0, parent_ref.shape[0], step, (jnp.int32(0),) * len(edges))

        picked = [find(*level) for level in zip(slot_refs, len_refs, local_counts)]
        edges = ()
        for level, parent_ref in enumerate((mid_up, leaf_up, None)):
            for node, _ in picked[level]:
                edges += (node, node + 1)
            if parent_ref is not None:
                edges = below(parent_ref, edges)
        tokens = token_ref[...]
        sizes = [length for level in picked for _, length in level]
        for k in range(node_total):
            for side in range(2):
                under = jnp.where(tokens < edges[2 * k + side], 1.0, 0.0)
                out_ref[side, k] = jnp.sum(under).astype(jnp.int32)
            out_ref[2, k] = sizes[k]

    smem = pl.BlockSpec(memory_space=pltpu.SMEM)
    vmem = pl.BlockSpec(memory_space=pltpu.VMEM)
    return pl.pallas_call(
        kernel,
        out_shape=jax.ShapeDtypeStruct((3, node_total), jnp.int32),
        in_specs=[smem, vmem] + [smem] * 8,
        out_specs=smem,
        name="own_nodes",
    )(owner[None], token_leaf.reshape(-1, HEAD), leaf_parent, mid_parent, *lengths, *slots)


def tree_attention(query_parts, caches, nodes, owner, kv_head):
    part_total = len(query_parts)
    own_rows, width = query_parts[0].shape
    total_rows = part_total * own_rows
    group_size = width // HEAD
    score_scale = 1.0 / math.sqrt(HEAD)
    levels = []
    for cache, capacity in zip(caches, (QROOT, QMID, QLEAF)):
        levels.append((cache.shape[0], cache.shape[1], min(capacity + ALIGN, total_rows)))

    def kernel(nodes_ref, owner_ref, *refs):
        query_refs = refs[:part_total]
        cache_refs = refs[part_total : part_total + 3]
        out_ref, all_rows, run_out, run_lse, acc, peak, total = refs[part_total + 3 :]
        me = owner_ref[0]
        for part in range(part_total):
            row = pl.multiple_of((me ^ part) * own_rows, ALIGN)
            all_rows[pl.ds(row, own_rows), :] = query_refs[part][...]
        run_out[...] = jnp.zeros_like(run_out)
        run_lse[...] = jnp.full_like(run_lse, LOWEST)
        node = 0
        for (slot_total, span, rows), cache_ref in zip(levels, cache_refs):
            lanes = rows * group_size
            block = min(BLOCK, span)
            for member in range(slot_total):
                low, high, length = nodes_ref[0, node], nodes_ref[1, node], nodes_ref[2, node]
                node += 1
                window = jnp.minimum(low - lax.rem(low, ALIGN), total_rows - rows)
                window = pl.multiple_of(window, ALIGN)
                columns = [h * HEAD for h in range(group_size)]
                if True:
                    grouped = jnp.concatenate(
                        [all_rows[pl.ds(window, rows), c : c + HEAD] for c in columns], axis=0
                    )
                    acc[:, :lanes] = jnp.zeros((HEAD, lanes), jnp.float32)
                    peak[:, :lanes] = jnp.full((1, lanes), LOWEST, jnp.float32)
                    total[:, :lanes] = jnp.zeros((1, lanes), jnp.float32)

                    def visit(index, carry, masked):
                        at = pl.multiple_of(index * block, block)
                        keys = cache_ref[
                            member, pl.ds(at, block), 2 * kv_head * HEAD : (2 * kv_head + 1) * HEAD
                        ]
                        values = cache_ref[
                            member,
                            pl.ds(at, block),
                            (2 * kv_head + 1) * HEAD : (2 * kv_head + 2) * HEAD,
                        ]
                        scores = lax.dot_general(
                            keys,
                            grouped,
                            (((1,), (1,)), ((), ())),
                            preferred_element_type=jnp.float32,
                        )
                        if masked:
                            position = at + lax.broadcasted_iota(jnp.int32, (block, lanes), 0)
                            scores = jnp.where(position < length, scores, LOWEST)
                        old_peak = peak[:, :lanes]
                        new_peak = jnp.maximum(old_peak, jnp.max(scores, axis=0, keepdims=True))
                        weights = jnp.exp((scores - new_peak) * score_scale)
                        fade = jnp.exp((old_peak - new_peak) * score_scale)
                        peak[:, :lanes] = new_peak
                        total[:, :lanes] = total[:, :lanes] * fade + jnp.sum(
                            weights, axis=0, keepdims=True
                        )
                        acc[:, :lanes] = acc[:, :lanes] * fade + lax.dot_general(
                            values,
                            weights.astype(jnp.bfloat16),
                            (((0,), (0,)), ((), ())),
                            preferred_element_type=jnp.float32,
                        )
                        return carry

                    whole = lax.div(length, block)
                    lax.fori_loop(0, whole, lambda i, c: visit(i, c, False), 0)

                    @pl.when(whole * block < length)
                    def _():
                        visit(whole, 0, True)

                    weight_sum = total[:, :lanes]
                    part_out = (acc[:, :lanes] / weight_sum).T
                    part_lse = jnp.broadcast_to(
                        peak[:, :lanes] * score_scale + jnp.log(weight_sum), (HEAD, lanes)
                    ).T
                    position = window + lax.broadcasted_iota(jnp.int32, (rows, HEAD), 0)
                    live = (position >= low) & (position < high)
                    for h, c in enumerate(columns):
                        here = (pl.ds(window, rows), slice(c, c + HEAD))
                        old_lse, old_out = run_lse[here], run_out[here]
                        add_lse = part_lse[h * rows : (h + 1) * rows]
                        add_out = part_out[h * rows : (h + 1) * rows]
                        best = jnp.maximum(old_lse, add_lse)
                        old_share = jnp.exp(old_lse - best)
                        add_share = jnp.exp(add_lse - best)
                        share = old_share + add_share
                        run_out[here] = jnp.where(
                            live, (old_out * old_share + add_out * add_share) / share, old_out
                        )
                        run_lse[here] = jnp.where(live, best + jnp.log(share), old_lse)
        lane = lax.broadcasted_iota(jnp.int32, (own_rows, HEAD), 1)
        for part in range(part_total):
            at = part * own_rows
            out_ref[part, :, :width] = run_out[at : at + own_rows, :].astype(jnp.bfloat16)
            lse = jnp.zeros((own_rows, HEAD), jnp.float32)
            for h in range(group_size):
                piece = run_lse[at : at + own_rows, h * HEAD : (h + 1) * HEAD]
                lse = jnp.where(lax.rem(lane, group_size) == h, piece, lse)
            first = lse.astype(jnp.bfloat16)
            rest = lse - first.astype(jnp.float32)
            second = rest.astype(jnp.bfloat16)
            third = rest - second.astype(jnp.float32)
            field = lax.div(lane, group_size)
            packed = jnp.where(
                field == 0,
                first.astype(jnp.float32),
                jnp.where(
                    field == 1,
                    second.astype(jnp.float32),
                    jnp.where(field == 2, third, 0.0),
                ),
            )
            out_ref[part, :, width:] = packed.astype(jnp.bfloat16)

    most = max(rows for _, _, rows in levels) * group_size
    vmem = pl.BlockSpec(memory_space=pltpu.VMEM)
    smem = pl.BlockSpec(memory_space=pltpu.SMEM)
    return pl.pallas_call(
        kernel,
        out_shape=jax.ShapeDtypeStruct((part_total, own_rows, width + HEAD), jnp.bfloat16),
        in_specs=[smem, smem] + [vmem] * (part_total + 3),
        out_specs=vmem,
        scratch_shapes=[
            pltpu.VMEM((total_rows, width), jnp.bfloat16),
            pltpu.VMEM((total_rows, width), jnp.float32),
            pltpu.VMEM((total_rows, width), jnp.float32),
            pltpu.VMEM((HEAD, most), jnp.float32),
            pltpu.VMEM((1, most), jnp.float32),
            pltpu.VMEM((1, most), jnp.float32),
        ],
        compiler_params=pltpu.CompilerParams(vmem_limit_bytes=48 << 20),
        name="tree_attention",
    )(nodes, owner[None], *query_parts, *caches)


def combine(every, group_size):
    width = group_size * HEAD
    fields = every[:, :, width : width + 3 * group_size].astype(jnp.float32)
    every_lse = (
        fields[:, :, :group_size]
        + fields[:, :, group_size : 2 * group_size]
        + fields[:, :, 2 * group_size :]
    )
    every_out = every[:, :, :width].reshape(every.shape[0], every.shape[1], group_size, HEAD)
    share = jnp.exp(every_lse - jnp.max(every_lse, axis=0))
    summed = jnp.sum(every_out.astype(jnp.float32) * share[..., None], axis=0)
    summed = summed / jnp.sum(share, axis=0)[..., None]
    return summed.reshape(every.shape[1], width).astype(jnp.bfloat16)


def swap(value, axis_name, mask):
    axis_total = lax.axis_size(axis_name)
    return lax.ppermute(value, axis_name, [(j, j ^ mask) for j in range(axis_total)])


def gather_parts(value, axis_name):
    parts = [value] * lax.axis_size(axis_name)
    for mask in range(len(parts) - 2, 0, -2):
        parts[mask] = swap(value, axis_name, mask)
    for mask in [0] + list(range(len(parts) - 2, 0, -2)):
        parts[mask + 1] = swap(parts[mask], axis_name, 1)
    return parts


def scatter_sum(parts, axis_name):
    wide = jnp.float32
    evens = list(range(len(parts) - 2, -1, -2))
    pairs = {
        mask: parts[mask].astype(wide) + swap(parts[mask + 1], axis_name, 1).astype(wide)
        for mask in evens
    }
    summed = pairs[0]
    for mask in evens[:-1]:
        summed = summed + swap(pairs[mask].astype(jnp.bfloat16), axis_name, mask).astype(wide)
    return summed


def shards(
    queries,
    root_cache,
    mid_cache,
    leaf_cache,
    token_leaf,
    leaf_parent,
    mid_parent,
    root_len,
    mid_len,
    leaf_len,
    root_slot,
    mid_slot,
    leaf_slot,
    stream,
    out_weight,
    norm_gain,
    gate_weight,
    up_weight,
    down_weight,
):
    own_rows, width = queries.shape
    owner = lax.axis_index("kv").astype(jnp.int32)
    caches = (root_cache, mid_cache, leaf_cache)
    nodes = own_nodes(
        owner,
        [cache.shape[0] for cache in caches],
        (token_leaf, leaf_parent, mid_parent),
        (root_len, mid_len, leaf_len),
        (root_slot, mid_slot, leaf_slot),
    )
    kv_count = root_cache.shape[2] // (2 * HEAD)
    group_width = width // kv_count
    group_size = group_width // HEAD
    gathered = [
        gather_parts(queries[:, k * group_width : (k + 1) * group_width], "kv")
        for k in range(kv_count)
    ]
    attended, projected = [], 0.0
    for k in range(kv_count):
        parts = tree_attention(gathered[k], caches, nodes, owner, k)
        attended.append(combine(lax.all_to_all(parts, "kv", 0, 0), group_size))
        projected = projected + jnp.dot(
            attended[k],
            out_weight[k * group_width : (k + 1) * group_width],
            preferred_element_type=jnp.float32,
        )
    attended = jnp.concatenate(attended, axis=1)
    mlp_total = lax.axis_size("mlp")
    own_width = stream.shape[1]
    projected = projected.astype(jnp.bfloat16)
    projected = projected.reshape(own_rows, mlp_total, own_width).transpose(1, 0, 2)
    projected = jnp.sum(lax.all_to_all(projected, "mlp", 0, 0).astype(jnp.float32), axis=0)
    residual = (stream.astype(jnp.float32) + projected).astype(jnp.bfloat16)
    rows = jnp.concatenate(gather_parts(residual, "kv"), axis=0)
    widened = lax.optimization_barrier(rows).astype(jnp.float32)
    squares = jnp.sum(widened * widened, axis=1)[None, :]
    step = 1
    while step < mlp_total:
        squares = squares + swap(squares, "mlp", step)
        step *= 2
    scaled = (widened * norm_gain).astype(jnp.bfloat16)
    gate_up = jnp.concatenate([gate_weight, up_weight], axis=1)
    unit_count = gate_weight.shape[1]
    gate_up_sum = jnp.dot(scaled, gate_up, preferred_element_type=jnp.float32)
    share_rows = halve(gate_up_sum.astype(jnp.bfloat16), "mlp", mlp_total)
    row_scale = halve_place(lax.rsqrt(squares[0] / D + EPSILON), "mlp", mlp_total)
    share_rows = share_rows.astype(jnp.float32) * row_scale[:, None]
    hidden = (jax.nn.silu(share_rows[:, :unit_count]) * share_rows[:, unit_count:]).astype(
        jnp.bfloat16
    )
    hidden = double(hidden, "mlp", mlp_total)
    partial_mixed = jnp.dot(hidden, down_weight, preferred_element_type=jnp.float32)
    partial_mixed = partial_mixed.astype(jnp.bfloat16)
    mixed = scatter_sum(jnp.split(partial_mixed, lax.axis_size("kv"), axis=0), "kv")
    return (attended, mixed.astype(jnp.bfloat16))


def halve_place(rows, axis_name, axis_total):
    place = lax.axis_index(axis_name)
    step = 1
    while step < axis_total:
        half = rows.shape[0] // 2
        rows = lax.dynamic_slice_in_dim(rows, ((place // step) % 2) * half, half, 0)
        step *= 2
    return rows


def halve(rows, axis_name, axis_total):
    place = lax.axis_index(axis_name)
    step = 1
    while step < axis_total:
        half = rows.shape[0] // 2
        side = (place // step) % 2
        keep = lax.dynamic_slice_in_dim(rows, side * half, half, 0)
        send = lax.dynamic_slice_in_dim(rows, (1 - side) * half, half, 0)
        got = lax.ppermute(send, axis_name, [(j, j ^ step) for j in range(axis_total)])
        rows = (keep.astype(jnp.float32) + got.astype(jnp.float32)).astype(jnp.bfloat16)
        step *= 2
    return rows


def double(rows, axis_name, axis_total):
    place = lax.axis_index(axis_name)
    step = axis_total // 2
    while step > 0:
        got = lax.ppermute(rows, axis_name, [(j, j ^ step) for j in range(axis_total)])
        low = (place // step) % 2 == 0
        rows = jnp.where(
            low, jnp.concatenate([rows, got], axis=0), jnp.concatenate([got, rows], axis=0)
        )
        step //= 2
    return rows


def solution(mesh):
    in_specs = (
        P("kv", "mlp"),
        P("kv", None, "mlp"),
        P("kv", None, "mlp"),
        P("kv", None, "mlp"),
        P(),
        P(),
        P(),
        P(),
        P(),
        P(),
        P(),
        P(),
        P(),
        P("kv", "mlp"),
        P("mlp", None),
        P("mlp"),
        P("mlp", "kv"),
        P("mlp", "kv"),
        P("kv", "mlp"),
    )
    out_specs = (P("kv", "mlp"), P("kv", "mlp"))
    return jax.shard_map(shards, mesh=mesh, in_specs=in_specs, out_specs=out_specs, check_vma=False)
```

```python
import math

import jax
import jax.numpy as jnp
from jax import lax
from jax.experimental import pallas as pl
from jax.experimental.pallas import tpu as pltpu
from jax.sharding import PartitionSpec as P

D = 4096
HEAD = 128
QLEAF = 16
QMID = 48
QROOT = 144


LOWEST = -1e30
EPSILON = 1e-05
ALIGN = 16
BLOCK = 512


def own_nodes(owner, local_counts, tree, lengths, slots):
    token_leaf, leaf_parent, mid_parent = tree
    node_total = sum(local_counts)

    def kernel(owner_ref, token_ref, leaf_up, mid_up, *refs):
        len_refs, slot_refs, out_ref = refs[:3], refs[3:6], refs[6]

        def find(slot_ref, len_ref, local):
            base = owner_ref[0] * local

            def step(j, found):
                at, size = slot_ref[j] - base, len_ref[j]
                return tuple(
                    (jnp.where(at == k, j, node), jnp.where(at == k, size, length))
                    for k, (node, length) in enumerate(found)
                )

            zero = jnp.int32(0)
            return lax.fori_loop(0, slot_ref.shape[0], step, ((zero, zero),) * local)

        def below(parent_ref, edges):
            def step(j, counted):
                parent = parent_ref[j]
                return tuple(
                    c + jnp.where(parent < edge, 1, 0) for c, edge in zip(counted, edges)
                )

            return lax.fori_loop(0, parent_ref.shape[0], step, (jnp.int32(0),) * len(edges))

        picked = [find(*level) for level in zip(slot_refs, len_refs, local_counts)]
        edges = ()
        for level, parent_ref in enumerate((mid_up, leaf_up, None)):
            for node, _ in picked[level]:
                edges += (node, node + 1)
            if parent_ref is not None:
                edges = below(parent_ref, edges)
        tokens = token_ref[...]
        sizes = [length for level in picked for _, length in level]
        for k in range(node_total):
            for side in range(2):
                under = jnp.where(tokens < edges[2 * k + side], 1.0, 0.0)
                out_ref[side, k] = jnp.sum(under).astype(jnp.int32)
            out_ref[2, k] = sizes[k]

    smem = pl.BlockSpec(memory_space=pltpu.SMEM)
    vmem = pl.BlockSpec(memory_space=pltpu.VMEM)
    return pl.pallas_call(
        kernel,
        out_shape=jax.ShapeDtypeStruct((3, node_total), jnp.int32),
        in_specs=[smem, vmem] + [smem] * 8,
        out_specs=smem,
        name="own_nodes",
    )(owner[None], token_leaf.reshape(-1, HEAD), leaf_parent, mid_parent, *lengths, *slots)


def tree_attention(query_parts, caches, nodes, owner, kv_head):
    part_total = len(query_parts)
    own_rows = query_parts[0].shape[0]
    total_rows = part_total * own_rows
    width = query_parts[0].shape[1] // (caches[0].shape[2] // (2 * HEAD))
    group_size = width // HEAD
    score_scale = 1.0 / math.sqrt(HEAD)
    levels = []
    for cache, capacity in zip(caches, (QROOT, QMID, QLEAF)):
        levels.append((cache.shape[0], cache.shape[1], min(capacity + ALIGN, total_rows)))

    def kernel(nodes_ref, owner_ref, *refs):
        query_refs = refs[:part_total]
        cache_refs = refs[part_total : part_total + 3]
        out_ref, all_rows, run_out, run_lse, acc, peak, total = refs[part_total + 3 :]
        me = owner_ref[0]
        for part in range(part_total):
            row = pl.multiple_of((me ^ part) * own_rows, ALIGN)
            all_rows[pl.ds(row, own_rows), :] = query_refs[part][
                :, kv_head * width : (kv_head + 1) * width
            ]
        run_out[...] = jnp.zeros_like(run_out)
        run_lse[...] = jnp.full_like(run_lse, LOWEST)
        node = 0
        for (slot_total, span, rows), cache_ref in zip(levels, cache_refs):
            lanes = rows * group_size
            block = min(BLOCK, span)
            for member in range(slot_total):
                low, high, length = nodes_ref[0, node], nodes_ref[1, node], nodes_ref[2, node]
                node += 1
                window = jnp.minimum(low - lax.rem(low, ALIGN), total_rows - rows)
                window = pl.multiple_of(window, ALIGN)
                columns = [h * HEAD for h in range(group_size)]
                grouped = jnp.concatenate(
                    [all_rows[pl.ds(window, rows), c : c + HEAD] for c in columns], axis=0
                )
                acc[:, :lanes] = jnp.zeros((HEAD, lanes), jnp.float32)
                peak[:, :lanes] = jnp.full((1, lanes), LOWEST, jnp.float32)
                total[:, :lanes] = jnp.zeros((1, lanes), jnp.float32)

                def visit(index, carry, masked):
                    at = pl.multiple_of(index * block, block)
                    keys = cache_ref[
                        member, pl.ds(at, block), 2 * kv_head * HEAD : (2 * kv_head + 1) * HEAD
                    ]
                    values = cache_ref[
                        member,
                        pl.ds(at, block),
                        (2 * kv_head + 1) * HEAD : (2 * kv_head + 2) * HEAD,
                    ]
                    scores = lax.dot_general(
                        keys,
                        grouped,
                        (((1,), (1,)), ((), ())),
                        preferred_element_type=jnp.float32,
                    )
                    if masked:
                        position = at + lax.broadcasted_iota(jnp.int32, (block, lanes), 0)
                        scores = jnp.where(position < length, scores, LOWEST)
                    old_peak = peak[:, :lanes]
                    new_peak = jnp.maximum(old_peak, jnp.max(scores, axis=0, keepdims=True))
                    weights = jnp.exp((scores - new_peak) * score_scale)
                    fade = jnp.exp((old_peak - new_peak) * score_scale)
                    peak[:, :lanes] = new_peak
                    total[:, :lanes] = total[:, :lanes] * fade + jnp.sum(
                        weights, axis=0, keepdims=True
                    )
                    acc[:, :lanes] = acc[:, :lanes] * fade + lax.dot_general(
                        values,
                        weights.astype(jnp.bfloat16),
                        (((0,), (0,)), ((), ())),
                        preferred_element_type=jnp.float32,
                    )
                    return carry

                whole = lax.div(length, block)
                lax.fori_loop(0, whole, lambda i, c: visit(i, c, False), 0)

                @pl.when(whole * block < length)
                def _():
                    visit(whole, 0, True)

                weight_sum = total[:, :lanes]
                part_out = (acc[:, :lanes] / weight_sum).T
                part_lse = jnp.broadcast_to(
                    peak[:, :lanes] * score_scale + jnp.log(weight_sum), (HEAD, lanes)
                ).T
                position = window + lax.broadcasted_iota(jnp.int32, (rows, HEAD), 0)
                live = (position >= low) & (position < high)
                for h, c in enumerate(columns):
                    here = (pl.ds(window, rows), slice(c, c + HEAD))
                    old_lse, old_out = run_lse[here], run_out[here]
                    add_lse = part_lse[h * rows : (h + 1) * rows]
                    add_out = part_out[h * rows : (h + 1) * rows]
                    best = jnp.maximum(old_lse, add_lse)
                    old_share = jnp.exp(old_lse - best)
                    add_share = jnp.exp(add_lse - best)
                    share = old_share + add_share
                    run_out[here] = jnp.where(
                        live, (old_out * old_share + add_out * add_share) / share, old_out
                    )
                    run_lse[here] = jnp.where(live, best + jnp.log(share), old_lse)
        lane = lax.broadcasted_iota(jnp.int32, (own_rows, HEAD), 1)
        for part in range(part_total):
            at = part * own_rows
            out_ref[part, :, :width] = run_out[at : at + own_rows, :].astype(jnp.bfloat16)
            lse = jnp.zeros((own_rows, HEAD), jnp.float32)
            for h in range(group_size):
                piece = run_lse[at : at + own_rows, h * HEAD : (h + 1) * HEAD]
                lse = jnp.where(lax.rem(lane, group_size) == h, piece, lse)
            first = lse.astype(jnp.bfloat16)
            rest = lse - first.astype(jnp.float32)
            second = rest.astype(jnp.bfloat16)
            third = rest - second.astype(jnp.float32)
            field = lax.div(lane, group_size)
            packed = jnp.where(
                field == 0,
                first.astype(jnp.float32),
                jnp.where(
                    field == 1,
                    second.astype(jnp.float32),
                    jnp.where(field == 2, third, 0.0),
                ),
            )
            out_ref[part, :, width:] = packed.astype(jnp.bfloat16)

    most = max(rows for _, _, rows in levels) * group_size
    vmem = pl.BlockSpec(memory_space=pltpu.VMEM)
    smem = pl.BlockSpec(memory_space=pltpu.SMEM)
    return pl.pallas_call(
        kernel,
        out_shape=jax.ShapeDtypeStruct((part_total, own_rows, width + HEAD), jnp.bfloat16),
        in_specs=[smem, smem] + [vmem] * (part_total + 3),
        out_specs=vmem,
        scratch_shapes=[
            pltpu.VMEM((total_rows, width), jnp.bfloat16),
            pltpu.VMEM((total_rows, width), jnp.float32),
            pltpu.VMEM((total_rows, width), jnp.float32),
            pltpu.VMEM((HEAD, most), jnp.float32),
            pltpu.VMEM((1, most), jnp.float32),
            pltpu.VMEM((1, most), jnp.float32),
        ],
        compiler_params=pltpu.CompilerParams(vmem_limit_bytes=48 << 20),
        name="tree_attention",
    )(nodes, owner[None], *query_parts, *caches)


def combine_project(every, weight, row_start, added, place, own_width):
    part_total, own_rows, wide = every.shape
    width = wide - HEAD
    group_size = width // HEAD
    block_total = weight.shape[1] // own_width
    last = added is not None or width == weight.shape[0]
    kind = jnp.bfloat16 if last else jnp.float32

    def kernel(place_ref, every_ref, weight_ref, *refs):
        added_refs = refs[:block_total] if added is not None else (None,) * block_total
        attended_ref, *block_refs = refs[len(refs) - 1 - block_total :]
        lse = []
        for part in range(part_total):
            terms = every_ref[part, :, width:].astype(jnp.float32)
            lse.append(
                terms
                + pltpu.roll(terms, HEAD - group_size, 1)
                + pltpu.roll(terms, HEAD - 2 * group_size, 1)
            )
        best = lse[0]
        for one in lse[1:]:
            best = jnp.maximum(best, one)
        share = [jnp.exp(one - best) for one in lse]
        whole = share[0]
        for one in share[1:]:
            whole = whole + one
        for h in range(group_size):
            summed = jnp.zeros((own_rows, HEAD), jnp.float32)
            for part in range(part_total):
                summed = summed + (
                    every_ref[part, :, h * HEAD : (h + 1) * HEAD].astype(jnp.float32)
                    * share[part][:, h : h + 1]
                )
            attended_ref[:, h * HEAD : (h + 1) * HEAD] = (summed / whole[:, h : h + 1]).astype(
                jnp.bfloat16
            )
        for block in range(block_total):
            at = pl.multiple_of((place_ref[0] ^ block) * own_width, HEAD)
            product = jnp.dot(
                attended_ref[...],
                weight_ref[row_start : row_start + width, pl.ds(at, own_width)],
                preferred_element_type=jnp.float32,
            )
            if added is not None:
                product = product + added_refs[block][...]
            block_refs[block][...] = product.astype(kind)

    vmem = pl.BlockSpec(memory_space=pltpu.VMEM)
    outs = pl.pallas_call(
        kernel,
        out_shape=[jax.ShapeDtypeStruct((own_rows, width), jnp.bfloat16)]
        + [jax.ShapeDtypeStruct((own_rows, own_width), kind)] * block_total,
        in_specs=[pl.BlockSpec(memory_space=pltpu.SMEM)]
        + [vmem] * (2 + (block_total if added is not None else 0)),
        out_specs=[vmem] * (1 + block_total),
        compiler_params=pltpu.CompilerParams(vmem_limit_bytes=48 << 20),
        name="combine_project",
    )(place[None], every, weight, *(added or ()))
    return outs[0], outs[1:]


def split_terms(value):
    first = value.astype(jnp.bfloat16).astype(jnp.float32)
    second = (value - first).astype(jnp.bfloat16).astype(jnp.float32)
    lane = lax.broadcasted_iota(jnp.int32, value.shape, 1)
    third = jnp.where(lane == 2, value - first - second, 0.0)
    return jnp.where(lane == 0, first, jnp.where(lane == 1, second, third)).astype(jnp.bfloat16)


def gate_up_rows(parts, norm_gain, gate_weight, up_weight, spot, group_total):
    own_rows, features = parts[0].shape
    rows = own_rows * len(parts)
    half = rows // 2
    each = len(parts) // group_total
    units = gate_weight.shape[1]

    def kernel(spot_ref, gain_ref, gate_ref, up_ref, *refs):
        part_refs = refs[: len(parts)]
        keep_ref, send_ref, scaled, squares = refs[len(parts) :]
        for index, part_ref in enumerate(part_refs):
            at = ((index // each) ^ spot_ref[0]) * each + index % each
            here = pl.ds(pl.multiple_of(at * own_rows, ALIGN), own_rows)
            wide = part_ref[...].astype(jnp.float32)
            scaled[here, :] = (wide * gain_ref[...]).astype(jnp.bfloat16)
            squares[here, :] = jnp.broadcast_to(
                jnp.sum(wide * wide, axis=1, keepdims=True), (own_rows, HEAD)
            )
        for column, weight_ref in ((0, gate_ref), (units, up_ref)):
            product = jnp.dot(
                scaled[...], weight_ref[...], preferred_element_type=jnp.float32
            ).astype(jnp.bfloat16)
            keep_ref[:, column : column + units] = product[:half]
            send_ref[:, column : column + units] = product[half:]
        terms = split_terms(squares[...])
        keep_ref[:, 2 * units :] = terms[:half]
        send_ref[:, 2 * units :] = terms[half:]

    vmem = pl.BlockSpec(memory_space=pltpu.VMEM)
    return pl.pallas_call(
        kernel,
        out_shape=[jax.ShapeDtypeStruct((half, 2 * units + HEAD), jnp.bfloat16)] * 2,
        in_specs=[pl.BlockSpec(memory_space=pltpu.SMEM)] + [vmem] * (3 + len(parts)),
        out_specs=[vmem, vmem],
        scratch_shapes=[
            pltpu.VMEM((rows, features), jnp.bfloat16),
            pltpu.VMEM((rows, HEAD), jnp.float32),
        ],
        compiler_params=pltpu.CompilerParams(vmem_limit_bytes=48 << 20),
        name="gate_up",
    )(spot[None], norm_gain[None, :], gate_weight, up_weight, *parts)


def add_halves(keep, got, units):
    half = keep.shape[0] // 2

    def kernel(keep_ref, got_ref, next_ref, send_ref):
        for ref, at in ((next_ref, 0), (send_ref, half)):
            here = pl.ds(at, half)
            ref[:, : 2 * units] = (
                keep_ref[here, : 2 * units].astype(jnp.float32)
                + got_ref[here, : 2 * units].astype(jnp.float32)
            ).astype(jnp.bfloat16)
            terms = keep_ref[here, 2 * units :].astype(jnp.float32)
            terms = terms + got_ref[here, 2 * units :].astype(jnp.float32)
            total = jnp.sum(terms, axis=1, keepdims=True)
            ref[:, 2 * units :] = split_terms(jnp.broadcast_to(total, (half, HEAD)))

    vmem = pl.BlockSpec(memory_space=pltpu.VMEM)
    return pl.pallas_call(
        kernel,
        out_shape=[jax.ShapeDtypeStruct((half, keep.shape[1]), jnp.bfloat16)] * 2,
        in_specs=[vmem, vmem],
        out_specs=[vmem, vmem],
        compiler_params=pltpu.CompilerParams(vmem_limit_bytes=48 << 20),
        name="add_halves",
    )(keep, got)


def gated(keep, got, units):
    def kernel(keep_ref, got_ref, out_ref):
        summed = keep_ref[...].astype(jnp.float32) + got_ref[...].astype(jnp.float32)
        square = jnp.sum(summed[:, 2 * units :], axis=1, keepdims=True)
        scale = lax.rsqrt(square / D + EPSILON)
        gate = summed[:, :units] * scale
        up = summed[:, units : 2 * units] * scale
        out_ref[...] = (gate / (1.0 + jnp.exp(-gate)) * up).astype(jnp.bfloat16)

    vmem = pl.BlockSpec(memory_space=pltpu.VMEM)
    return pl.pallas_call(
        kernel,
        out_shape=jax.ShapeDtypeStruct((keep.shape[0], units), jnp.bfloat16),
        in_specs=[vmem, vmem],
        out_specs=vmem,
        compiler_params=pltpu.CompilerParams(vmem_limit_bytes=48 << 20),
        name="gated",
    )(keep, got)


def down_rows(pieces, down_weight, spot, part_count, own_rows, group_total):
    rows = part_count * own_rows
    each = part_count // group_total
    units, features = down_weight.shape

    def kernel(spot_ref, weight_ref, *refs):
        piece_refs = refs[: len(pieces)]
        out_refs = refs[len(pieces) : len(pieces) + part_count]
        hidden, product = refs[len(pieces) + part_count :]
        at = 0
        for piece_ref in piece_refs:
            hidden[at : at + piece_ref.shape[0], :] = piece_ref[...]
            at += piece_ref.shape[0]
        product[...] = jnp.dot(
            hidden[...], weight_ref[...], preferred_element_type=jnp.float32
        )
        for index, out_ref in enumerate(out_refs):
            at = ((index // each) ^ spot_ref[0]) * each + index % each
            here = pl.ds(pl.multiple_of(at * own_rows, ALIGN), own_rows)
            out_ref[...] = product[here, :].astype(jnp.bfloat16)

    vmem = pl.BlockSpec(memory_space=pltpu.VMEM)
    return pl.pallas_call(
        kernel,
        out_shape=[jax.ShapeDtypeStruct((own_rows, features), jnp.bfloat16)] * part_count,
        in_specs=[pl.BlockSpec(memory_space=pltpu.SMEM)] + [vmem] * (1 + len(pieces)),
        out_specs=[vmem] * part_count,
        scratch_shapes=[
            pltpu.VMEM((rows, units), jnp.bfloat16),
            pltpu.VMEM((rows, features), jnp.float32),
        ],
        compiler_params=pltpu.CompilerParams(vmem_limit_bytes=48 << 20),
        name="down",
    )(spot[None], down_weight, *pieces)


def swap(value, axis_name, mask):
    axis_total = lax.axis_size(axis_name)
    return lax.ppermute(value, axis_name, [(j, j ^ mask) for j in range(axis_total)])


def gather_parts(value, axis_name):
    parts = [value] * lax.axis_size(axis_name)
    for mask in range(len(parts) - 2, 0, -2):
        parts[mask] = swap(value, axis_name, mask)
    for mask in [0] + list(range(len(parts) - 2, 0, -2)):
        parts[mask + 1] = swap(parts[mask], axis_name, 1)
    return parts


def scatter_sum(parts, axis_name):
    wide = jnp.float32
    evens = sorted((mask for mask in parts if mask % 2 == 0), reverse=True)
    got = {mask: swap(parts[mask + 1], axis_name, 1) for mask in evens}
    summed = 0.0
    for mask in evens:
        pair = parts[mask].astype(wide) + got[mask].astype(wide)
        if mask:
            pair = swap(pair.astype(jnp.bfloat16), axis_name, mask).astype(wide)
        summed = summed + pair
    return summed


def shards(
    queries,
    root_cache,
    mid_cache,
    leaf_cache,
    token_leaf,
    leaf_parent,
    mid_parent,
    root_len,
    mid_len,
    leaf_len,
    root_slot,
    mid_slot,
    leaf_slot,
    stream,
    out_weight,
    norm_gain,
    gate_weight,
    up_weight,
    down_weight,
):
    own_rows, width = queries.shape
    owner = lax.axis_index("kv").astype(jnp.int32)
    caches = (root_cache, mid_cache, leaf_cache)
    nodes = own_nodes(
        owner,
        [cache.shape[0] for cache in caches],
        (token_leaf, leaf_parent, mid_parent),
        (root_len, mid_len, leaf_len),
        (root_slot, mid_slot, leaf_slot),
    )
    kv_count = root_cache.shape[2] // (2 * HEAD)
    group_width = width // kv_count
    mlp_total = lax.axis_size("mlp")
    mlp_place = lax.axis_index("mlp").astype(jnp.int32)
    own_width = stream.shape[1]
    query_parts = gather_parts(queries, "kv")
    attended, blocks = [], None
    for k in range(kv_count):
        parts = tree_attention(query_parts, caches, nodes, owner, k)
        every = lax.all_to_all(parts, "kv", 0, 0)
        one, blocks = combine_project(
            every, out_weight, k * group_width, blocks, mlp_place, own_width
        )
        attended.append(one)
    projected = scatter_sum(dict(enumerate(blocks)), "mlp")
    residual = (stream.astype(jnp.float32) + projected).astype(jnp.bfloat16)
    steps = [1 << bit for bit in range(mlp_total.bit_length() - 1)]
    spot = jnp.int32(0)
    for step in steps:
        spot = 2 * spot + (mlp_place // step) % 2
    units = gate_weight.shape[1]
    row_parts = gather_parts(residual, "kv")
    chunks = [
        [mask for mask in range(len(row_parts)) if (mask // 2) % 2 == side] for side in range(2)
    ]
    mixed = 0.0
    for masks in chunks:
        keep, send = gate_up_rows(
            [row_parts[mask] for mask in masks],
            norm_gain,
            gate_weight,
            up_weight,
            spot,
            mlp_total,
        )
        for step in steps[:-1]:
            keep, send = add_halves(keep, swap(send, "mlp", step), units)
        pieces = [gated(keep, swap(send, "mlp", steps[-1]), units)]
        for step in reversed(steps):
            held = pieces[0] if len(pieces) == 1 else jnp.concatenate(pieces, axis=0)
            pieces.append(swap(held, "mlp", step))
        outs = down_rows(pieces, down_weight, spot, len(masks), own_rows, mlp_total)
        mixed = mixed + scatter_sum(dict(zip(masks, outs)), "kv")
    return (jnp.concatenate(attended, axis=1), mixed.astype(jnp.bfloat16))


def solution(mesh):
    in_specs = (
        P("kv", "mlp"),
        P("kv", None, "mlp"),
        P("kv", None, "mlp"),
        P("kv", None, "mlp"),
        P(),
        P(),
        P(),
        P(),
        P(),
        P(),
        P(),
        P(),
        P(),
        P("kv", "mlp"),
        P("mlp", None),
        P("mlp"),
        P("mlp", "kv"),
        P("mlp", "kv"),
        P("kv", "mlp"),
    )
    out_specs = (P("kv", "mlp"), P("kv", "mlp"))
    return jax.shard_map(shards, mesh=mesh, in_specs=in_specs, out_specs=out_specs, check_vma=False)
```

```python
import math

import jax
import jax.numpy as jnp
from jax import lax
from jax.experimental import pallas as pl
from jax.experimental.pallas import tpu as pltpu
from jax.sharding import PartitionSpec as P

D = 4096
HEAD = 128
QLEAF = 16
QMID = 48
QROOT = 144


LOWEST = -1e30
EPSILON = 1e-05
ALIGN = 16
BLOCK = 512
VMEM_BYTES = 50 << 20


def cost(flops, moved, exps):
    return pl.CostEstimate(flops=flops, bytes_accessed=moved, transcendentals=exps)


def streamed(pairs, sems):
    copies = [
        pltpu.make_async_copy(source, target, sems.at[k]) for k, (source, target) in enumerate(pairs)
    ]
    for copy in copies:
        copy.start()
    return copies


def own_nodes(owner, local_counts, tree, lengths, slots):
    token_leaf, leaf_parent, mid_parent = tree
    node_total = sum(local_counts)

    def kernel(owner_ref, token_ref, leaf_up, mid_up, *refs):
        len_refs, slot_refs, out_ref = refs[:3], refs[3:6], refs[6]

        def find(slot_ref, len_ref, local):
            base = owner_ref[0] * local

            def step(j, found):
                at, size = slot_ref[j] - base, len_ref[j]
                return tuple(
                    (jnp.where(at == k, j, node), jnp.where(at == k, size, length))
                    for k, (node, length) in enumerate(found)
                )

            zero = jnp.int32(0)
            return lax.fori_loop(0, slot_ref.shape[0], step, ((zero, zero),) * local)

        def below(parent_ref, edges):
            def step(j, counted):
                parent = parent_ref[j]
                return tuple(
                    c + jnp.where(parent < edge, 1, 0) for c, edge in zip(counted, edges)
                )

            return lax.fori_loop(0, parent_ref.shape[0], step, (jnp.int32(0),) * len(edges))

        picked = [find(*level) for level in zip(slot_refs, len_refs, local_counts)]
        edges = ()
        for level, parent_ref in enumerate((mid_up, leaf_up, None)):
            for node, _ in picked[level]:
                edges += (node, node + 1)
            if parent_ref is not None:
                edges = below(parent_ref, edges)
        tokens = token_ref[...]
        sizes = [length for level in picked for _, length in level]
        for k in range(node_total):
            for side in range(2):
                under = jnp.where(tokens < edges[2 * k + side], 1.0, 0.0)
                out_ref[side, k] = jnp.sum(under).astype(jnp.int32)
            out_ref[2, k] = sizes[k]

    smem = pl.BlockSpec(memory_space=pltpu.SMEM)
    vmem = pl.BlockSpec(memory_space=pltpu.VMEM)
    return pl.pallas_call(
        kernel,
        out_shape=jax.ShapeDtypeStruct((3, node_total), jnp.int32),
        in_specs=[smem, vmem] + [smem] * 8,
        out_specs=smem,
        name="own_nodes",
    )(owner[None], token_leaf.reshape(-1, HEAD), leaf_parent, mid_parent, *lengths, *slots)


def tree_attention(query_parts, caches, nodes, owner, kv_head):
    part_total = len(query_parts)
    own_rows = query_parts[0].shape[0]
    total_rows = part_total * own_rows
    width = query_parts[0].shape[1] // (caches[0].shape[2] // (2 * HEAD))
    group_size = width // HEAD
    score_scale = 1.0 / math.sqrt(HEAD)
    levels = []
    for cache, capacity in zip(caches, (QROOT, QMID, QLEAF)):
        levels.append((cache.shape[0], cache.shape[1], min(capacity + ALIGN, total_rows)))

    def kernel(nodes_ref, owner_ref, *refs):
        query_refs = refs[:part_total]
        cache_refs = refs[part_total : part_total + 3]
        out_ref, all_rows, run_out, run_lse, acc, peak, total, *rest = refs[part_total + 3 :]
        kept_refs, sems = rest[:3], rest[3]
        columns = pl.ds(kv_head * 2 * HEAD, 2 * HEAD)

        def copies(act):
            node, flag = 0, 0
            for (slot_total, span, _), cache_ref, kept_ref in zip(levels, cache_refs, kept_refs):
                block = min(BLOCK, span)
                for member in range(slot_total):
                    for index in range(span // block):
                        here = pl.ds(index * block, block)
                        copy = pltpu.make_async_copy(
                            cache_ref.at[member, here, columns],
                            kept_ref.at[member, here, :],
                            sems.at[flag + index],
                        )

                        @pl.when(index * block < nodes_ref[2, node])
                        def _(copy=copy):
                            act(copy)

                    node += 1
                    flag += span // block

        copies(lambda copy: copy.start())
        me = owner_ref[0]
        for part in range(part_total):
            row = pl.multiple_of((me ^ part) * own_rows, ALIGN)
            all_rows[pl.ds(row, own_rows), :] = query_refs[part][
                :, kv_head * width : (kv_head + 1) * width
            ]
        run_out[...] = jnp.zeros_like(run_out)
        run_lse[...] = jnp.full_like(run_lse, LOWEST)
        node, flag = 0, 0
        for (slot_total, span, rows), cache_ref, kept_ref in zip(levels, cache_refs, kept_refs):
            lanes = rows * group_size
            block = min(BLOCK, span)
            for member in range(slot_total):
                low, high, length = nodes_ref[0, node], nodes_ref[1, node], nodes_ref[2, node]
                node += 1
                window = jnp.minimum(low - lax.rem(low, ALIGN), total_rows - rows)
                window = pl.multiple_of(window, ALIGN)
                offsets = [h * HEAD for h in range(group_size)]
                first = flag
                flag += span // block
                grouped = jnp.concatenate(
                    [all_rows[pl.ds(window, rows), c : c + HEAD] for c in offsets], axis=0
                )
                acc[:, :lanes] = jnp.zeros((HEAD, lanes), jnp.float32)
                peak[:, :lanes] = jnp.full((1, lanes), LOWEST, jnp.float32)
                total[:, :lanes] = jnp.zeros((1, lanes), jnp.float32)

                def visit(index, carry, masked):
                    at = pl.multiple_of(index * block, block)
                    pltpu.make_async_copy(
                        cache_ref.at[member, pl.ds(at, block), columns],
                        kept_ref.at[member, pl.ds(at, block), :],
                        sems.at[first + index],
                    ).wait()
                    keys = kept_ref[member, pl.ds(at, block), :HEAD]
                    values = kept_ref[member, pl.ds(at, block), HEAD:]
                    scores = lax.dot_general(
                        keys,
                        grouped,
                        (((1,), (1,)), ((), ())),
                        preferred_element_type=jnp.float32,
                    )
                    if masked:
                        position = at + lax.broadcasted_iota(jnp.int32, (block, lanes), 0)
                        scores = jnp.where(position < length, scores, LOWEST)
                    old_peak = peak[:, :lanes]
                    new_peak = jnp.maximum(old_peak, jnp.max(scores, axis=0, keepdims=True))
                    weights = jnp.exp((scores - new_peak) * score_scale)
                    fade = jnp.exp((old_peak - new_peak) * score_scale)
                    peak[:, :lanes] = new_peak
                    total[:, :lanes] = total[:, :lanes] * fade + jnp.sum(
                        weights, axis=0, keepdims=True
                    )
                    acc[:, :lanes] = acc[:, :lanes] * fade + lax.dot_general(
                        values,
                        weights.astype(jnp.bfloat16),
                        (((0,), (0,)), ((), ())),
                        preferred_element_type=jnp.float32,
                    )
                    return carry

                whole = lax.div(length, block)
                lax.fori_loop(0, whole, lambda i, c: visit(i, c, False), 0)

                @pl.when(whole * block < length)
                def _():
                    visit(whole, 0, True)

                weight_sum = total[:, :lanes]
                part_out = (acc[:, :lanes] / weight_sum).T
                part_lse = jnp.broadcast_to(
                    peak[:, :lanes] * score_scale + jnp.log(weight_sum), (HEAD, lanes)
                ).T
                position = window + lax.broadcasted_iota(jnp.int32, (rows, HEAD), 0)
                live = (position >= low) & (position < high)
                for h, c in enumerate(offsets):
                    here = (pl.ds(window, rows), slice(c, c + HEAD))
                    old_lse, old_out = run_lse[here], run_out[here]
                    add_lse = part_lse[h * rows : (h + 1) * rows]
                    add_out = part_out[h * rows : (h + 1) * rows]
                    best = jnp.maximum(old_lse, add_lse)
                    old_share = jnp.exp(old_lse - best)
                    add_share = jnp.exp(add_lse - best)
                    share = old_share + add_share
                    run_out[here] = jnp.where(
                        live, (old_out * old_share + add_out * add_share) / share, old_out
                    )
                    run_lse[here] = jnp.where(live, best + jnp.log(share), old_lse)
        lane = lax.broadcasted_iota(jnp.int32, (own_rows, HEAD), 1)
        for part in range(part_total):
            at = part * own_rows
            out_ref[part, :, :width] = run_out[at : at + own_rows, :].astype(jnp.bfloat16)
            lse = jnp.zeros((own_rows, HEAD), jnp.float32)
            for h in range(group_size):
                piece = run_lse[at : at + own_rows, h * HEAD : (h + 1) * HEAD]
                lse = jnp.where(lax.rem(lane, group_size) == h, piece, lse)
            first = lse.astype(jnp.bfloat16)
            rest = lse - first.astype(jnp.float32)
            second = rest.astype(jnp.bfloat16)
            third = rest - second.astype(jnp.float32)
            field = lax.div(lane, group_size)
            packed = jnp.where(
                field == 0,
                first.astype(jnp.float32),
                jnp.where(
                    field == 1,
                    second.astype(jnp.float32),
                    jnp.where(field == 2, third, 0.0),
                ),
            )
            out_ref[part, :, width:] = packed.astype(jnp.bfloat16)

    block_total = sum(count * (span // min(BLOCK, span)) for count, span, _ in levels)
    most = max(rows for _, _, rows in levels) * group_size
    vmem = pl.BlockSpec(memory_space=pltpu.VMEM)
    smem = pl.BlockSpec(memory_space=pltpu.SMEM)
    return pl.pallas_call(
        kernel,
        out_shape=jax.ShapeDtypeStruct((part_total, own_rows, width + HEAD), jnp.bfloat16),
        in_specs=[smem, smem]
        + [vmem] * part_total
        + [pl.BlockSpec(memory_space=pltpu.HBM)] * 3,
        out_specs=vmem,
        scratch_shapes=[
            pltpu.VMEM((total_rows, width), jnp.bfloat16),
            pltpu.VMEM((total_rows, width), jnp.float32),
            pltpu.VMEM((total_rows, width), jnp.float32),
            pltpu.VMEM((HEAD, most), jnp.float32),
            pltpu.VMEM((1, most), jnp.float32),
            pltpu.VMEM((1, most), jnp.float32),
        ]
        + [pltpu.VMEM((count, span, 2 * HEAD), jnp.bfloat16) for count, span, _ in levels]
        + [pltpu.SemaphoreType.DMA((block_total,))],
        compiler_params=pltpu.CompilerParams(vmem_limit_bytes=VMEM_BYTES),
        cost_estimate=cost(
            4 * HEAD * group_size * sum(c * span * rows for c, span, rows in levels),
            2 * 2 * HEAD * sum(count * span for count, span, _ in levels),
            group_size * sum(c * span * rows for c, span, rows in levels),
        ),
        name="tree_attention",
    )(nodes, owner[None], *query_parts, *caches)


def combine_project(every, weight, row_start, added, place, own_width):
    part_total, own_rows, wide = every.shape
    width = wide - HEAD
    group_size = width // HEAD
    block_total = weight.shape[1] // own_width
    last = added is not None or width == weight.shape[0]
    kind = jnp.bfloat16 if last else jnp.float32

    def kernel(place_ref, every_ref, weight_ref, *refs):
        added_refs = refs[:block_total] if added is not None else (None,) * block_total
        attended_ref, *block_refs = refs[len(refs) - 3 - block_total : -2]
        kept, sems = refs[-2:]
        columns = [
            pl.ds(pl.multiple_of((place_ref[0] ^ block) * own_width, HEAD), own_width)
            for block in range(block_total)
        ]
        copies = streamed(
            [
                (weight_ref.at[pl.ds(row_start, width), column], kept.at[block])
                for block, column in enumerate(columns)
            ],
            sems,
        )
        lse = []
        for part in range(part_total):
            terms = every_ref[part, :, width:].astype(jnp.float32)
            lse.append(
                terms
                + pltpu.roll(terms, HEAD - group_size, 1)
                + pltpu.roll(terms, HEAD - 2 * group_size, 1)
            )
        best = lse[0]
        for one in lse[1:]:
            best = jnp.maximum(best, one)
        share = [jnp.exp(one - best) for one in lse]
        whole = share[0]
        for one in share[1:]:
            whole = whole + one
        for h in range(group_size):
            summed = jnp.zeros((own_rows, HEAD), jnp.float32)
            for part in range(part_total):
                summed = summed + (
                    every_ref[part, :, h * HEAD : (h + 1) * HEAD].astype(jnp.float32)
                    * share[part][:, h : h + 1]
                )
            attended_ref[:, h * HEAD : (h + 1) * HEAD] = (summed / whole[:, h : h + 1]).astype(
                jnp.bfloat16
            )
        for block in range(block_total):
            copies[block].wait()
            product = jnp.dot(
                attended_ref[...], kept[block], preferred_element_type=jnp.float32
            )
            if added is not None:
                product = product + added_refs[block][...]
            block_refs[block][...] = product.astype(kind)

    vmem = pl.BlockSpec(memory_space=pltpu.VMEM)
    outs = pl.pallas_call(
        kernel,
        out_shape=[jax.ShapeDtypeStruct((own_rows, width), jnp.bfloat16)]
        + [jax.ShapeDtypeStruct((own_rows, own_width), kind)] * block_total,
        in_specs=[pl.BlockSpec(memory_space=pltpu.SMEM), vmem]
        + [pl.BlockSpec(memory_space=pltpu.HBM)]
        + [vmem] * (block_total if added is not None else 0),
        out_specs=[vmem] * (1 + block_total),
        scratch_shapes=[
            pltpu.VMEM((block_total, width, own_width), jnp.bfloat16),
            pltpu.SemaphoreType.DMA((block_total,)),
        ],
        compiler_params=pltpu.CompilerParams(vmem_limit_bytes=VMEM_BYTES),
        cost_estimate=cost(
            2 * own_rows * width * weight.shape[1],
            2 * width * weight.shape[1],
            part_total * own_rows * HEAD,
        ),
        name="combine_project",
    )(place[None], every, weight, *(added or ()))
    return outs[0], outs[1:]


def split_terms(value):
    first = value.astype(jnp.bfloat16).astype(jnp.float32)
    second = (value - first).astype(jnp.bfloat16).astype(jnp.float32)
    lane = lax.broadcasted_iota(jnp.int32, value.shape, 1)
    third = jnp.where(lane == 2, value - first - second, 0.0)
    return jnp.where(lane == 0, first, jnp.where(lane == 1, second, third)).astype(jnp.bfloat16)


def gate_up_rows(parts, norm_gain, gate_weight, up_weight, spot, group_total):
    own_rows, features = parts[0].shape
    rows = own_rows * len(parts)
    half = rows // 2
    piece = half // 2
    each = len(parts) // group_total
    units = gate_weight.shape[1]
    tile = units // 2 if (units // 2) % HEAD == 0 else units

    def kernel(spot_ref, gain_ref, gate_ref, up_ref, *refs):
        part_refs = refs[: len(parts)]
        keep_ref, *send_refs, scaled, squares, kept_gate, kept_up, sems = refs[len(parts) :]
        tiles = [
            (ref, kept, base, at)
            for ref, kept, base in ((gate_ref, kept_gate, 0), (up_ref, kept_up, units))
            for at in range(0, units, tile)
        ]
        copies = streamed(
            [
                (ref, kept)
                if tile == units
                else (ref.at[:, pl.ds(at, tile)], kept.at[:, pl.ds(at, tile)])
                for ref, kept, _, at in tiles
            ],
            sems,
        )
        for index, part_ref in enumerate(part_refs):
            at = ((index // each) ^ spot_ref[0]) * each + index % each
            here = pl.ds(pl.multiple_of(at * own_rows, ALIGN), own_rows)
            wide = part_ref[...].astype(jnp.float32)
            scaled[here, :] = (wide * gain_ref[...]).astype(jnp.bfloat16)
            squares[here, :] = jnp.broadcast_to(
                jnp.sum(wide * wide, axis=1, keepdims=True), (own_rows, HEAD)
            )
        for copy, (_, kept, base, at) in zip(copies, tiles):
            copy.wait()
            here = slice(base + at, base + at + tile)
            product = jnp.dot(
                scaled[...], kept[:, at : at + tile], preferred_element_type=jnp.float32
            ).astype(jnp.bfloat16)
            keep_ref[:, here] = product[:half]
            for k, send_ref in enumerate(send_refs):
                send_ref[:, here] = product[half + k * piece : half + (k + 1) * piece]
        terms = split_terms(squares[...])
        keep_ref[:, 2 * units :] = terms[:half]
        for k, send_ref in enumerate(send_refs):
            send_ref[:, 2 * units :] = terms[half + k * piece : half + (k + 1) * piece]

    vmem = pl.BlockSpec(memory_space=pltpu.VMEM)
    keep, *send = pl.pallas_call(
        kernel,
        out_shape=[jax.ShapeDtypeStruct((half, 2 * units + HEAD), jnp.bfloat16)]
        + [jax.ShapeDtypeStruct((piece, 2 * units + HEAD), jnp.bfloat16)] * 2,
        in_specs=[pl.BlockSpec(memory_space=pltpu.SMEM), vmem]
        + [pl.BlockSpec(memory_space=pltpu.HBM)] * 2
        + [vmem] * len(parts),
        out_specs=[vmem] * 3,
        scratch_shapes=[
            pltpu.VMEM((rows, features), jnp.bfloat16),
            pltpu.VMEM((rows, HEAD), jnp.float32),
            pltpu.VMEM((features, units), jnp.bfloat16),
            pltpu.VMEM((features, units), jnp.bfloat16),
            pltpu.SemaphoreType.DMA((2 * units // tile,)),
        ],
        compiler_params=pltpu.CompilerParams(vmem_limit_bytes=VMEM_BYTES),
        cost_estimate=cost(4 * rows * features * units, 4 * features * units, 0),
        name="gate_up",
    )(spot[None], norm_gain[None, :], gate_weight, up_weight, *parts)
    return keep, send


def add_halves(keep, got, units):
    half = keep.shape[0] // 2

    def kernel(keep_ref, low_ref, high_ref, next_ref, send_ref):
        for ref, got_ref, at in ((next_ref, low_ref, 0), (send_ref, high_ref, half)):
            here = pl.ds(at, half)
            ref[:, : 2 * units] = (
                keep_ref[here, : 2 * units].astype(jnp.float32)
                + got_ref[:, : 2 * units].astype(jnp.float32)
            ).astype(jnp.bfloat16)
            terms = keep_ref[here, 2 * units :].astype(jnp.float32)
            terms = terms + got_ref[:, 2 * units :].astype(jnp.float32)
            total = jnp.sum(terms, axis=1, keepdims=True)
            ref[:, 2 * units :] = split_terms(jnp.broadcast_to(total, (half, HEAD)))

    vmem = pl.BlockSpec(memory_space=pltpu.VMEM)
    return pl.pallas_call(
        kernel,
        out_shape=[jax.ShapeDtypeStruct((half, keep.shape[1]), jnp.bfloat16)] * 2,
        in_specs=[vmem] * 3,
        out_specs=[vmem, vmem],
        compiler_params=pltpu.CompilerParams(vmem_limit_bytes=VMEM_BYTES),
        cost_estimate=cost(2 * keep.size, 6 * keep.size, 0),
        name="add_halves",
    )(keep, *got)


def gated(keep, got, units):
    def kernel(keep_ref, got_ref, out_ref):
        summed = keep_ref[...].astype(jnp.float32) + got_ref[...].astype(jnp.float32)
        square = jnp.sum(summed[:, 2 * units :], axis=1, keepdims=True)
        scale = lax.rsqrt(square / D + EPSILON)
        gate = summed[:, :units] * scale
        up = summed[:, units : 2 * units] * scale
        out_ref[...] = (gate / (1.0 + jnp.exp(-gate)) * up).astype(jnp.bfloat16)

    vmem = pl.BlockSpec(memory_space=pltpu.VMEM)
    return pl.pallas_call(
        kernel,
        out_shape=jax.ShapeDtypeStruct((keep.shape[0], units), jnp.bfloat16),
        in_specs=[vmem, vmem],
        out_specs=vmem,
        compiler_params=pltpu.CompilerParams(vmem_limit_bytes=VMEM_BYTES),
        cost_estimate=cost(4 * keep.size, 5 * keep.size, keep.size // 2),
        name="gated",
    )(keep, got)


def down_rows(pieces, down_weight, spot, part_count, own_rows, group_total):
    rows = part_count * own_rows
    each = part_count // group_total
    units, features = down_weight.shape

    def kernel(spot_ref, weight_ref, *refs):
        piece_refs = refs[: len(pieces)]
        out_refs = refs[len(pieces) : len(pieces) + part_count]
        hidden, product = refs[len(pieces) + part_count :]
        at = 0
        for piece_ref in piece_refs:
            hidden[at : at + piece_ref.shape[0], :] = piece_ref[...]
            at += piece_ref.shape[0]
        product[...] = jnp.dot(
            hidden[...], weight_ref[...], preferred_element_type=jnp.float32
        )
        for index, out_ref in enumerate(out_refs):
            at = ((index // each) ^ spot_ref[0]) * each + index % each
            here = pl.ds(pl.multiple_of(at * own_rows, ALIGN), own_rows)
            out_ref[...] = product[here, :].astype(jnp.bfloat16)

    vmem = pl.BlockSpec(memory_space=pltpu.VMEM)
    return pl.pallas_call(
        kernel,
        out_shape=[jax.ShapeDtypeStruct((own_rows, features), jnp.bfloat16)] * part_count,
        in_specs=[pl.BlockSpec(memory_space=pltpu.SMEM)] + [vmem] * (1 + len(pieces)),
        out_specs=[vmem] * part_count,
        scratch_shapes=[
            pltpu.VMEM((rows, units), jnp.bfloat16),
            pltpu.VMEM((rows, features), jnp.float32),
        ],
        compiler_params=pltpu.CompilerParams(vmem_limit_bytes=VMEM_BYTES),
        cost_estimate=cost(2 * rows * features * units, 2 * features * units, 0),
        name="down",
    )(spot[None], down_weight, *pieces)


def swap(value, axis_name, mask):
    axis_total = lax.axis_size(axis_name)
    return lax.ppermute(value, axis_name, [(j, j ^ mask) for j in range(axis_total)])


def after(value, token):
    return lax.optimization_barrier((value, token))[0]


def gather_parts(value, axis_name, token=None):
    parts = [value] * lax.axis_size(axis_name)
    for mask in range(len(parts) - 2, 0, -2):
        parts[mask] = swap(value, axis_name, mask)
    for mask in [0] + list(range(len(parts) - 2, 0, -2)):
        held = parts[mask] if token is None or mask == 0 else after(parts[mask], token)
        parts[mask + 1] = swap(held, axis_name, 1)
    return parts


def scatter_sum(parts, axis_name):
    wide = jnp.float32
    evens = sorted((mask for mask in parts if mask % 2 == 0), reverse=True)
    got = {mask: swap(parts[mask + 1], axis_name, 1) for mask in evens}
    summed = 0.0
    for mask in evens:
        pair = parts[mask].astype(wide) + got[mask].astype(wide)
        if mask:
            pair = swap(pair.astype(jnp.bfloat16), axis_name, mask).astype(wide)
        summed = summed + pair
    return summed


def shards(
    queries,
    root_cache,
    mid_cache,
    leaf_cache,
    token_leaf,
    leaf_parent,
    mid_parent,
    root_len,
    mid_len,
    leaf_len,
    root_slot,
    mid_slot,
    leaf_slot,
    stream,
    out_weight,
    norm_gain,
    gate_weight,
    up_weight,
    down_weight,
):
    own_rows, width = queries.shape
    owner = lax.axis_index("kv").astype(jnp.int32)
    caches = (root_cache, mid_cache, leaf_cache)
    nodes = own_nodes(
        owner,
        [cache.shape[0] for cache in caches],
        (token_leaf, leaf_parent, mid_parent),
        (root_len, mid_len, leaf_len),
        (root_slot, mid_slot, leaf_slot),
    )
    kv_count = root_cache.shape[2] // (2 * HEAD)
    group_width = width // kv_count
    mlp_total = lax.axis_size("mlp")
    mlp_place = lax.axis_index("mlp").astype(jnp.int32)
    own_width = stream.shape[1]
    query_parts = gather_parts(queries, "kv", nodes)
    attended, blocks = [], None
    for k in range(kv_count):
        parts = tree_attention(query_parts, caches, nodes, owner, k)
        every = lax.all_to_all(parts, "kv", 0, 0)
        one, blocks = combine_project(
            every, out_weight, k * group_width, blocks, mlp_place, own_width
        )
        attended.append(one)
    projected = scatter_sum(dict(enumerate(blocks)), "mlp")
    residual = (stream.astype(jnp.float32) + projected).astype(jnp.bfloat16)
    steps = [1 << bit for bit in range(mlp_total.bit_length() - 1)]
    spot = jnp.int32(0)
    for step in steps:
        spot = 2 * spot + (mlp_place // step) % 2
    units = gate_weight.shape[1]
    row_parts = gather_parts(residual, "kv")
    first, second = (
        [mask for mask in range(len(row_parts)) if (mask // 2) % 2 == side] for side in range(2)
    )
    row_parts[0] = after(row_parts[0], [row_parts[mask] for mask in second if mask % 2 == 0])

    def multiply(masks):
        parts = [row_parts[mask] for mask in masks]
        return gate_up_rows(parts, norm_gain, gate_weight, up_weight, spot, mlp_total)

    def reduce_once(keep, send, token=None):
        for step in steps[:-1]:
            if step > 1:
                send = jnp.split(send, 2, axis=0)
            got = [swap(piece, "mlp", step) for piece in send]
            if token is not None and step == 1:
                keep = after(keep, token)
            keep, send = add_halves(keep, got, units)
        return keep, send

    def regather(hidden):
        pieces = [hidden]
        for step in reversed(steps):
            held = pieces[0] if len(pieces) == 1 else jnp.concatenate(pieces, axis=0)
            pieces.append(swap(held, "mlp", step))
        return pieces

    def finish(pieces, masks):
        outs = down_rows(pieces, down_weight, spot, len(masks), own_rows, mlp_total)
        return outs, scatter_sum(dict(zip(masks, outs)), "kv")

    keep, send = reduce_once(*multiply(first))
    row_parts[second[0]] = after(row_parts[second[0]], send)
    later = multiply(second)
    hidden = gated(after(keep, later[0]), swap(send, "mlp", steps[-1]), units)
    keep, send = reduce_once(*later, hidden)
    outs, mixed = finish(regather(hidden), first)
    hidden = gated(after(keep, outs[0]), swap(send, "mlp", steps[-1]), units)
    pieces = regather(hidden)
    pieces[0] = after(pieces[0], mixed)
    mixed = mixed + finish(pieces, second)[1]
    return (jnp.concatenate(attended, axis=1), mixed.astype(jnp.bfloat16))


def solution(mesh):
    in_specs = (
        P("kv", "mlp"),
        P("kv", None, "mlp"),
        P("kv", None, "mlp"),
        P("kv", None, "mlp"),
        P(),
        P(),
        P(),
        P(),
        P(),
        P(),
        P(),
        P(),
        P(),
        P("kv", "mlp"),
        P("mlp", None),
        P("mlp"),
        P("mlp", "kv"),
        P("mlp", "kv"),
        P("kv", "mlp"),
    )
    out_specs = (P("kv", "mlp"), P("kv", "mlp"))
    return jax.shard_map(shards, mesh=mesh, in_specs=in_specs, out_specs=out_specs, check_vma=False)
```

```python
import math

import jax
import jax.numpy as jnp
from jax import lax
from jax.experimental import pallas as pl
from jax.experimental.pallas import tpu as pltpu
from jax.sharding import PartitionSpec as P

D = 4096
HEAD = 128
QLEAF = 16
QMID = 48
QROOT = 144


LOWEST = -1e30
EPSILON = 1e-05
ALIGN = 16
BLOCK = 512
VMEM_BYTES = 50 << 20
SMALL_BYTES = 24 << 20


def cost(flops, moved, exps):
    return pl.CostEstimate(flops=flops, bytes_accessed=moved, transcendentals=exps)


def streamed(pairs, sems):
    copies = [
        pltpu.make_async_copy(source, target, sems.at[k]) for k, (source, target) in enumerate(pairs)
    ]
    for copy in copies:
        copy.start()
    return copies


def own_nodes(owner, local_counts, tree, lengths, slots):
    token_leaf, leaf_parent, mid_parent = tree
    node_total = sum(local_counts)

    def kernel(owner_ref, token_ref, leaf_up, mid_up, *refs):
        len_refs, slot_refs, out_ref = refs[:3], refs[3:6], refs[6]

        def find(slot_ref, len_ref, local):
            base = owner_ref[0] * local

            def step(j, found):
                at, size = slot_ref[j] - base, len_ref[j]
                return tuple(
                    (jnp.where(at == k, j, node), jnp.where(at == k, size, length))
                    for k, (node, length) in enumerate(found)
                )

            zero = jnp.int32(0)
            return lax.fori_loop(0, slot_ref.shape[0], step, ((zero, zero),) * local)

        def below(parent_ref, edges):
            def step(j, counted):
                parent = parent_ref[j]
                return tuple(
                    c + jnp.where(parent < edge, 1, 0) for c, edge in zip(counted, edges)
                )

            return lax.fori_loop(0, parent_ref.shape[0], step, (jnp.int32(0),) * len(edges))

        picked = [find(*level) for level in zip(slot_refs, len_refs, local_counts)]
        edges = ()
        for level, parent_ref in enumerate((mid_up, leaf_up, None)):
            for node, _ in picked[level]:
                edges += (node, node + 1)
            if parent_ref is not None:
                edges = below(parent_ref, edges)
        tokens = token_ref[...]
        sizes = [length for level in picked for _, length in level]
        for k in range(node_total):
            for side in range(2):
                under = jnp.where(tokens < edges[2 * k + side], 1.0, 0.0)
                out_ref[side, k] = jnp.sum(under).astype(jnp.int32)
            out_ref[2, k] = sizes[k]

    smem = pl.BlockSpec(memory_space=pltpu.SMEM)
    vmem = pl.BlockSpec(memory_space=pltpu.VMEM)
    return pl.pallas_call(
        kernel,
        out_shape=jax.ShapeDtypeStruct((3, node_total), jnp.int32),
        in_specs=[smem, vmem] + [smem] * 8,
        out_specs=smem,
        name="own_nodes",
    )(owner[None], token_leaf.reshape(-1, HEAD), leaf_parent, mid_parent, *lengths, *slots)


def tree_attention(query_parts, caches, nodes, owner, kv_head):
    part_total = len(query_parts)
    own_rows = query_parts[0].shape[0]
    total_rows = part_total * own_rows
    width = query_parts[0].shape[1] // (caches[0].shape[2] // (2 * HEAD))
    group_size = width // HEAD
    score_scale = 1.0 / math.sqrt(HEAD)
    levels = []
    for cache, capacity in zip(caches, (QROOT, QMID, QLEAF)):
        levels.append((cache.shape[0], cache.shape[1], min(capacity + ALIGN, total_rows)))

    def kernel(nodes_ref, owner_ref, *refs):
        query_refs = refs[:part_total]
        cache_refs = refs[part_total : part_total + 3]
        out_ref, all_rows, run_out, run_lse, acc, peak, total, *rest = refs[part_total + 3 :]
        kept_refs, sems = rest[:3], rest[3]
        columns = pl.ds(kv_head * 2 * HEAD, 2 * HEAD)
        starts = [0, levels[0][0], levels[0][0] + levels[1][0]]
        lengths, flag_starts, flag = [], [], 0
        for start, (slot_total, span, _) in zip(starts, levels):
            lengths.append([nodes_ref[2, start + member] for member in range(slot_total)])
            flag_starts.append(flag)
            flag += slot_total * (span // min(BLOCK, span))

        def block_copy(level, member, index):
            span = levels[level][1]
            block = min(BLOCK, span)
            at = index * block
            here = pl.ds(at if isinstance(at, int) else pl.multiple_of(at, block), block)
            return pltpu.make_async_copy(
                cache_refs[level].at[member, here, columns],
                kept_refs[level].at[member, here, :],
                sems.at[flag_starts[level] + member * (span // block) + index],
            )

        steps = []
        for level, (slot_total, span, _) in enumerate(levels):
            block = min(BLOCK, span)
            pair = min(2 * block, span)
            longest = lengths[level][0]
            shortest = lengths[level][0]
            for length in lengths[level][1:]:
                longest, shortest = jnp.maximum(longest, length), jnp.minimum(shortest, length)
            whole, most = lax.div(shortest, pair), lax.div(longest + pair - 1, pair)
            steps.append((block, pair, whole, most))
            for index in range(span // pair):

                @pl.when(index < most)
                def _(level=level, index=index, ratio=pair // block, slot_total=slot_total):
                    for piece in range(ratio):
                        for member in range(slot_total):
                            block_copy(level, member, index * ratio + piece).start()

        me = owner_ref[0]
        for part in range(part_total):
            row = pl.multiple_of((me ^ part) * own_rows, ALIGN)
            all_rows[pl.ds(row, own_rows), :] = query_refs[part][
                :, kv_head * width : (kv_head + 1) * width
            ]
        run_out[...] = jnp.zeros_like(run_out)
        run_lse[...] = jnp.full_like(run_lse, LOWEST)
        offsets = [h * HEAD for h in range(group_size)]
        for level, (slot_total, span, rows) in enumerate(levels):
            block, pair, whole, most = steps[level]
            lanes = rows * group_size
            every = lanes * slot_total
            windows, grouped = [], []
            for member in range(slot_total):
                low = nodes_ref[0, starts[level] + member]
                window = jnp.minimum(low - lax.rem(low, ALIGN), total_rows - rows)
                window = pl.multiple_of(window, ALIGN)
                windows.append(window)
                grouped.append(
                    jnp.concatenate(
                        [all_rows[pl.ds(window, rows), c : c + HEAD] for c in offsets], axis=0
                    )
                )
            lane_of = lax.broadcasted_iota(jnp.int32, (1, every), 1)
            limits = jnp.full((1, every), lengths[level][0], jnp.int32)
            for member in range(1, slot_total):
                limits = jnp.where(lane_of >= member * lanes, lengths[level][member], limits)
            acc[:, :every] = jnp.zeros((HEAD, every), jnp.float32)
            peak[:, :every] = jnp.full((1, every), LOWEST, jnp.float32)
            total[:, :every] = jnp.zeros((1, every), jnp.float32)

            def visit(index, carry, masked):
                ratio = pair // block
                for piece in range(ratio):
                    for member in range(slot_total):
                        block_copy(level, member, index * ratio + piece).wait()
                scores = []
                for piece in range(ratio):
                    at = pl.multiple_of((index * ratio + piece) * block, block)
                    found = [
                        lax.dot_general(
                            kept_refs[level][member, pl.ds(at, block), :HEAD],
                            grouped[member],
                            (((1,), (1,)), ((), ())),
                            preferred_element_type=jnp.float32,
                        )
                        for member in range(slot_total)
                    ]
                    found = found[0] if slot_total == 1 else jnp.concatenate(found, axis=1)
                    if masked:
                        position = lax.broadcasted_iota(jnp.int32, (block, every), 0)
                        found = jnp.where(position < limits - at, found, LOWEST)
                    scores.append((at, found))
                for at, found in scores:
                    old_peak = peak[:, :every]
                    new_peak = jnp.maximum(old_peak, jnp.max(found, axis=0, keepdims=True))
                    weights = jnp.exp((found - new_peak) * score_scale)
                    if masked:
                        position = lax.broadcasted_iota(jnp.int32, (block, every), 0)
                        weights = jnp.where(position < limits - at, weights, 0.0)
                    fade = jnp.exp((old_peak - new_peak) * score_scale)
                    peak[:, :every] = new_peak
                    total[:, :every] = total[:, :every] * fade + jnp.sum(
                        weights, axis=0, keepdims=True
                    )
                    rounded = weights.astype(jnp.bfloat16)
                    for member in range(slot_total):
                        here = slice(member * lanes, (member + 1) * lanes)
                        acc[:, here] = acc[:, here] * fade[:, here] + lax.dot_general(
                            kept_refs[level][member, pl.ds(at, block), HEAD:],
                            rounded[:, here],
                            (((0,), (0,)), ((), ())),
                            preferred_element_type=jnp.float32,
                        )
                return carry

            lax.fori_loop(0, whole, lambda i, c: visit(i, c, False), 0)
            lax.fori_loop(whole, most, lambda i, c: visit(i, c, True), 0)

            weight_sum = total[:, :every]
            part_out = (acc[:, :every] / weight_sum).T
            part_lse = jnp.broadcast_to(
                peak[:, :every] * score_scale + jnp.log(weight_sum), (HEAD, every)
            ).T
            for member, window in enumerate(windows):
                low = nodes_ref[0, starts[level] + member]
                high = nodes_ref[1, starts[level] + member]
                position = window + lax.broadcasted_iota(jnp.int32, (rows, HEAD), 0)
                live = (position >= low) & (position < high)
                for h, c in enumerate(offsets):
                    here = (pl.ds(window, rows), slice(c, c + HEAD))
                    old_lse, old_out = run_lse[here], run_out[here]
                    at = member * lanes + h * rows
                    add_lse = part_lse[at : at + rows]
                    add_out = part_out[at : at + rows]
                    if level == 0:
                        run_out[here] = jnp.where(live, add_out, old_out)
                        run_lse[here] = jnp.where(live, add_lse, old_lse)
                        continue
                    best = jnp.maximum(old_lse, add_lse)
                    old_share = jnp.exp(old_lse - best)
                    add_share = jnp.exp(add_lse - best)
                    share = old_share + add_share
                    run_out[here] = jnp.where(
                        live, (old_out * old_share + add_out * add_share) / share, old_out
                    )
                    run_lse[here] = jnp.where(live, best + jnp.log(share), old_lse)
        lane = lax.broadcasted_iota(jnp.int32, (own_rows, HEAD), 1)
        for part in range(part_total):
            at = part * own_rows
            out_ref[part, :, :width] = run_out[at : at + own_rows, :].astype(jnp.bfloat16)
            lse = jnp.zeros((own_rows, HEAD), jnp.float32)
            for h in range(group_size):
                piece = run_lse[at : at + own_rows, h * HEAD : (h + 1) * HEAD]
                lse = jnp.where(lax.rem(lane, group_size) == h, piece, lse)
            first = lse.astype(jnp.bfloat16)
            rest = lse - first.astype(jnp.float32)
            second = rest.astype(jnp.bfloat16)
            third = rest - second.astype(jnp.float32)
            field = lax.div(lane, group_size)
            packed = jnp.where(
                field == 0,
                first.astype(jnp.float32),
                jnp.where(
                    field == 1,
                    second.astype(jnp.float32),
                    jnp.where(field == 2, third, 0.0),
                ),
            )
            out_ref[part, :, width:] = packed.astype(jnp.bfloat16)

    block_total = sum(count * (span // min(BLOCK, span)) for count, span, _ in levels)
    most = max(count * rows for count, _, rows in levels) * group_size
    vmem = pl.BlockSpec(memory_space=pltpu.VMEM)
    smem = pl.BlockSpec(memory_space=pltpu.SMEM)
    return pl.pallas_call(
        kernel,
        out_shape=jax.ShapeDtypeStruct((part_total, own_rows, width + HEAD), jnp.bfloat16),
        in_specs=[smem, smem]
        + [vmem] * part_total
        + [pl.BlockSpec(memory_space=pltpu.HBM)] * 3,
        out_specs=vmem,
        scratch_shapes=[
            pltpu.VMEM((total_rows, width), jnp.bfloat16),
            pltpu.VMEM((total_rows, width), jnp.float32),
            pltpu.VMEM((total_rows, width), jnp.float32),
            pltpu.VMEM((HEAD, most), jnp.float32),
            pltpu.VMEM((1, most), jnp.float32),
            pltpu.VMEM((1, most), jnp.float32),
        ]
        + [pltpu.VMEM((count, span, 2 * HEAD), jnp.bfloat16) for count, span, _ in levels]
        + [pltpu.SemaphoreType.DMA((block_total,))],
        compiler_params=pltpu.CompilerParams(vmem_limit_bytes=VMEM_BYTES),
        cost_estimate=cost(
            4 * HEAD * group_size * sum(c * span * rows for c, span, rows in levels),
            2 * 2 * HEAD * sum(count * span for count, span, _ in levels),
            group_size * sum(c * span * rows for c, span, rows in levels),
        ),
        name="tree_attention",
    )(nodes, owner[None], *query_parts, *caches)


def combine_project(every, weight, row_start, added, place, own_width):
    part_total, own_rows, wide = every.shape
    width = wide - HEAD
    group_size = width // HEAD
    block_total = weight.shape[1] // own_width
    last = added is not None or width == weight.shape[0]
    kind = jnp.bfloat16 if last else jnp.float32

    def kernel(place_ref, every_ref, weight_ref, *refs):
        added_refs = refs[:block_total] if added is not None else (None,) * block_total
        attended_ref, *block_refs = refs[len(refs) - 3 - block_total : -2]
        kept, sems = refs[-2:]
        columns = [
            pl.ds(pl.multiple_of((place_ref[0] ^ block) * own_width, HEAD), own_width)
            for block in range(block_total)
        ]
        copies = streamed(
            [
                (weight_ref.at[pl.ds(row_start, width), column], kept.at[block])
                for block, column in enumerate(columns)
            ],
            sems,
        )
        lse = []
        for part in range(part_total):
            terms = every_ref[part, :, width:].astype(jnp.float32)
            lse.append(
                terms
                + pltpu.roll(terms, HEAD - group_size, 1)
                + pltpu.roll(terms, HEAD - 2 * group_size, 1)
            )
        best = lse[0]
        for one in lse[1:]:
            best = jnp.maximum(best, one)
        share = [jnp.exp(one - best) for one in lse]
        whole = share[0]
        for one in share[1:]:
            whole = whole + one
        for h in range(group_size):
            summed = jnp.zeros((own_rows, HEAD), jnp.float32)
            for part in range(part_total):
                summed = summed + (
                    every_ref[part, :, h * HEAD : (h + 1) * HEAD].astype(jnp.float32)
                    * share[part][:, h : h + 1]
                )
            attended_ref[:, h * HEAD : (h + 1) * HEAD] = (summed / whole[:, h : h + 1]).astype(
                jnp.bfloat16
            )
        for block in range(block_total):
            copies[block].wait()
            product = jnp.dot(
                attended_ref[...], kept[block], preferred_element_type=jnp.float32
            )
            if added is not None:
                product = product + added_refs[block][...]
            block_refs[block][...] = product.astype(kind)

    vmem = pl.BlockSpec(memory_space=pltpu.VMEM)
    outs = pl.pallas_call(
        kernel,
        out_shape=[jax.ShapeDtypeStruct((own_rows, width), jnp.bfloat16)]
        + [jax.ShapeDtypeStruct((own_rows, own_width), kind)] * block_total,
        in_specs=[pl.BlockSpec(memory_space=pltpu.SMEM), vmem]
        + [pl.BlockSpec(memory_space=pltpu.HBM)]
        + [vmem] * (block_total if added is not None else 0),
        out_specs=[vmem] * (1 + block_total),
        scratch_shapes=[
            pltpu.VMEM((block_total, width, own_width), jnp.bfloat16),
            pltpu.SemaphoreType.DMA((block_total,)),
        ],
        compiler_params=pltpu.CompilerParams(vmem_limit_bytes=VMEM_BYTES),
        cost_estimate=cost(
            2 * own_rows * width * weight.shape[1],
            2 * width * weight.shape[1],
            part_total * own_rows * HEAD,
        ),
        name="combine_project",
    )(place[None], every, weight, *(added or ()))
    return outs[0], outs[1:]


def split_terms(value):
    first = value.astype(jnp.bfloat16).astype(jnp.float32)
    second = (value - first).astype(jnp.bfloat16).astype(jnp.float32)
    lane = lax.broadcasted_iota(jnp.int32, value.shape, 1)
    third = jnp.where(lane == 2, value - first - second, 0.0)
    return jnp.where(lane == 0, first, jnp.where(lane == 1, second, third)).astype(jnp.bfloat16)


def gate_up_rows(parts, norm_gain, gate_weight, up_weight, spot, group_total):
    own_rows, features = parts[0].shape
    rows = own_rows * len(parts)
    half = rows // 2
    piece = half // 2
    each = len(parts) // group_total
    units = gate_weight.shape[1]
    tile = units // 2 if (units // 2) % HEAD == 0 else units

    def kernel(spot_ref, gain_ref, gate_ref, up_ref, *refs):
        part_refs = refs[: len(parts)]
        keep_ref, *send_refs, scaled, squares, kept_gate, kept_up, sems = refs[len(parts) :]
        tiles = [
            (ref, kept, base, at)
            for ref, kept, base in ((gate_ref, kept_gate, 0), (up_ref, kept_up, units))
            for at in range(0, units, tile)
        ]
        copies = streamed(
            [
                (ref, kept)
                if tile == units
                else (ref.at[:, pl.ds(at, tile)], kept.at[:, pl.ds(at, tile)])
                for ref, kept, _, at in tiles
            ],
            sems,
        )
        for index, part_ref in enumerate(part_refs):
            at = ((index // each) ^ spot_ref[0]) * each + index % each
            here = pl.ds(pl.multiple_of(at * own_rows, ALIGN), own_rows)
            wide = part_ref[...].astype(jnp.float32)
            scaled[here, :] = (wide * gain_ref[...]).astype(jnp.bfloat16)
            squares[here, :] = jnp.broadcast_to(
                jnp.sum(wide * wide, axis=1, keepdims=True), (own_rows, HEAD)
            )
        for copy, (_, kept, base, at) in zip(copies, tiles):
            copy.wait()
            here = slice(base + at, base + at + tile)
            product = jnp.dot(
                scaled[...], kept[:, at : at + tile], preferred_element_type=jnp.float32
            ).astype(jnp.bfloat16)
            keep_ref[:, here] = product[:half]
            for k, send_ref in enumerate(send_refs):
                send_ref[:, here] = product[half + k * piece : half + (k + 1) * piece]
        terms = split_terms(squares[...])
        keep_ref[:, 2 * units :] = terms[:half]
        for k, send_ref in enumerate(send_refs):
            send_ref[:, 2 * units :] = terms[half + k * piece : half + (k + 1) * piece]

    vmem = pl.BlockSpec(memory_space=pltpu.VMEM)
    keep, *send = pl.pallas_call(
        kernel,
        out_shape=[jax.ShapeDtypeStruct((half, 2 * units + HEAD), jnp.bfloat16)]
        + [jax.ShapeDtypeStruct((piece, 2 * units + HEAD), jnp.bfloat16)] * 2,
        in_specs=[pl.BlockSpec(memory_space=pltpu.SMEM), vmem]
        + [pl.BlockSpec(memory_space=pltpu.HBM)] * 2
        + [vmem] * len(parts),
        out_specs=[vmem] * 3,
        scratch_shapes=[
            pltpu.VMEM((rows, features), jnp.bfloat16),
            pltpu.VMEM((rows, HEAD), jnp.float32),
            pltpu.VMEM((features, units), jnp.bfloat16),
            pltpu.VMEM((features, units), jnp.bfloat16),
            pltpu.SemaphoreType.DMA((2 * units // tile,)),
        ],
        compiler_params=pltpu.CompilerParams(vmem_limit_bytes=VMEM_BYTES),
        cost_estimate=cost(4 * rows * features * units, 4 * features * units, 0),
        name="gate_up",
    )(spot[None], norm_gain[None, :], gate_weight, up_weight, *parts)
    return keep, send


def add_halves(keep, got, units):
    half = keep.shape[0] // 2

    def kernel(keep_ref, low_ref, high_ref, next_ref, send_ref):
        for ref, got_ref, at in ((next_ref, low_ref, 0), (send_ref, high_ref, half)):
            here = pl.ds(at, half)
            ref[:, : 2 * units] = (
                keep_ref[here, : 2 * units].astype(jnp.float32)
                + got_ref[:, : 2 * units].astype(jnp.float32)
            ).astype(jnp.bfloat16)
            terms = keep_ref[here, 2 * units :].astype(jnp.float32)
            terms = terms + got_ref[:, 2 * units :].astype(jnp.float32)
            total = jnp.sum(terms, axis=1, keepdims=True)
            ref[:, 2 * units :] = split_terms(jnp.broadcast_to(total, (half, HEAD)))

    vmem = pl.BlockSpec(memory_space=pltpu.VMEM)
    return pl.pallas_call(
        kernel,
        out_shape=[jax.ShapeDtypeStruct((half, keep.shape[1]), jnp.bfloat16)] * 2,
        in_specs=[vmem] * 3,
        out_specs=[vmem, vmem],
        compiler_params=pltpu.CompilerParams(vmem_limit_bytes=SMALL_BYTES),
        cost_estimate=cost(2 * keep.size, 6 * keep.size, 0),
        name="add_halves",
    )(keep, *got)


def gated(keep, got, units):
    def kernel(keep_ref, got_ref, out_ref):
        summed = keep_ref[...].astype(jnp.float32) + got_ref[...].astype(jnp.float32)
        square = jnp.sum(summed[:, 2 * units :], axis=1, keepdims=True)
        scale = lax.rsqrt(square / D + EPSILON)
        gate = summed[:, :units] * scale
        up = summed[:, units : 2 * units] * scale
        out_ref[...] = (gate / (1.0 + jnp.exp(-gate)) * up).astype(jnp.bfloat16)

    vmem = pl.BlockSpec(memory_space=pltpu.VMEM)
    return pl.pallas_call(
        kernel,
        out_shape=jax.ShapeDtypeStruct((keep.shape[0], units), jnp.bfloat16),
        in_specs=[vmem, vmem],
        out_specs=vmem,
        compiler_params=pltpu.CompilerParams(vmem_limit_bytes=SMALL_BYTES),
        cost_estimate=cost(4 * keep.size, 5 * keep.size, keep.size // 2),
        name="gated",
    )(keep, got)


def down_rows(pieces, down_weight, spot, part_count, own_rows, group_total):
    rows = part_count * own_rows
    each = part_count // group_total
    units, features = down_weight.shape

    def kernel(spot_ref, weight_ref, *refs):
        piece_refs = refs[: len(pieces)]
        out_refs = refs[len(pieces) : len(pieces) + part_count]
        hidden, product = refs[len(pieces) + part_count :]
        at = 0
        for piece_ref in piece_refs:
            hidden[at : at + piece_ref.shape[0], :] = piece_ref[...]
            at += piece_ref.shape[0]
        product[...] = jnp.dot(
            hidden[...], weight_ref[...], preferred_element_type=jnp.float32
        )
        for index, out_ref in enumerate(out_refs):
            at = ((index // each) ^ spot_ref[0]) * each + index % each
            here = pl.ds(pl.multiple_of(at * own_rows, ALIGN), own_rows)
            out_ref[...] = product[here, :].astype(jnp.bfloat16)

    vmem = pl.BlockSpec(memory_space=pltpu.VMEM)
    return pl.pallas_call(
        kernel,
        out_shape=[jax.ShapeDtypeStruct((own_rows, features), jnp.bfloat16)] * part_count,
        in_specs=[pl.BlockSpec(memory_space=pltpu.SMEM)] + [vmem] * (1 + len(pieces)),
        out_specs=[vmem] * part_count,
        scratch_shapes=[
            pltpu.VMEM((rows, units), jnp.bfloat16),
            pltpu.VMEM((rows, features), jnp.float32),
        ],
        compiler_params=pltpu.CompilerParams(vmem_limit_bytes=SMALL_BYTES),
        cost_estimate=cost(2 * rows * features * units, 2 * features * units, 0),
        name="down",
    )(spot[None], down_weight, *pieces)


def swap(value, axis_name, mask):
    axis_total = lax.axis_size(axis_name)
    return lax.ppermute(value, axis_name, [(j, j ^ mask) for j in range(axis_total)])


def after(value, token):
    return lax.optimization_barrier((value, token))[0]


def gather_parts(value, axis_name, token=None):
    parts = [value] * lax.axis_size(axis_name)
    for mask in range(len(parts) - 2, 0, -2):
        parts[mask] = swap(value, axis_name, mask)
    for mask in [0] + list(range(len(parts) - 2, 0, -2)):
        held = parts[mask] if token is None or mask == 0 else after(parts[mask], token)
        parts[mask + 1] = swap(held, axis_name, 1)
    return parts


def pair_sums(parts, axis_name):
    evens = sorted((mask for mask in parts if mask % 2 == 0), reverse=True)
    got = {mask: swap(parts[mask + 1], axis_name, 1) for mask in evens}
    pairs = {
        mask: parts[mask].astype(jnp.float32) + got[mask].astype(jnp.float32) for mask in evens
    }
    return {mask: pair.astype(jnp.bfloat16) if mask else pair for mask, pair in pairs.items()}


def far_sum(pairs, axis_name):
    summed = 0.0
    for mask, pair in pairs.items():
        summed = summed + (swap(pair, axis_name, mask).astype(jnp.float32) if mask else pair)
    return summed


def scatter_sum(parts, axis_name):
    return far_sum(pair_sums(parts, axis_name), axis_name)


def shards(
    queries,
    root_cache,
    mid_cache,
    leaf_cache,
    token_leaf,
    leaf_parent,
    mid_parent,
    root_len,
    mid_len,
    leaf_len,
    root_slot,
    mid_slot,
    leaf_slot,
    stream,
    out_weight,
    norm_gain,
    gate_weight,
    up_weight,
    down_weight,
):
    own_rows, width = queries.shape
    owner = lax.axis_index("kv").astype(jnp.int32)
    caches = (root_cache, mid_cache, leaf_cache)
    nodes = own_nodes(
        owner,
        [cache.shape[0] for cache in caches],
        (token_leaf, leaf_parent, mid_parent),
        (root_len, mid_len, leaf_len),
        (root_slot, mid_slot, leaf_slot),
    )
    kv_count = root_cache.shape[2] // (2 * HEAD)
    group_width = width // kv_count
    mlp_total = lax.axis_size("mlp")
    mlp_place = lax.axis_index("mlp").astype(jnp.int32)
    own_width = stream.shape[1]
    query_parts = gather_parts(queries, "kv", nodes)
    attended, blocks = [], None
    for k in range(kv_count):
        parts = tree_attention(query_parts, caches, nodes, owner, k)
        every = lax.all_to_all(parts, "kv", 0, 0)
        one, blocks = combine_project(
            every, out_weight, k * group_width, blocks, mlp_place, own_width
        )
        attended.append(one)
    projected = scatter_sum(dict(enumerate(blocks)), "mlp")
    residual = (stream.astype(jnp.float32) + projected).astype(jnp.bfloat16)
    steps = [1 << bit for bit in range(mlp_total.bit_length() - 1)]
    spot = jnp.int32(0)
    for step in steps:
        spot = 2 * spot + (mlp_place // step) % 2
    units = gate_weight.shape[1]
    row_parts = gather_parts(residual, "kv")
    first, second = (
        [mask for mask in range(len(row_parts)) if (mask // 2) % 2 == side] for side in range(2)
    )
    row_parts[0] = after(row_parts[0], [row_parts[mask] for mask in second if mask % 2 == 0])

    def multiply(masks):
        parts = [row_parts[mask] for mask in masks]
        return gate_up_rows(parts, norm_gain, gate_weight, up_weight, spot, mlp_total)

    def reduce_once(keep, send, token=None):
        for step in steps[:-1]:
            if step > 1:
                send = jnp.split(send, 2, axis=0)
            got = [swap(piece, "mlp", step) for piece in send]
            if token is not None and step == 1:
                keep = after(keep, token)
            keep, send = add_halves(keep, got, units)
        return keep, send

    def regather(hidden):
        pieces = [hidden]
        for step in reversed(steps):
            held = pieces[0] if len(pieces) == 1 else jnp.concatenate(pieces, axis=0)
            pieces.append(swap(held, "mlp", step))
        return pieces

    def finish(pieces, masks):
        outs = down_rows(pieces, down_weight, spot, len(masks), own_rows, mlp_total)
        return pair_sums(dict(zip(masks, outs)), "kv")

    keep, send = reduce_once(*multiply(first))
    row_parts[second[0]] = after(row_parts[second[0]], send)
    later = multiply(second)
    hidden = gated(after(keep, later[0]), swap(send, "mlp", steps[-1]), units)
    keep, send = reduce_once(*later, hidden)
    pairs = finish(regather(hidden), first)
    keep = after(keep, [pair for mask, pair in pairs.items() if mask])
    hidden = gated(keep, swap(send, "mlp", steps[-1]), units)
    mixed = far_sum(pairs, "kv")
    pieces = regather(hidden)
    pieces[0] = after(pieces[0], mixed)
    mixed = mixed + far_sum(finish(pieces, second), "kv")
    return (jnp.concatenate(attended, axis=1), mixed.astype(jnp.bfloat16))


def solution(mesh):
    in_specs = (
        P("kv", "mlp"),
        P("kv", None, "mlp"),
        P("kv", None, "mlp"),
        P("kv", None, "mlp"),
        P(),
        P(),
        P(),
        P(),
        P(),
        P(),
        P(),
        P(),
        P(),
        P("kv", "mlp"),
        P("mlp", None),
        P("mlp"),
        P("mlp", "kv"),
        P("mlp", "kv"),
        P("kv", "mlp"),
    )
    out_specs = (P("kv", "mlp"), P("kv", "mlp"))
    return jax.shard_map(shards, mesh=mesh, in_specs=in_specs, out_specs=out_specs, check_vma=False)
```

```python
import math

import jax
import jax.numpy as jnp
from jax import lax
from jax.experimental import pallas as pl
from jax.experimental.pallas import tpu as pltpu
from jax.sharding import PartitionSpec as P

D = 4096
HEAD = 128
QLEAF = 16
QMID = 48
QROOT = 144


LOWEST = -1e30
EPSILON = 1e-05
ALIGN = 16
BLOCK = 512
VMEM_BYTES = 50 << 20
SMALL_BYTES = 24 << 20


def cost(flops, moved, exps):
    return pl.CostEstimate(flops=flops, bytes_accessed=moved, transcendentals=exps)


def streamed(pairs, sems):
    copies = [
        pltpu.make_async_copy(source, target, sems.at[k]) for k, (source, target) in enumerate(pairs)
    ]
    for copy in copies:
        copy.start()
    return copies


def own_nodes(owner, local_counts, tree, lengths, slots):
    token_leaf, leaf_parent, mid_parent = tree
    node_total = sum(local_counts)

    def kernel(owner_ref, token_ref, leaf_up, mid_up, *refs):
        len_refs, slot_refs, out_ref = refs[:3], refs[3:6], refs[6]

        def find(slot_ref, len_ref, local):
            base = owner_ref[0] * local

            def step(j, found):
                at, size = slot_ref[j] - base, len_ref[j]
                return tuple(
                    (jnp.where(at == k, j, node), jnp.where(at == k, size, length))
                    for k, (node, length) in enumerate(found)
                )

            zero = jnp.int32(0)
            return lax.fori_loop(0, slot_ref.shape[0], step, ((zero, zero),) * local)

        def below(parent_ref, edges):
            def step(j, counted):
                parent = parent_ref[j]
                return tuple(
                    c + jnp.where(parent < edge, 1, 0) for c, edge in zip(counted, edges)
                )

            return lax.fori_loop(0, parent_ref.shape[0], step, (jnp.int32(0),) * len(edges))

        picked = [find(*level) for level in zip(slot_refs, len_refs, local_counts)]
        edges = ()
        for level, parent_ref in enumerate((mid_up, leaf_up, None)):
            for node, _ in picked[level]:
                edges += (node, node + 1)
            if parent_ref is not None:
                edges = below(parent_ref, edges)
        tokens = token_ref[...]
        sizes = [length for level in picked for _, length in level]
        for k in range(node_total):
            for side in range(2):
                under = jnp.where(tokens < edges[2 * k + side], 1.0, 0.0)
                out_ref[side, k] = jnp.sum(under).astype(jnp.int32)
            out_ref[2, k] = sizes[k]

    smem = pl.BlockSpec(memory_space=pltpu.SMEM)
    vmem = pl.BlockSpec(memory_space=pltpu.VMEM)
    return pl.pallas_call(
        kernel,
        out_shape=jax.ShapeDtypeStruct((3, node_total), jnp.int32),
        in_specs=[smem, vmem] + [smem] * 8,
        out_specs=smem,
        name="own_nodes",
    )(owner[None], token_leaf.reshape(-1, HEAD), leaf_parent, mid_parent, *lengths, *slots)


def tree_attention(query_parts, caches, nodes, owner, kv_head):
    part_total = len(query_parts)
    own_rows = query_parts[0].shape[0]
    total_rows = part_total * own_rows
    width = query_parts[0].shape[1] // (caches[0].shape[2] // (2 * HEAD))
    group_size = width // HEAD
    score_scale = 1.0 / math.sqrt(HEAD)
    levels = []
    for cache, capacity in zip(caches, (QROOT, QMID, QLEAF)):
        levels.append((cache.shape[0], cache.shape[1], min(capacity + ALIGN, total_rows)))

    def kernel(nodes_ref, owner_ref, *refs):
        query_refs = refs[:part_total]
        cache_refs = refs[part_total : part_total + 3]
        near_ref, far_ref, all_rows, run_out, run_lse, acc, peak, total, *rest = refs[
            part_total + 3 :
        ]
        kept_refs, sems = rest[:3], rest[3]
        columns = pl.ds(kv_head * 2 * HEAD, 2 * HEAD)
        starts = [0, levels[0][0], levels[0][0] + levels[1][0]]
        lengths, flag_starts, flag = [], [], 0
        for start, (slot_total, span, _) in zip(starts, levels):
            lengths.append([nodes_ref[2, start + member] for member in range(slot_total)])
            flag_starts.append(flag)
            flag += slot_total * (span // min(BLOCK, span))

        def block_copy(level, member, index):
            span = levels[level][1]
            block = min(BLOCK, span)
            at = index * block
            here = pl.ds(at if isinstance(at, int) else pl.multiple_of(at, block), block)
            return pltpu.make_async_copy(
                cache_refs[level].at[member, here, columns],
                kept_refs[level].at[member, here, :],
                sems.at[flag_starts[level] + member * (span // block) + index],
            )

        steps = []
        for level, (slot_total, span, _) in enumerate(levels):
            block = min(BLOCK, span)
            pair = min(2 * block, span)
            longest = lengths[level][0]
            shortest = lengths[level][0]
            for length in lengths[level][1:]:
                longest, shortest = jnp.maximum(longest, length), jnp.minimum(shortest, length)
            whole, most = lax.div(shortest, pair), lax.div(longest + pair - 1, pair)
            steps.append((block, pair, whole, most))
            for index in range(span // pair):

                @pl.when(index < most)
                def _(level=level, index=index, ratio=pair // block, slot_total=slot_total):
                    for piece in range(ratio):
                        for member in range(slot_total):
                            block_copy(level, member, index * ratio + piece).start()

        me = owner_ref[0]
        for part in range(part_total):
            row = pl.multiple_of((me ^ part) * own_rows, ALIGN)
            all_rows[pl.ds(row, own_rows), :] = query_refs[part][
                :, kv_head * width : (kv_head + 1) * width
            ]
        run_out[...] = jnp.zeros_like(run_out)
        run_lse[...] = jnp.full_like(run_lse, LOWEST)
        offsets = [h * HEAD for h in range(group_size)]
        for level, (slot_total, span, rows) in enumerate(levels):
            block, pair, whole, most = steps[level]
            lanes = rows * group_size
            every = lanes * slot_total
            windows, grouped = [], []
            for member in range(slot_total):
                low = nodes_ref[0, starts[level] + member]
                window = jnp.minimum(low - lax.rem(low, ALIGN), total_rows - rows)
                window = pl.multiple_of(window, ALIGN)
                windows.append(window)
                grouped.append(
                    jnp.concatenate(
                        [all_rows[pl.ds(window, rows), c : c + HEAD] for c in offsets], axis=0
                    )
                )
            lane_of = lax.broadcasted_iota(jnp.int32, (1, every), 1)
            limits = jnp.full((1, every), lengths[level][0], jnp.int32)
            for member in range(1, slot_total):
                limits = jnp.where(lane_of >= member * lanes, lengths[level][member], limits)
            acc[:, :every] = jnp.zeros((HEAD, every), jnp.float32)
            peak[:, :every] = jnp.full((1, every), LOWEST, jnp.float32)
            total[:, :every] = jnp.zeros((1, every), jnp.float32)

            def visit(index, carry, masked):
                ratio = pair // block
                for piece in range(ratio):
                    for member in range(slot_total):
                        block_copy(level, member, index * ratio + piece).wait()
                scores = []
                for piece in range(ratio):
                    at = pl.multiple_of((index * ratio + piece) * block, block)
                    found = [
                        lax.dot_general(
                            kept_refs[level][member, pl.ds(at, block), :HEAD],
                            grouped[member],
                            (((1,), (1,)), ((), ())),
                            preferred_element_type=jnp.float32,
                        )
                        for member in range(slot_total)
                    ]
                    found = found[0] if slot_total == 1 else jnp.concatenate(found, axis=1)
                    if masked:
                        position = lax.broadcasted_iota(jnp.int32, (block, every), 0)
                        found = jnp.where(position < limits - at, found, LOWEST)
                    scores.append((at, found))
                for at, found in scores:
                    old_peak = peak[:, :every]
                    new_peak = jnp.maximum(old_peak, jnp.max(found, axis=0, keepdims=True))
                    weights = jnp.exp((found - new_peak) * score_scale)
                    if masked:
                        position = lax.broadcasted_iota(jnp.int32, (block, every), 0)
                        weights = jnp.where(position < limits - at, weights, 0.0)
                    fade = jnp.exp((old_peak - new_peak) * score_scale)
                    peak[:, :every] = new_peak
                    total[:, :every] = total[:, :every] * fade + jnp.sum(
                        weights, axis=0, keepdims=True
                    )
                    rounded = weights.astype(jnp.bfloat16)
                    for member in range(slot_total):
                        here = slice(member * lanes, (member + 1) * lanes)
                        acc[:, here] = acc[:, here] * fade[:, here] + lax.dot_general(
                            kept_refs[level][member, pl.ds(at, block), HEAD:],
                            rounded[:, here],
                            (((0,), (0,)), ((), ())),
                            preferred_element_type=jnp.float32,
                        )
                return carry

            lax.fori_loop(0, whole, lambda i, c: visit(i, c, False), 0)
            lax.fori_loop(whole, most, lambda i, c: visit(i, c, True), 0)

            weight_sum = total[:, :every]
            part_out = (acc[:, :every] / weight_sum).T
            part_lse = jnp.broadcast_to(
                peak[:, :every] * score_scale + jnp.log(weight_sum), (HEAD, every)
            ).T
            for member, window in enumerate(windows):
                low = nodes_ref[0, starts[level] + member]
                high = nodes_ref[1, starts[level] + member]
                position = window + lax.broadcasted_iota(jnp.int32, (rows, HEAD), 0)
                live = (position >= low) & (position < high)
                for h, c in enumerate(offsets):
                    here = (pl.ds(window, rows), slice(c, c + HEAD))
                    old_lse, old_out = run_lse[here], run_out[here]
                    at = member * lanes + h * rows
                    add_lse = part_lse[at : at + rows]
                    add_out = part_out[at : at + rows]
                    if level == 0:
                        run_out[here] = jnp.where(live, add_out, old_out)
                        run_lse[here] = jnp.where(live, add_lse, old_lse)
                        continue
                    best = jnp.maximum(old_lse, add_lse)
                    old_share = jnp.exp(old_lse - best)
                    add_share = jnp.exp(add_lse - best)
                    share = old_share + add_share
                    run_out[here] = jnp.where(
                        live, (old_out * old_share + add_out * add_share) / share, old_out
                    )
                    run_lse[here] = jnp.where(live, best + jnp.log(share), old_lse)
        lane = lax.broadcasted_iota(jnp.int32, (own_rows, HEAD), 1)
        for part in range(part_total):
            out_ref = far_ref if part % 2 else near_ref
            here = pl.ds(pl.multiple_of((me ^ part) * own_rows, ALIGN), own_rows)
            out_ref[part // 2, :, :width] = run_out[here, :].astype(jnp.bfloat16)
            lse = jnp.zeros((own_rows, HEAD), jnp.float32)
            for h in range(group_size):
                piece = run_lse[here, h * HEAD : (h + 1) * HEAD]
                lse = jnp.where(lax.rem(lane, group_size) == h, piece, lse)
            out_ref[part // 2, :, width:] = lse_terms(lse, lane, group_size)

    block_total = sum(count * (span // min(BLOCK, span)) for count, span, _ in levels)
    most = max(count * rows for count, _, rows in levels) * group_size
    vmem = pl.BlockSpec(memory_space=pltpu.VMEM)
    smem = pl.BlockSpec(memory_space=pltpu.SMEM)
    return pl.pallas_call(
        kernel,
        out_shape=[
            jax.ShapeDtypeStruct((part_total // 2, own_rows, width + HEAD), jnp.bfloat16)
        ]
        * 2,
        in_specs=[smem, smem]
        + [vmem] * part_total
        + [pl.BlockSpec(memory_space=pltpu.HBM)] * 3,
        out_specs=[vmem, vmem],
        scratch_shapes=[
            pltpu.VMEM((total_rows, width), jnp.bfloat16),
            pltpu.VMEM((total_rows, width), jnp.float32),
            pltpu.VMEM((total_rows, width), jnp.float32),
            pltpu.VMEM((HEAD, most), jnp.float32),
            pltpu.VMEM((1, most), jnp.float32),
            pltpu.VMEM((1, most), jnp.float32),
        ]
        + [pltpu.VMEM((count, span, 2 * HEAD), jnp.bfloat16) for count, span, _ in levels]
        + [pltpu.SemaphoreType.DMA((block_total,))],
        compiler_params=pltpu.CompilerParams(vmem_limit_bytes=VMEM_BYTES),
        cost_estimate=cost(
            4 * HEAD * group_size * sum(c * span * rows for c, span, rows in levels),
            2 * 2 * HEAD * sum(count * span for count, span, _ in levels),
            group_size * sum(c * span * rows for c, span, rows in levels),
        ),
        name="tree_attention",
    )(nodes, owner[None], *query_parts, *caches)


def lse_of(packed, group_size):
    terms = packed.astype(jnp.float32)
    return (
        terms
        + pltpu.roll(terms, HEAD - group_size, 1)
        + pltpu.roll(terms, HEAD - 2 * group_size, 1)
    )


def lse_terms(lse, lane, group_size):
    first = lse.astype(jnp.bfloat16).astype(jnp.float32)
    second = (lse - first).astype(jnp.bfloat16).astype(jnp.float32)
    third = lse - first - second
    field = lax.div(lane, group_size)
    packed = jnp.where(field == 2, third, 0.0)
    packed = jnp.where(field == 1, second, packed)
    return jnp.where(field == 0, first, packed).astype(jnp.bfloat16)


def merge_pairs(near, got):
    pair_total, own_rows, wide = near.shape
    width = wide - HEAD
    group_size = width // HEAD

    def kernel(near_ref, got_ref, *out_refs):
        lane = lax.broadcasted_iota(jnp.int32, (own_rows, HEAD), 1)
        for k, out_ref in enumerate(out_refs):
            left = lse_of(near_ref[k, :, width:], group_size)
            right = lse_of(got_ref[k, :, width:], group_size)
            best = jnp.maximum(left, right)
            left, right = jnp.exp(left - best), jnp.exp(right - best)
            whole = left + right
            left, right = left / whole, right / whole
            for h in range(group_size):
                here = slice(h * HEAD, (h + 1) * HEAD)
                out_ref[:, here] = (
                    near_ref[k, :, here].astype(jnp.float32) * left[:, h : h + 1]
                    + got_ref[k, :, here].astype(jnp.float32) * right[:, h : h + 1]
                ).astype(jnp.bfloat16)
            lse = jnp.where(lane < group_size, best + jnp.log(whole), 0.0)
            lse = lse + pltpu.roll(lse, group_size, 1) + pltpu.roll(lse, 2 * group_size, 1)
            out_ref[:, width:] = lse_terms(lse, lane, group_size)

    vmem = pl.BlockSpec(memory_space=pltpu.VMEM)
    return pl.pallas_call(
        kernel,
        out_shape=[jax.ShapeDtypeStruct((own_rows, wide), jnp.bfloat16)] * pair_total,
        in_specs=[vmem, vmem],
        out_specs=[vmem] * pair_total,
        compiler_params=pltpu.CompilerParams(vmem_limit_bytes=SMALL_BYTES),
        cost_estimate=cost(4 * near.size, 6 * near.size, pair_total * own_rows * 2 * HEAD),
        name="merge_pairs",
    )(near, got)


def combine_project(every, weight, row_start, added, place, own_width):
    part_total = len(every)
    own_rows, wide = every[0].shape
    width = wide - HEAD
    group_size = width // HEAD
    block_total = weight.shape[1] // own_width
    last = added is not None or width == weight.shape[0]
    kind = jnp.bfloat16 if last else jnp.float32

    def kernel(place_ref, weight_ref, *refs):
        every_refs, refs = refs[:part_total], refs[part_total:]
        added_refs = refs[:block_total] if added is not None else (None,) * block_total
        attended_ref, *block_refs = refs[len(refs) - 3 - block_total : -2]
        kept, sems = refs[-2:]
        columns = [
            pl.ds(pl.multiple_of((place_ref[0] ^ block) * own_width, HEAD), own_width)
            for block in range(block_total)
        ]
        copies = streamed(
            [
                (weight_ref.at[pl.ds(row_start, width), column], kept.at[block])
                for block, column in enumerate(columns)
            ],
            sems,
        )
        lse = [lse_of(ref[:, width:], group_size) for ref in every_refs]
        best = lse[0]
        for one in lse[1:]:
            best = jnp.maximum(best, one)
        share = [jnp.exp(one - best) for one in lse]
        whole = share[0]
        for one in share[1:]:
            whole = whole + one
        for h in range(group_size):
            summed = jnp.zeros((own_rows, HEAD), jnp.float32)
            for part in range(part_total):
                summed = summed + (
                    every_refs[part][:, h * HEAD : (h + 1) * HEAD].astype(jnp.float32)
                    * share[part][:, h : h + 1]
                )
            attended_ref[:, h * HEAD : (h + 1) * HEAD] = (summed / whole[:, h : h + 1]).astype(
                jnp.bfloat16
            )
        for block in range(block_total):
            copies[block].wait()
            product = jnp.dot(
                attended_ref[...], kept[block], preferred_element_type=jnp.float32
            )
            if added is not None:
                product = product + added_refs[block][...]
            block_refs[block][...] = product.astype(kind)

    vmem = pl.BlockSpec(memory_space=pltpu.VMEM)
    outs = pl.pallas_call(
        kernel,
        out_shape=[jax.ShapeDtypeStruct((own_rows, width), jnp.bfloat16)]
        + [jax.ShapeDtypeStruct((own_rows, own_width), kind)] * block_total,
        in_specs=[pl.BlockSpec(memory_space=pltpu.SMEM), pl.BlockSpec(memory_space=pltpu.HBM)]
        + [vmem] * (part_total + (block_total if added is not None else 0)),
        out_specs=[vmem] * (1 + block_total),
        scratch_shapes=[
            pltpu.VMEM((block_total, width, own_width), jnp.bfloat16),
            pltpu.SemaphoreType.DMA((block_total,)),
        ],
        compiler_params=pltpu.CompilerParams(vmem_limit_bytes=VMEM_BYTES),
        cost_estimate=cost(
            2 * own_rows * width * weight.shape[1],
            2 * width * weight.shape[1],
            part_total * own_rows * HEAD,
        ),
        name="combine_project",
    )(place[None], weight, *every, *(added or ()))
    return outs[0], outs[1:]


def split_terms(value):
    first = value.astype(jnp.bfloat16).astype(jnp.float32)
    second = (value - first).astype(jnp.bfloat16).astype(jnp.float32)
    lane = lax.broadcasted_iota(jnp.int32, value.shape, 1)
    third = jnp.where(lane == 2, value - first - second, 0.0)
    return jnp.where(lane == 0, first, jnp.where(lane == 1, second, third)).astype(jnp.bfloat16)


def gate_up_rows(parts, norm_gain, gate_weight, up_weight, spot, group_total):
    own_rows, features = parts[0].shape
    rows = own_rows * len(parts)
    half = rows // 2
    piece = half // 2
    each = len(parts) // group_total
    units = gate_weight.shape[1]
    tile = units // 2 if (units // 2) % HEAD == 0 else units

    def kernel(spot_ref, gain_ref, gate_ref, up_ref, *refs):
        part_refs = refs[: len(parts)]
        keep_ref, *send_refs, scaled, squares, kept_gate, kept_up, sems = refs[len(parts) :]
        tiles = [
            (ref, kept, base, at)
            for ref, kept, base in ((gate_ref, kept_gate, 0), (up_ref, kept_up, units))
            for at in range(0, units, tile)
        ]
        copies = streamed(
            [
                (ref, kept)
                if tile == units
                else (ref.at[:, pl.ds(at, tile)], kept.at[:, pl.ds(at, tile)])
                for ref, kept, _, at in tiles
            ],
            sems,
        )
        for index, part_ref in enumerate(part_refs):
            at = ((index // each) ^ spot_ref[0]) * each + index % each
            here = pl.ds(pl.multiple_of(at * own_rows, ALIGN), own_rows)
            wide = part_ref[...].astype(jnp.float32)
            scaled[here, :] = (wide * gain_ref[...]).astype(jnp.bfloat16)
            squares[here, :] = jnp.broadcast_to(
                jnp.sum(wide * wide, axis=1, keepdims=True), (own_rows, HEAD)
            )
        for copy, (_, kept, base, at) in zip(copies, tiles):
            copy.wait()
            here = slice(base + at, base + at + tile)
            product = jnp.dot(
                scaled[...], kept[:, at : at + tile], preferred_element_type=jnp.float32
            ).astype(jnp.bfloat16)
            keep_ref[:, here] = product[:half]
            for k, send_ref in enumerate(send_refs):
                send_ref[:, here] = product[half + k * piece : half + (k + 1) * piece]
        terms = split_terms(squares[...])
        keep_ref[:, 2 * units :] = terms[:half]
        for k, send_ref in enumerate(send_refs):
            send_ref[:, 2 * units :] = terms[half + k * piece : half + (k + 1) * piece]

    vmem = pl.BlockSpec(memory_space=pltpu.VMEM)
    keep, *send = pl.pallas_call(
        kernel,
        out_shape=[jax.ShapeDtypeStruct((half, 2 * units + HEAD), jnp.bfloat16)]
        + [jax.ShapeDtypeStruct((piece, 2 * units + HEAD), jnp.bfloat16)] * 2,
        in_specs=[pl.BlockSpec(memory_space=pltpu.SMEM), vmem]
        + [pl.BlockSpec(memory_space=pltpu.HBM)] * 2
        + [vmem] * len(parts),
        out_specs=[vmem] * 3,
        scratch_shapes=[
            pltpu.VMEM((rows, features), jnp.bfloat16),
            pltpu.VMEM((rows, HEAD), jnp.float32),
            pltpu.VMEM((features, units), jnp.bfloat16),
            pltpu.VMEM((features, units), jnp.bfloat16),
            pltpu.SemaphoreType.DMA((2 * units // tile,)),
        ],
        compiler_params=pltpu.CompilerParams(vmem_limit_bytes=VMEM_BYTES),
        cost_estimate=cost(4 * rows * features * units, 4 * features * units, 0),
        name="gate_up",
    )(spot[None], norm_gain[None, :], gate_weight, up_weight, *parts)
    return keep, send


def add_halves(keep, got, units):
    half = keep.shape[0] // 2

    def kernel(keep_ref, low_ref, high_ref, next_ref, send_ref):
        for ref, got_ref, at in ((next_ref, low_ref, 0), (send_ref, high_ref, half)):
            here = pl.ds(at, half)
            ref[:, : 2 * units] = (
                keep_ref[here, : 2 * units].astype(jnp.float32)
                + got_ref[:, : 2 * units].astype(jnp.float32)
            ).astype(jnp.bfloat16)
            terms = keep_ref[here, 2 * units :].astype(jnp.float32)
            terms = terms + got_ref[:, 2 * units :].astype(jnp.float32)
            total = jnp.sum(terms, axis=1, keepdims=True)
            ref[:, 2 * units :] = split_terms(jnp.broadcast_to(total, (half, HEAD)))

    vmem = pl.BlockSpec(memory_space=pltpu.VMEM)
    return pl.pallas_call(
        kernel,
        out_shape=[jax.ShapeDtypeStruct((half, keep.shape[1]), jnp.bfloat16)] * 2,
        in_specs=[vmem] * 3,
        out_specs=[vmem, vmem],
        compiler_params=pltpu.CompilerParams(vmem_limit_bytes=SMALL_BYTES),
        cost_estimate=cost(2 * keep.size, 6 * keep.size, 0),
        name="add_halves",
    )(keep, *got)


def gated(keep, got, units):
    def kernel(keep_ref, got_ref, out_ref):
        summed = keep_ref[...].astype(jnp.float32) + got_ref[...].astype(jnp.float32)
        square = jnp.sum(summed[:, 2 * units :], axis=1, keepdims=True)
        scale = lax.rsqrt(square / D + EPSILON)
        gate = summed[:, :units] * scale
        up = summed[:, units : 2 * units] * scale
        out_ref[...] = (gate / (1.0 + jnp.exp(-gate)) * up).astype(jnp.bfloat16)

    vmem = pl.BlockSpec(memory_space=pltpu.VMEM)
    return pl.pallas_call(
        kernel,
        out_shape=jax.ShapeDtypeStruct((keep.shape[0], units), jnp.bfloat16),
        in_specs=[vmem, vmem],
        out_specs=vmem,
        compiler_params=pltpu.CompilerParams(vmem_limit_bytes=SMALL_BYTES),
        cost_estimate=cost(4 * keep.size, 5 * keep.size, keep.size // 2),
        name="gated",
    )(keep, got)


def down_rows(pieces, down_weight, spot, part_count, own_rows, group_total):
    rows = part_count * own_rows
    each = part_count // group_total
    units, features = down_weight.shape

    def kernel(spot_ref, weight_ref, *refs):
        piece_refs = refs[: len(pieces)]
        out_refs = refs[len(pieces) : len(pieces) + part_count]
        hidden, product = refs[len(pieces) + part_count :]
        at = 0
        for piece_ref in piece_refs:
            hidden[at : at + piece_ref.shape[0], :] = piece_ref[...]
            at += piece_ref.shape[0]
        product[...] = jnp.dot(
            hidden[...], weight_ref[...], preferred_element_type=jnp.float32
        )
        for index, out_ref in enumerate(out_refs):
            at = ((index // each) ^ spot_ref[0]) * each + index % each
            here = pl.ds(pl.multiple_of(at * own_rows, ALIGN), own_rows)
            out_ref[...] = product[here, :].astype(jnp.bfloat16)

    vmem = pl.BlockSpec(memory_space=pltpu.VMEM)
    return pl.pallas_call(
        kernel,
        out_shape=[jax.ShapeDtypeStruct((own_rows, features), jnp.bfloat16)] * part_count,
        in_specs=[pl.BlockSpec(memory_space=pltpu.SMEM)] + [vmem] * (1 + len(pieces)),
        out_specs=[vmem] * part_count,
        scratch_shapes=[
            pltpu.VMEM((rows, units), jnp.bfloat16),
            pltpu.VMEM((rows, features), jnp.float32),
        ],
        compiler_params=pltpu.CompilerParams(vmem_limit_bytes=SMALL_BYTES),
        cost_estimate=cost(2 * rows * features * units, 2 * features * units, 0),
        name="down",
    )(spot[None], down_weight, *pieces)


def swap(value, axis_name, mask):
    axis_total = lax.axis_size(axis_name)
    return lax.ppermute(value, axis_name, [(j, j ^ mask) for j in range(axis_total)])


def after(value, token):
    return lax.optimization_barrier((value, token))[0]


def gather_parts(value, axis_name, token=None):
    parts = [value] * lax.axis_size(axis_name)
    for mask in range(len(parts) - 2, 0, -2):
        parts[mask] = swap(value, axis_name, mask)
    for mask in [0] + list(range(len(parts) - 2, 0, -2)):
        held = parts[mask] if token is None or mask == 0 else after(parts[mask], token)
        parts[mask + 1] = swap(held, axis_name, 1)
    return parts


def pair_sums(parts, axis_name):
    evens = sorted((mask for mask in parts if mask % 2 == 0), reverse=True)
    got = {mask: swap(parts[mask + 1], axis_name, 1) for mask in evens}
    pairs = {
        mask: parts[mask].astype(jnp.float32) + got[mask].astype(jnp.float32) for mask in evens
    }
    return {mask: pair.astype(jnp.bfloat16) if mask else pair for mask, pair in pairs.items()}


def far_sum(pairs, axis_name):
    summed = 0.0
    for mask, pair in pairs.items():
        summed = summed + (swap(pair, axis_name, mask).astype(jnp.float32) if mask else pair)
    return summed


def scatter_sum(parts, axis_name):
    return far_sum(pair_sums(parts, axis_name), axis_name)


def shards(
    queries,
    root_cache,
    mid_cache,
    leaf_cache,
    token_leaf,
    leaf_parent,
    mid_parent,
    root_len,
    mid_len,
    leaf_len,
    root_slot,
    mid_slot,
    leaf_slot,
    stream,
    out_weight,
    norm_gain,
    gate_weight,
    up_weight,
    down_weight,
):
    own_rows, width = queries.shape
    owner = lax.axis_index("kv").astype(jnp.int32)
    caches = (root_cache, mid_cache, leaf_cache)
    nodes = own_nodes(
        owner,
        [cache.shape[0] for cache in caches],
        (token_leaf, leaf_parent, mid_parent),
        (root_len, mid_len, leaf_len),
        (root_slot, mid_slot, leaf_slot),
    )
    kv_count = root_cache.shape[2] // (2 * HEAD)
    group_width = width // kv_count
    mlp_total = lax.axis_size("mlp")
    mlp_place = lax.axis_index("mlp").astype(jnp.int32)
    own_width = stream.shape[1]
    query_parts = gather_parts(queries, "kv", nodes)
    attended, blocks = [], None
    for k in range(kv_count):
        near, far = tree_attention(query_parts, caches, nodes, owner, k)
        merged = merge_pairs(near, swap(far, "kv", 1))
        every = [swap(one, "kv", 2 * pair) if pair else one for pair, one in enumerate(merged)]
        one, blocks = combine_project(
            every, out_weight, k * group_width, blocks, mlp_place, own_width
        )
        attended.append(one)
    projected = scatter_sum(dict(enumerate(blocks)), "mlp")
    residual = (stream.astype(jnp.float32) + projected).astype(jnp.bfloat16)
    steps = [1 << bit for bit in range(mlp_total.bit_length() - 1)]
    spot = jnp.int32(0)
    for step in steps:
        spot = 2 * spot + (mlp_place // step) % 2
    units = gate_weight.shape[1]
    row_parts = gather_parts(residual, "kv")
    first, second = (
        [mask for mask in range(len(row_parts)) if (mask // 2) % 2 == side] for side in range(2)
    )
    row_parts[0] = after(row_parts[0], [row_parts[mask] for mask in second if mask % 2 == 0])

    def multiply(masks):
        parts = [row_parts[mask] for mask in masks]
        return gate_up_rows(parts, norm_gain, gate_weight, up_weight, spot, mlp_total)

    def reduce_once(keep, send, token=None):
        for step in steps[:-1]:
            if step > 1:
                send = jnp.split(send, 2, axis=0)
            got = [swap(piece, "mlp", step) for piece in send]
            if token is not None and step == 1:
                keep = after(keep, token)
            keep, send = add_halves(keep, got, units)
        return keep, send

    def regather(hidden, token):
        pieces = [hidden]
        for step in reversed(steps):
            held = pieces[0] if len(pieces) == 1 else jnp.concatenate(pieces, axis=0)
            if step != steps[-1] and token is not None:
                held = after(held, token)
            pieces.append(swap(held, "mlp", step))
        return pieces

    def finish(pieces, masks):
        outs = down_rows(pieces, down_weight, spot, len(masks), own_rows, mlp_total)
        return pair_sums(dict(zip(masks, outs)), "kv")

    keep, send = reduce_once(*multiply(first))
    row_parts[second[0]] = after(row_parts[second[0]], send)
    later = multiply(second)
    hidden = gated(after(keep, later[0]), swap(send, "mlp", steps[-1]), units)
    keep, send = reduce_once(*later, hidden)
    pairs = finish(regather(hidden, None), first)
    keep = after(keep, pairs[0])
    hidden = gated(keep, swap(send, "mlp", steps[-1]), units)
    mixed = far_sum(pairs, "kv")
    mixed = mixed + far_sum(finish(regather(hidden, mixed), second), "kv")
    return (jnp.concatenate(attended, axis=1), mixed.astype(jnp.bfloat16))


def solution(mesh):
    in_specs = (
        P("kv", "mlp"),
        P("kv", None, "mlp"),
        P("kv", None, "mlp"),
        P("kv", None, "mlp"),
        P(),
        P(),
        P(),
        P(),
        P(),
        P(),
        P(),
        P(),
        P(),
        P("kv", "mlp"),
        P("mlp", None),
        P("mlp"),
        P("mlp", "kv"),
        P("mlp", "kv"),
        P("kv", "mlp"),
    )
    out_specs = (P("kv", "mlp"), P("kv", "mlp"))
    return jax.shard_map(shards, mesh=mesh, in_specs=in_specs, out_specs=out_specs, check_vma=False)
```

```python
import math

import jax
import jax.numpy as jnp
from jax import lax
from jax.experimental import pallas as pl
from jax.experimental.pallas import tpu as pltpu
from jax.sharding import PartitionSpec as P

D = 4096
HEAD = 128
QLEAF = 16
QMID = 48
QROOT = 144


LOWEST = -1e30
EPSILON = 1e-05
ALIGN = 16
BLOCK = 512
VMEM_BYTES = 50 << 20
SMALL_BYTES = 24 << 20


def cost(flops, moved, exps):
    return pl.CostEstimate(flops=flops, bytes_accessed=moved, transcendentals=exps)


def streamed(pairs, sems):
    copies = [
        pltpu.make_async_copy(source, target, sems.at[k]) for k, (source, target) in enumerate(pairs)
    ]
    for copy in copies:
        copy.start()
    return copies


def own_nodes(owner, local_counts, tree, lengths, slots):
    token_leaf, leaf_parent, mid_parent = tree
    node_total = sum(local_counts)

    def kernel(owner_ref, token_ref, leaf_up, mid_up, *refs):
        len_refs, slot_refs, out_ref = refs[:3], refs[3:6], refs[6]

        def find(slot_ref, len_ref, local):
            base = owner_ref[0] * local

            def step(j, found):
                at, size = slot_ref[j] - base, len_ref[j]
                return tuple(
                    (jnp.where(at == k, j, node), jnp.where(at == k, size, length))
                    for k, (node, length) in enumerate(found)
                )

            zero = jnp.int32(0)
            return lax.fori_loop(0, slot_ref.shape[0], step, ((zero, zero),) * local)

        def below(parent_ref, edges):
            def step(j, counted):
                parent = parent_ref[j]
                return tuple(
                    c + jnp.where(parent < edge, 1, 0) for c, edge in zip(counted, edges)
                )

            return lax.fori_loop(0, parent_ref.shape[0], step, (jnp.int32(0),) * len(edges))

        picked = [find(*level) for level in zip(slot_refs, len_refs, local_counts)]
        edges = ()
        for level, parent_ref in enumerate((mid_up, leaf_up, None)):
            for node, _ in picked[level]:
                edges += (node, node + 1)
            if parent_ref is not None:
                edges = below(parent_ref, edges)
        tokens = token_ref[...]
        sizes = [length for level in picked for _, length in level]
        for k in range(node_total):
            for side in range(2):
                under = jnp.where(tokens < edges[2 * k + side], 1.0, 0.0)
                out_ref[side, k] = jnp.sum(under).astype(jnp.int32)
            out_ref[2, k] = sizes[k]

    smem = pl.BlockSpec(memory_space=pltpu.SMEM)
    vmem = pl.BlockSpec(memory_space=pltpu.VMEM)
    return pl.pallas_call(
        kernel,
        out_shape=jax.ShapeDtypeStruct((3, node_total), jnp.int32),
        in_specs=[smem, vmem] + [smem] * 8,
        out_specs=smem,
        name="own_nodes",
    )(owner[None], token_leaf.reshape(-1, HEAD), leaf_parent, mid_parent, *lengths, *slots)


def tree_attention(query_parts, caches, nodes, owner, kv_head):
    part_total = len(query_parts)
    own_rows = query_parts[0].shape[0]
    total_rows = part_total * own_rows
    width = query_parts[0].shape[1] // (caches[0].shape[2] // (2 * HEAD))
    group_size = width // HEAD
    score_scale = 1.0 / math.sqrt(HEAD)
    levels = []
    for cache, capacity in zip(caches, (QROOT, QMID, QLEAF)):
        levels.append((cache.shape[0], cache.shape[1], min(capacity + ALIGN, total_rows)))

    def kernel(nodes_ref, owner_ref, *refs):
        query_refs = refs[:part_total]
        cache_refs = refs[part_total : part_total + 3]
        near_ref, far_ref, all_rows, run_out, run_lse, acc, peak, total, *rest = refs[
            part_total + 3 :
        ]
        kept_refs, sems = rest[:3], rest[3]
        columns = pl.ds(kv_head * 2 * HEAD, 2 * HEAD)
        starts = [0, levels[0][0], levels[0][0] + levels[1][0]]
        lengths, flag_starts, flag = [], [], 0
        for start, (slot_total, span, _) in zip(starts, levels):
            lengths.append([nodes_ref[2, start + member] for member in range(slot_total)])
            flag_starts.append(flag)
            flag += slot_total * (span // min(BLOCK, span))

        def block_copy(level, member, index):
            span = levels[level][1]
            block = min(BLOCK, span)
            at = index * block
            here = pl.ds(at if isinstance(at, int) else pl.multiple_of(at, block), block)
            return pltpu.make_async_copy(
                cache_refs[level].at[member, here, columns],
                kept_refs[level].at[member, here, :],
                sems.at[flag_starts[level] + member * (span // block) + index],
            )

        steps = []
        for level, (slot_total, span, _) in enumerate(levels):
            block = min(BLOCK, span)
            pair = min(2 * block, span)
            longest = lengths[level][0]
            shortest = lengths[level][0]
            for length in lengths[level][1:]:
                longest, shortest = jnp.maximum(longest, length), jnp.minimum(shortest, length)
            whole, most = lax.div(shortest, pair), lax.div(longest + pair - 1, pair)
            steps.append((block, pair, whole, most))
            for index in range(span // pair):

                @pl.when(index < most)
                def _(level=level, index=index, ratio=pair // block, slot_total=slot_total):
                    for piece in range(ratio):
                        for member in range(slot_total):
                            block_copy(level, member, index * ratio + piece).start()

        me = owner_ref[0]
        for part in range(part_total):
            row = pl.multiple_of((me ^ part) * own_rows, ALIGN)
            all_rows[pl.ds(row, own_rows), :] = query_refs[part][
                :, kv_head * width : (kv_head + 1) * width
            ]
        run_out[...] = jnp.zeros_like(run_out)
        run_lse[...] = jnp.full_like(run_lse, LOWEST)
        offsets = [h * HEAD for h in range(group_size)]
        for level, (slot_total, span, rows) in enumerate(levels):
            block, pair, whole, most = steps[level]
            lanes = rows * group_size
            every = lanes * slot_total
            windows, grouped = [], []
            for member in range(slot_total):
                low = nodes_ref[0, starts[level] + member]
                window = jnp.minimum(low - lax.rem(low, ALIGN), total_rows - rows)
                window = pl.multiple_of(window, ALIGN)
                windows.append(window)
                grouped.append(
                    jnp.concatenate(
                        [all_rows[pl.ds(window, rows), c : c + HEAD] for c in offsets], axis=0
                    )
                )
            lane_of = lax.broadcasted_iota(jnp.int32, (1, every), 1)
            limits = jnp.full((1, every), lengths[level][0], jnp.int32)
            for member in range(1, slot_total):
                limits = jnp.where(lane_of >= member * lanes, lengths[level][member], limits)
            acc[:, :every] = jnp.zeros((HEAD, every), jnp.float32)
            peak[:, :every] = jnp.full((1, every), LOWEST, jnp.float32)
            total[:, :every] = jnp.zeros((1, every), jnp.float32)

            def visit(index, carry, masked):
                ratio = pair // block
                for piece in range(ratio):
                    for member in range(slot_total):
                        block_copy(level, member, index * ratio + piece).wait()
                scores = []
                for piece in range(ratio):
                    at = pl.multiple_of((index * ratio + piece) * block, block)
                    found = [
                        lax.dot_general(
                            kept_refs[level][member, pl.ds(at, block), :HEAD],
                            grouped[member],
                            (((1,), (1,)), ((), ())),
                            preferred_element_type=jnp.float32,
                        )
                        for member in range(slot_total)
                    ]
                    found = found[0] if slot_total == 1 else jnp.concatenate(found, axis=1)
                    if masked:
                        position = lax.broadcasted_iota(jnp.int32, (block, every), 0)
                        found = jnp.where(position < limits - at, found, LOWEST)
                    scores.append((at, found))
                for at, found in scores:
                    old_peak = peak[:, :every]
                    new_peak = jnp.maximum(old_peak, jnp.max(found, axis=0, keepdims=True))
                    weights = jnp.exp((found - new_peak) * score_scale)
                    fade = jnp.exp((old_peak - new_peak) * score_scale)
                    peak[:, :every] = new_peak
                    total[:, :every] = total[:, :every] * fade + jnp.sum(
                        weights, axis=0, keepdims=True
                    )
                    rounded = weights.astype(jnp.bfloat16)
                    for member in range(slot_total):
                        here = slice(member * lanes, (member + 1) * lanes)
                        acc[:, here] = acc[:, here] * fade[:, here] + lax.dot_general(
                            kept_refs[level][member, pl.ds(at, block), HEAD:],
                            rounded[:, here],
                            (((0,), (0,)), ((), ())),
                            preferred_element_type=jnp.float32,
                        )
                return carry

            lax.fori_loop(0, whole, lambda i, c: visit(i, c, False), 0)
            lax.fori_loop(whole, most, lambda i, c: visit(i, c, True), 0)

            weight_sum = total[:, :every]
            part_out = (acc[:, :every] / weight_sum).T
            part_lse = jnp.broadcast_to(
                peak[:, :every] * score_scale + jnp.log(weight_sum), (HEAD, every)
            ).T
            for member, window in enumerate(windows):
                low = nodes_ref[0, starts[level] + member]
                high = nodes_ref[1, starts[level] + member]
                position = window + lax.broadcasted_iota(jnp.int32, (rows, HEAD), 0)
                live = (position >= low) & (position < high)
                for h, c in enumerate(offsets):
                    here = (pl.ds(window, rows), slice(c, c + HEAD))
                    old_lse, old_out = run_lse[here], run_out[here]
                    at = member * lanes + h * rows
                    add_lse = part_lse[at : at + rows]
                    add_out = part_out[at : at + rows]
                    if level == 0:
                        run_out[here] = jnp.where(live, add_out, old_out)
                        run_lse[here] = jnp.where(live, add_lse, old_lse)
                        continue
                    best = jnp.maximum(old_lse, add_lse)
                    old_share = jnp.exp(old_lse - best)
                    add_share = jnp.exp(add_lse - best)
                    share = old_share + add_share
                    run_out[here] = jnp.where(
                        live, (old_out * old_share + add_out * add_share) / share, old_out
                    )
                    run_lse[here] = jnp.where(live, best + jnp.log(share), old_lse)
        lane = lax.broadcasted_iota(jnp.int32, (own_rows, HEAD), 1)
        for part in range(part_total):
            out_ref = far_ref if part % 2 else near_ref
            here = pl.ds(pl.multiple_of((me ^ part) * own_rows, ALIGN), own_rows)
            out_ref[part // 2, :, :width] = run_out[here, :].astype(jnp.bfloat16)
            lse = jnp.zeros((own_rows, HEAD), jnp.float32)
            for h in range(group_size):
                piece = run_lse[here, h * HEAD : (h + 1) * HEAD]
                lse = jnp.where(lax.rem(lane, group_size) == h, piece, lse)
            out_ref[part // 2, :, width:] = lse_terms(lse, lane, group_size)

    block_total = sum(count * (span // min(BLOCK, span)) for count, span, _ in levels)
    most = max(count * rows for count, _, rows in levels) * group_size
    vmem = pl.BlockSpec(memory_space=pltpu.VMEM)
    smem = pl.BlockSpec(memory_space=pltpu.SMEM)
    return pl.pallas_call(
        kernel,
        out_shape=[
            jax.ShapeDtypeStruct((part_total // 2, own_rows, width + HEAD), jnp.bfloat16)
        ]
        * 2,
        in_specs=[smem, smem]
        + [vmem] * part_total
        + [pl.BlockSpec(memory_space=pltpu.HBM)] * 3,
        out_specs=[vmem, vmem],
        scratch_shapes=[
            pltpu.VMEM((total_rows, width), jnp.bfloat16),
            pltpu.VMEM((total_rows, width), jnp.float32),
            pltpu.VMEM((total_rows, width), jnp.float32),
            pltpu.VMEM((HEAD, most), jnp.float32),
            pltpu.VMEM((1, most), jnp.float32),
            pltpu.VMEM((1, most), jnp.float32),
        ]
        + [pltpu.VMEM((count, span, 2 * HEAD), jnp.bfloat16) for count, span, _ in levels]
        + [pltpu.SemaphoreType.DMA((block_total,))],
        compiler_params=pltpu.CompilerParams(vmem_limit_bytes=VMEM_BYTES),
        cost_estimate=cost(
            4 * HEAD * group_size * sum(c * span * rows for c, span, rows in levels),
            2 * 2 * HEAD * sum(count * span for count, span, _ in levels),
            group_size * sum(c * span * rows for c, span, rows in levels),
        ),
        name="tree_attention",
    )(nodes, owner[None], *query_parts, *caches)


def lse_of(packed, group_size):
    terms = packed.astype(jnp.float32)
    return (
        terms
        + pltpu.roll(terms, HEAD - group_size, 1)
        + pltpu.roll(terms, HEAD - 2 * group_size, 1)
    )


def lse_terms(lse, lane, group_size):
    first = lse.astype(jnp.bfloat16).astype(jnp.float32)
    second = (lse - first).astype(jnp.bfloat16).astype(jnp.float32)
    third = lse - first - second
    field = lax.div(lane, group_size)
    packed = jnp.where(field == 2, third, 0.0)
    packed = jnp.where(field == 1, second, packed)
    return jnp.where(field == 0, first, packed).astype(jnp.bfloat16)


def merge_pairs(near, got):
    pair_total, own_rows, wide = near.shape
    width = wide - HEAD
    group_size = width // HEAD

    def kernel(near_ref, got_ref, *out_refs):
        lane = lax.broadcasted_iota(jnp.int32, (own_rows, HEAD), 1)
        for k, out_ref in enumerate(out_refs):
            left = lse_of(near_ref[k, :, width:], group_size)
            right = lse_of(got_ref[k, :, width:], group_size)
            best = jnp.maximum(left, right)
            left, right = jnp.exp(left - best), jnp.exp(right - best)
            whole = left + right
            left, right = left / whole, right / whole
            for h in range(group_size):
                here = slice(h * HEAD, (h + 1) * HEAD)
                out_ref[:, here] = (
                    near_ref[k, :, here].astype(jnp.float32) * left[:, h : h + 1]
                    + got_ref[k, :, here].astype(jnp.float32) * right[:, h : h + 1]
                ).astype(jnp.bfloat16)
            lse = jnp.where(lane < group_size, best + jnp.log(whole), 0.0)
            lse = lse + pltpu.roll(lse, group_size, 1) + pltpu.roll(lse, 2 * group_size, 1)
            out_ref[:, width:] = lse_terms(lse, lane, group_size)

    vmem = pl.BlockSpec(memory_space=pltpu.VMEM)
    return pl.pallas_call(
        kernel,
        out_shape=[jax.ShapeDtypeStruct((own_rows, wide), jnp.bfloat16)] * pair_total,
        in_specs=[vmem, vmem],
        out_specs=[vmem] * pair_total,
        compiler_params=pltpu.CompilerParams(vmem_limit_bytes=SMALL_BYTES),
        cost_estimate=cost(4 * near.size, 6 * near.size, pair_total * own_rows * 2 * HEAD),
        name="merge_pairs",
    )(near, got)


def combine_project(every, weight, row_start, added, place, own_width):
    part_total = len(every)
    own_rows, wide = every[0].shape
    width = wide - HEAD
    group_size = width // HEAD
    block_total = weight.shape[1] // own_width
    last = added is not None or width == weight.shape[0]
    kind = jnp.bfloat16 if last else jnp.float32

    def kernel(place_ref, weight_ref, *refs):
        every_refs, refs = refs[:part_total], refs[part_total:]
        added_refs = refs[:block_total] if added is not None else (None,) * block_total
        attended_ref, *block_refs = refs[len(refs) - 3 - block_total : -2]
        kept, sems = refs[-2:]
        columns = [
            pl.ds(pl.multiple_of((place_ref[0] ^ block) * own_width, HEAD), own_width)
            for block in range(block_total)
        ]
        copies = streamed(
            [
                (weight_ref.at[pl.ds(row_start, width), column], kept.at[block])
                for block, column in enumerate(columns)
            ],
            sems,
        )
        lse = [lse_of(ref[:, width:], group_size) for ref in every_refs]
        best = lse[0]
        for one in lse[1:]:
            best = jnp.maximum(best, one)
        share = [jnp.exp(one - best) for one in lse]
        whole = share[0]
        for one in share[1:]:
            whole = whole + one
        for h in range(group_size):
            summed = jnp.zeros((own_rows, HEAD), jnp.float32)
            for part in range(part_total):
                summed = summed + (
                    every_refs[part][:, h * HEAD : (h + 1) * HEAD].astype(jnp.float32)
                    * share[part][:, h : h + 1]
                )
            attended_ref[:, h * HEAD : (h + 1) * HEAD] = (summed / whole[:, h : h + 1]).astype(
                jnp.bfloat16
            )
        for block in range(block_total):
            copies[block].wait()
            product = jnp.dot(
                attended_ref[...], kept[block], preferred_element_type=jnp.float32
            )
            if added is not None:
                product = product + added_refs[block][...]
            block_refs[block][...] = product.astype(kind)

    vmem = pl.BlockSpec(memory_space=pltpu.VMEM)
    outs = pl.pallas_call(
        kernel,
        out_shape=[jax.ShapeDtypeStruct((own_rows, width), jnp.bfloat16)]
        + [jax.ShapeDtypeStruct((own_rows, own_width), kind)] * block_total,
        in_specs=[pl.BlockSpec(memory_space=pltpu.SMEM), pl.BlockSpec(memory_space=pltpu.HBM)]
        + [vmem] * (part_total + (block_total if added is not None else 0)),
        out_specs=[vmem] * (1 + block_total),
        scratch_shapes=[
            pltpu.VMEM((block_total, width, own_width), jnp.bfloat16),
            pltpu.SemaphoreType.DMA((block_total,)),
        ],
        compiler_params=pltpu.CompilerParams(vmem_limit_bytes=VMEM_BYTES),
        cost_estimate=cost(
            2 * own_rows * width * weight.shape[1],
            2 * width * weight.shape[1],
            part_total * own_rows * HEAD,
        ),
        name="combine_project",
    )(place[None], weight, *every, *(added or ()))
    return outs[0], outs[1:]


def split_terms(value):
    first = value.astype(jnp.bfloat16).astype(jnp.float32)
    second = (value - first).astype(jnp.bfloat16).astype(jnp.float32)
    lane = lax.broadcasted_iota(jnp.int32, value.shape, 1)
    third = jnp.where(lane == 2, value - first - second, 0.0)
    return jnp.where(lane == 0, first, jnp.where(lane == 1, second, third)).astype(jnp.bfloat16)


def gate_up_rows(parts, norm_gain, gate_weight, up_weight, spot, group_total):
    own_rows, features = parts[0].shape
    rows = own_rows * len(parts)
    half = rows // 2
    piece = half // 2
    each = len(parts) // group_total
    units = gate_weight.shape[1]
    tile = units // 2 if (units // 2) % HEAD == 0 else units

    def kernel(spot_ref, gain_ref, gate_ref, up_ref, *refs):
        part_refs = refs[: len(parts)]
        keep_ref, *send_refs, scaled, squares, kept_gate, kept_up, sems = refs[len(parts) :]
        tiles = [
            (ref, kept, base, at)
            for ref, kept, base in ((gate_ref, kept_gate, 0), (up_ref, kept_up, units))
            for at in range(0, units, tile)
        ]
        copies = streamed(
            [
                (ref, kept)
                if tile == units
                else (ref.at[:, pl.ds(at, tile)], kept.at[:, pl.ds(at, tile)])
                for ref, kept, _, at in tiles
            ],
            sems,
        )
        for index, part_ref in enumerate(part_refs):
            at = ((index // each) ^ spot_ref[0]) * each + index % each
            here = pl.ds(pl.multiple_of(at * own_rows, ALIGN), own_rows)
            wide = part_ref[...].astype(jnp.float32)
            scaled[here, :] = (wide * gain_ref[...]).astype(jnp.bfloat16)
            squares[here, :] = jnp.broadcast_to(
                jnp.sum(wide * wide, axis=1, keepdims=True), (own_rows, HEAD)
            )
        for copy, (_, kept, base, at) in zip(copies, tiles):
            copy.wait()
            here = slice(base + at, base + at + tile)
            product = jnp.dot(
                scaled[...], kept[:, at : at + tile], preferred_element_type=jnp.float32
            ).astype(jnp.bfloat16)
            keep_ref[:, here] = product[:half]
            for k, send_ref in enumerate(send_refs):
                send_ref[:, here] = product[half + k * piece : half + (k + 1) * piece]
        terms = split_terms(squares[...])
        keep_ref[:, 2 * units :] = terms[:half]
        for k, send_ref in enumerate(send_refs):
            send_ref[:, 2 * units :] = terms[half + k * piece : half + (k + 1) * piece]

    vmem = pl.BlockSpec(memory_space=pltpu.VMEM)
    keep, *send = pl.pallas_call(
        kernel,
        out_shape=[jax.ShapeDtypeStruct((half, 2 * units + HEAD), jnp.bfloat16)]
        + [jax.ShapeDtypeStruct((piece, 2 * units + HEAD), jnp.bfloat16)] * 2,
        in_specs=[pl.BlockSpec(memory_space=pltpu.SMEM), vmem]
        + [pl.BlockSpec(memory_space=pltpu.HBM)] * 2
        + [vmem] * len(parts),
        out_specs=[vmem] * 3,
        scratch_shapes=[
            pltpu.VMEM((rows, features), jnp.bfloat16),
            pltpu.VMEM((rows, HEAD), jnp.float32),
            pltpu.VMEM((features, units), jnp.bfloat16),
            pltpu.VMEM((features, units), jnp.bfloat16),
            pltpu.SemaphoreType.DMA((2 * units // tile,)),
        ],
        compiler_params=pltpu.CompilerParams(vmem_limit_bytes=VMEM_BYTES),
        cost_estimate=cost(4 * rows * features * units, 4 * features * units, 0),
        name="gate_up",
    )(spot[None], norm_gain[None, :], gate_weight, up_weight, *parts)
    return keep, send


def add_halves(keep, got, units):
    half = keep.shape[0] // 2

    def kernel(keep_ref, low_ref, high_ref, next_ref, send_ref):
        for ref, got_ref, at in ((next_ref, low_ref, 0), (send_ref, high_ref, half)):
            here = pl.ds(at, half)
            ref[:, : 2 * units] = (
                keep_ref[here, : 2 * units].astype(jnp.float32)
                + got_ref[:, : 2 * units].astype(jnp.float32)
            ).astype(jnp.bfloat16)
            terms = keep_ref[here, 2 * units :].astype(jnp.float32)
            terms = terms + got_ref[:, 2 * units :].astype(jnp.float32)
            total = jnp.sum(terms, axis=1, keepdims=True)
            ref[:, 2 * units :] = split_terms(jnp.broadcast_to(total, (half, HEAD)))

    vmem = pl.BlockSpec(memory_space=pltpu.VMEM)
    return pl.pallas_call(
        kernel,
        out_shape=[jax.ShapeDtypeStruct((half, keep.shape[1]), jnp.bfloat16)] * 2,
        in_specs=[vmem] * 3,
        out_specs=[vmem, vmem],
        compiler_params=pltpu.CompilerParams(vmem_limit_bytes=SMALL_BYTES),
        cost_estimate=cost(2 * keep.size, 6 * keep.size, 0),
        name="add_halves",
    )(keep, *got)


def gated(keep, got, units):
    def kernel(keep_ref, got_ref, out_ref):
        summed = keep_ref[...].astype(jnp.float32) + got_ref[...].astype(jnp.float32)
        square = jnp.sum(summed[:, 2 * units :], axis=1, keepdims=True)
        scale = lax.rsqrt(square / D + EPSILON)
        gate = summed[:, :units] * scale
        up = summed[:, units : 2 * units] * scale
        out_ref[...] = (gate / (1.0 + jnp.exp(-gate)) * up).astype(jnp.bfloat16)

    vmem = pl.BlockSpec(memory_space=pltpu.VMEM)
    return pl.pallas_call(
        kernel,
        out_shape=jax.ShapeDtypeStruct((keep.shape[0], units), jnp.bfloat16),
        in_specs=[vmem, vmem],
        out_specs=vmem,
        compiler_params=pltpu.CompilerParams(vmem_limit_bytes=SMALL_BYTES),
        cost_estimate=cost(4 * keep.size, 5 * keep.size, keep.size // 2),
        name="gated",
    )(keep, got)


def down_rows(pieces, down_weight, spot, part_count, own_rows, group_total):
    rows = part_count * own_rows
    each = part_count // group_total
    units, features = down_weight.shape

    def kernel(spot_ref, weight_ref, *refs):
        piece_refs = refs[: len(pieces)]
        out_refs = refs[len(pieces) : len(pieces) + part_count]
        hidden, product = refs[len(pieces) + part_count :]
        at = 0
        for piece_ref in piece_refs:
            hidden[at : at + piece_ref.shape[0], :] = piece_ref[...]
            at += piece_ref.shape[0]
        product[...] = jnp.dot(
            hidden[...], weight_ref[...], preferred_element_type=jnp.float32
        )
        for index, out_ref in enumerate(out_refs):
            at = ((index // each) ^ spot_ref[0]) * each + index % each
            here = pl.ds(pl.multiple_of(at * own_rows, ALIGN), own_rows)
            out_ref[...] = product[here, :].astype(jnp.bfloat16)

    vmem = pl.BlockSpec(memory_space=pltpu.VMEM)
    return pl.pallas_call(
        kernel,
        out_shape=[jax.ShapeDtypeStruct((own_rows, features), jnp.bfloat16)] * part_count,
        in_specs=[pl.BlockSpec(memory_space=pltpu.SMEM)] + [vmem] * (1 + len(pieces)),
        out_specs=[vmem] * part_count,
        scratch_shapes=[
            pltpu.VMEM((rows, units), jnp.bfloat16),
            pltpu.VMEM((rows, features), jnp.float32),
        ],
        compiler_params=pltpu.CompilerParams(vmem_limit_bytes=SMALL_BYTES),
        cost_estimate=cost(2 * rows * features * units, 2 * features * units, 0),
        name="down",
    )(spot[None], down_weight, *pieces)


def swap(value, axis_name, mask):
    axis_total = lax.axis_size(axis_name)
    return lax.ppermute(value, axis_name, [(j, j ^ mask) for j in range(axis_total)])


def after(value, token):
    return lax.optimization_barrier((value, token))[0]


def gather_parts(value, axis_name, token=None):
    parts = [value] * lax.axis_size(axis_name)
    for mask in range(len(parts) - 2, 0, -2):
        parts[mask] = swap(value, axis_name, mask)
    for mask in [0] + list(range(len(parts) - 2, 0, -2)):
        held = parts[mask] if token is None or mask == 0 else after(parts[mask], token)
        parts[mask + 1] = swap(held, axis_name, 1)
    return parts


def pair_sums(parts, axis_name):
    evens = sorted((mask for mask in parts if mask % 2 == 0), reverse=True)
    got = {mask: swap(parts[mask + 1], axis_name, 1) for mask in evens}
    pairs = {
        mask: parts[mask].astype(jnp.float32) + got[mask].astype(jnp.float32) for mask in evens
    }
    return {mask: pair.astype(jnp.bfloat16) if mask else pair for mask, pair in pairs.items()}


def far_sum(pairs, axis_name):
    summed = 0.0
    for mask, pair in pairs.items():
        summed = summed + (swap(pair, axis_name, mask).astype(jnp.float32) if mask else pair)
    return summed


def scatter_sum(parts, axis_name):
    return far_sum(pair_sums(parts, axis_name), axis_name)


def shards(
    queries,
    root_cache,
    mid_cache,
    leaf_cache,
    token_leaf,
    leaf_parent,
    mid_parent,
    root_len,
    mid_len,
    leaf_len,
    root_slot,
    mid_slot,
    leaf_slot,
    stream,
    out_weight,
    norm_gain,
    gate_weight,
    up_weight,
    down_weight,
):
    own_rows, width = queries.shape
    owner = lax.axis_index("kv").astype(jnp.int32)
    caches = (root_cache, mid_cache, leaf_cache)
    nodes = own_nodes(
        owner,
        [cache.shape[0] for cache in caches],
        (token_leaf, leaf_parent, mid_parent),
        (root_len, mid_len, leaf_len),
        (root_slot, mid_slot, leaf_slot),
    )
    kv_count = root_cache.shape[2] // (2 * HEAD)
    group_width = width // kv_count
    mlp_total = lax.axis_size("mlp")
    mlp_place = lax.axis_index("mlp").astype(jnp.int32)
    own_width = stream.shape[1]
    query_parts = gather_parts(queries, "kv")
    attended, blocks = [], None
    for k in range(kv_count):
        near, far = tree_attention(query_parts, caches, nodes, owner, k)
        merged = merge_pairs(near, swap(far, "kv", 1))
        every = [swap(one, "kv", 2 * pair) if pair else one for pair, one in enumerate(merged)]
        one, blocks = combine_project(
            every, out_weight, k * group_width, blocks, mlp_place, own_width
        )
        attended.append(one)
    projected = scatter_sum(dict(enumerate(blocks)), "mlp")
    residual = (stream.astype(jnp.float32) + projected).astype(jnp.bfloat16)
    steps = [1 << bit for bit in range(mlp_total.bit_length() - 1)]
    spot = jnp.int32(0)
    for step in steps:
        spot = 2 * spot + (mlp_place // step) % 2
    units = gate_weight.shape[1]
    row_parts = gather_parts(residual, "kv")
    first, second = (
        [mask for mask in range(len(row_parts)) if (mask // 2) % 2 == side] for side in range(2)
    )
    row_parts[0] = after(row_parts[0], [row_parts[mask] for mask in second if mask % 2 == 0])

    def multiply(masks):
        parts = [row_parts[mask] for mask in masks]
        return gate_up_rows(parts, norm_gain, gate_weight, up_weight, spot, mlp_total)

    def reduce_once(keep, send, token=None):
        for step in steps[:-1]:
            if step > 1:
                send = jnp.split(send, 2, axis=0)
            got = [swap(piece, "mlp", step) for piece in send]
            if token is not None and step == 1:
                keep = after(keep, token)
            keep, send = add_halves(keep, got, units)
        return keep, send

    def regather(hidden, token):
        pieces = [hidden]
        for step in reversed(steps):
            pieces += [
                swap(piece if k == 0 or step == steps[-1] else after(piece, token), "mlp", step)
                for k, piece in enumerate(pieces)
            ]
        return pieces

    def finish(pieces, masks):
        outs = down_rows(pieces, down_weight, spot, len(masks), own_rows, mlp_total)
        return dict(zip(masks, outs))

    keep, send = reduce_once(*multiply(first))
    row_parts[second[0]] = after(row_parts[second[0]], send)
    later = multiply(second)
    hidden = gated(after(keep, later[0]), swap(send, "mlp", steps[-1]), units)
    keep, send = reduce_once(*later, hidden)
    pairs = pair_sums(finish(regather(hidden, send), first), "kv")
    keep = after(keep, pairs[0])
    hidden = gated(keep, swap(send, "mlp", steps[-1]), units)
    mixed = far_sum(pairs, "kv")
    late = finish(regather(hidden, mixed), second)
    for mask in sorted(late, reverse=True):
        mixed = mixed + swap(late[mask], "kv", mask).astype(jnp.float32)
    return (jnp.concatenate(attended, axis=1), mixed.astype(jnp.bfloat16))


def solution(mesh):
    in_specs = (
        P("kv", "mlp"),
        P("kv", None, "mlp"),
        P("kv", None, "mlp"),
        P("kv", None, "mlp"),
        P(),
        P(),
        P(),
        P(),
        P(),
        P(),
        P(),
        P(),
        P(),
        P("kv", "mlp"),
        P("mlp", None),
        P("mlp"),
        P("mlp", "kv"),
        P("mlp", "kv"),
        P("kv", "mlp"),
    )
    out_specs = (P("kv", "mlp"), P("kv", "mlp"))
    return jax.shard_map(shards, mesh=mesh, in_specs=in_specs, out_specs=out_specs, check_vma=False)
```

```python
import math

import jax
import jax.numpy as jnp
from jax import lax
from jax.experimental import pallas as pl
from jax.experimental.pallas import tpu as pltpu
from jax.sharding import PartitionSpec as P

D = 4096
HEAD = 128
QLEAF = 16
QMID = 48
QROOT = 144


LOWEST = -1e30
EPSILON = 1e-05
ALIGN = 16
BLOCK = 512
VMEM_BYTES = 50 << 20
SMALL_BYTES = 24 << 20


def cost(flops, moved, exps):
    return pl.CostEstimate(flops=flops, bytes_accessed=moved, transcendentals=exps)


def streamed(pairs, sems):
    copies = [
        pltpu.make_async_copy(source, target, sems.at[k]) for k, (source, target) in enumerate(pairs)
    ]
    for copy in copies:
        copy.start()
    return copies


def own_nodes(owner, local_counts, tree, lengths, slots):
    token_leaf, leaf_parent, mid_parent = tree
    node_total = sum(local_counts)

    def kernel(owner_ref, token_ref, leaf_up, mid_up, *refs):
        len_refs, slot_refs, out_ref = refs[:3], refs[3:6], refs[6]

        def find(slot_ref, len_ref, local):
            base = owner_ref[0] * local

            def step(j, found):
                at, size = slot_ref[j] - base, len_ref[j]
                return tuple(
                    (jnp.where(at == k, j, node), jnp.where(at == k, size, length))
                    for k, (node, length) in enumerate(found)
                )

            zero = jnp.int32(0)
            return lax.fori_loop(0, slot_ref.shape[0], step, ((zero, zero),) * local)

        def below(parent_ref, edges):
            def step(j, counted):
                parent = parent_ref[j]
                return tuple(
                    c + jnp.where(parent < edge, 1, 0) for c, edge in zip(counted, edges)
                )

            return lax.fori_loop(0, parent_ref.shape[0], step, (jnp.int32(0),) * len(edges))

        picked = [find(*level) for level in zip(slot_refs, len_refs, local_counts)]
        edges = ()
        for level, parent_ref in enumerate((mid_up, leaf_up, None)):
            for node, _ in picked[level]:
                edges += (node, node + 1)
            if parent_ref is not None:
                edges = below(parent_ref, edges)
        tokens = token_ref[...]
        sizes = [length for level in picked for _, length in level]
        for k in range(node_total):
            for side in range(2):
                under = jnp.where(tokens < edges[2 * k + side], 1.0, 0.0)
                out_ref[side, k] = jnp.sum(under).astype(jnp.int32)
            out_ref[2, k] = sizes[k]

    smem = pl.BlockSpec(memory_space=pltpu.SMEM)
    vmem = pl.BlockSpec(memory_space=pltpu.VMEM)
    return pl.pallas_call(
        kernel,
        out_shape=jax.ShapeDtypeStruct((3, node_total), jnp.int32),
        in_specs=[smem, vmem] + [smem] * 8,
        out_specs=smem,
        name="own_nodes",
    )(owner[None], token_leaf.reshape(-1, HEAD), leaf_parent, mid_parent, *lengths, *slots)


def tree_attention(query_parts, caches, nodes, owner, kv_head):
    part_total = len(query_parts)
    own_rows = query_parts[0].shape[0]
    total_rows = part_total * own_rows
    width = query_parts[0].shape[1] // (caches[0].shape[2] // (2 * HEAD))
    group_size = width // HEAD
    score_scale = 1.0 / math.sqrt(HEAD)
    levels = []
    for cache, capacity in zip(caches, (QROOT, QMID, QLEAF)):
        levels.append((cache.shape[0], cache.shape[1], min(capacity + ALIGN, total_rows)))

    def kernel(nodes_ref, owner_ref, *refs):
        query_refs = refs[:part_total]
        cache_refs = refs[part_total : part_total + 3]
        near_ref, far_ref, all_rows, run_out, run_lse, acc, peak, total, *rest = refs[
            part_total + 3 :
        ]
        kept_refs, sems = rest[:3], rest[3]
        columns = pl.ds(kv_head * 2 * HEAD, 2 * HEAD)
        starts = [0, levels[0][0], levels[0][0] + levels[1][0]]
        lengths, flag_starts, flag = [], [], 0
        for start, (slot_total, span, _) in zip(starts, levels):
            lengths.append([nodes_ref[2, start + member] for member in range(slot_total)])
            flag_starts.append(flag)
            flag += slot_total * (span // min(BLOCK, span))

        def block_copy(level, member, index):
            span = levels[level][1]
            block = min(BLOCK, span)
            at = index * block
            here = pl.ds(at if isinstance(at, int) else pl.multiple_of(at, block), block)
            return pltpu.make_async_copy(
                cache_refs[level].at[member, here, columns],
                kept_refs[level].at[member, here, :],
                sems.at[flag_starts[level] + member * (span // block) + index],
            )

        steps = []
        for level, (slot_total, span, _) in enumerate(levels):
            block = min(BLOCK, span)
            pair = min(2 * block, span)
            longest = lengths[level][0]
            shortest = lengths[level][0]
            for length in lengths[level][1:]:
                longest, shortest = jnp.maximum(longest, length), jnp.minimum(shortest, length)
            whole, most = lax.div(shortest, pair), lax.div(longest + pair - 1, pair)
            steps.append((block, pair, whole, most))
            for index in range(span // pair):

                @pl.when(index < most)
                def _(level=level, index=index, ratio=pair // block, slot_total=slot_total):
                    for piece in range(ratio):
                        for member in range(slot_total):
                            block_copy(level, member, index * ratio + piece).start()

        me = owner_ref[0]
        for part in range(part_total):
            row = pl.multiple_of((me ^ part) * own_rows, ALIGN)
            all_rows[pl.ds(row, own_rows), :] = query_refs[part][
                :, kv_head * width : (kv_head + 1) * width
            ]
        run_out[...] = jnp.zeros_like(run_out)
        run_lse[...] = jnp.full_like(run_lse, LOWEST)
        offsets = [h * HEAD for h in range(group_size)]
        for level, (slot_total, span, rows) in enumerate(levels):
            block, pair, whole, most = steps[level]
            lanes = rows * group_size
            every = lanes * slot_total
            windows, grouped = [], []
            for member in range(slot_total):
                low = nodes_ref[0, starts[level] + member]
                window = jnp.minimum(low - lax.rem(low, ALIGN), total_rows - rows)
                window = pl.multiple_of(window, ALIGN)
                windows.append(window)
                grouped.append(
                    jnp.concatenate(
                        [all_rows[pl.ds(window, rows), c : c + HEAD] for c in offsets], axis=0
                    )
                )
            lane_of = lax.broadcasted_iota(jnp.int32, (1, every), 1)
            limits = jnp.full((1, every), lengths[level][0], jnp.int32)
            for member in range(1, slot_total):
                limits = jnp.where(lane_of >= member * lanes, lengths[level][member], limits)
            acc[:, :every] = jnp.zeros((HEAD, every), jnp.float32)
            peak[:, :every] = jnp.full((1, every), LOWEST, jnp.float32)
            total[:, :every] = jnp.zeros((1, every), jnp.float32)

            def visit(index, carry, masked):
                ratio = pair // block
                for piece in range(ratio):
                    for member in range(slot_total):
                        block_copy(level, member, index * ratio + piece).wait()
                scores = []
                for piece in range(ratio):
                    at = pl.multiple_of((index * ratio + piece) * block, block)
                    found = [
                        lax.dot_general(
                            kept_refs[level][member, pl.ds(at, block), :HEAD],
                            grouped[member],
                            (((1,), (1,)), ((), ())),
                            preferred_element_type=jnp.float32,
                        )
                        for member in range(slot_total)
                    ]
                    found = found[0] if slot_total == 1 else jnp.concatenate(found, axis=1)
                    if masked:
                        position = lax.broadcasted_iota(jnp.int32, (block, every), 0)
                        found = jnp.where(position < limits - at, found, LOWEST)
                    scores.append((at, found))
                for at, found in scores:
                    old_peak = peak[:, :every]
                    new_peak = jnp.maximum(old_peak, jnp.max(found, axis=0, keepdims=True))
                    weights = jnp.exp((found - new_peak) * score_scale)
                    fade = jnp.exp((old_peak - new_peak) * score_scale)
                    peak[:, :every] = new_peak
                    total[:, :every] = total[:, :every] * fade + jnp.sum(
                        weights, axis=0, keepdims=True
                    )
                    rounded = weights.astype(jnp.bfloat16)
                    for member in range(slot_total):
                        here = slice(member * lanes, (member + 1) * lanes)
                        acc[:, here] = acc[:, here] * fade[:, here] + lax.dot_general(
                            kept_refs[level][member, pl.ds(at, block), HEAD:],
                            rounded[:, here],
                            (((0,), (0,)), ((), ())),
                            preferred_element_type=jnp.float32,
                        )
                return carry

            lax.fori_loop(0, whole, lambda i, c: visit(i, c, False), 0)
            lax.fori_loop(whole, most, lambda i, c: visit(i, c, True), 0)

            weight_sum = total[:, :every]
            part_out = (acc[:, :every] / weight_sum).T
            part_lse = jnp.broadcast_to(
                peak[:, :every] * score_scale + jnp.log(weight_sum), (HEAD, every)
            ).T
            for member, window in enumerate(windows):
                low = nodes_ref[0, starts[level] + member]
                high = nodes_ref[1, starts[level] + member]
                position = window + lax.broadcasted_iota(jnp.int32, (rows, HEAD), 0)
                live = (position >= low) & (position < high)
                for h, c in enumerate(offsets):
                    here = (pl.ds(window, rows), slice(c, c + HEAD))
                    old_lse, old_out = run_lse[here], run_out[here]
                    at = member * lanes + h * rows
                    add_lse = part_lse[at : at + rows]
                    add_out = part_out[at : at + rows]
                    if level == 0:
                        run_out[here] = jnp.where(live, add_out, old_out)
                        run_lse[here] = jnp.where(live, add_lse, old_lse)
                        continue
                    best = jnp.maximum(old_lse, add_lse)
                    old_share = jnp.exp(old_lse - best)
                    add_share = jnp.exp(add_lse - best)
                    share = old_share + add_share
                    run_out[here] = jnp.where(
                        live, (old_out * old_share + add_out * add_share) / share, old_out
                    )
                    run_lse[here] = jnp.where(live, best + jnp.log(share), old_lse)
        lane = lax.broadcasted_iota(jnp.int32, (own_rows, HEAD), 1)
        for part in range(part_total):
            out_ref = far_ref if part % 2 else near_ref
            here = pl.ds(pl.multiple_of((me ^ part) * own_rows, ALIGN), own_rows)
            out_ref[part // 2, :, :width] = run_out[here, :].astype(jnp.bfloat16)
            lse = jnp.zeros((own_rows, HEAD), jnp.float32)
            for h in range(group_size):
                piece = run_lse[here, h * HEAD : (h + 1) * HEAD]
                lse = jnp.where(lax.rem(lane, group_size) == h, piece, lse)
            out_ref[part // 2, :, width:] = lse_terms(lse, lane, group_size)

    block_total = sum(count * (span // min(BLOCK, span)) for count, span, _ in levels)
    most = max(count * rows for count, _, rows in levels) * group_size
    vmem = pl.BlockSpec(memory_space=pltpu.VMEM)
    smem = pl.BlockSpec(memory_space=pltpu.SMEM)
    return pl.pallas_call(
        kernel,
        out_shape=[
            jax.ShapeDtypeStruct((part_total // 2, own_rows, width + HEAD), jnp.bfloat16)
        ]
        * 2,
        in_specs=[smem, smem]
        + [vmem] * part_total
        + [pl.BlockSpec(memory_space=pltpu.HBM)] * 3,
        out_specs=[vmem, vmem],
        scratch_shapes=[
            pltpu.VMEM((total_rows, width), jnp.bfloat16),
            pltpu.VMEM((total_rows, width), jnp.float32),
            pltpu.VMEM((total_rows, width), jnp.float32),
            pltpu.VMEM((HEAD, most), jnp.float32),
            pltpu.VMEM((1, most), jnp.float32),
            pltpu.VMEM((1, most), jnp.float32),
        ]
        + [pltpu.VMEM((count, span, 2 * HEAD), jnp.bfloat16) for count, span, _ in levels]
        + [pltpu.SemaphoreType.DMA((block_total,))],
        compiler_params=pltpu.CompilerParams(vmem_limit_bytes=VMEM_BYTES),
        cost_estimate=cost(
            4 * HEAD * group_size * sum(c * span * rows for c, span, rows in levels),
            2 * 2 * HEAD * sum(count * span for count, span, _ in levels),
            group_size * sum(c * span * rows for c, span, rows in levels),
        ),
        name="tree_attention",
    )(nodes, owner[None], *query_parts, *caches)


def lse_of(packed, group_size):
    terms = packed.astype(jnp.float32)
    return (
        terms
        + pltpu.roll(terms, HEAD - group_size, 1)
        + pltpu.roll(terms, HEAD - 2 * group_size, 1)
    )


def lse_terms(lse, lane, group_size):
    first = lse.astype(jnp.bfloat16).astype(jnp.float32)
    second = (lse - first).astype(jnp.bfloat16).astype(jnp.float32)
    third = lse - first - second
    field = lax.div(lane, group_size)
    packed = jnp.where(field == 2, third, 0.0)
    packed = jnp.where(field == 1, second, packed)
    return jnp.where(field == 0, first, packed).astype(jnp.bfloat16)


def merge_pairs(near, got):
    pair_total, own_rows, wide = near.shape
    width = wide - HEAD
    group_size = width // HEAD

    def kernel(near_ref, got_ref, *out_refs):
        lane = lax.broadcasted_iota(jnp.int32, (own_rows, HEAD), 1)
        for k, out_ref in enumerate(out_refs):
            left = lse_of(near_ref[k, :, width:], group_size)
            right = lse_of(got_ref[k, :, width:], group_size)
            best = jnp.maximum(left, right)
            left, right = jnp.exp(left - best), jnp.exp(right - best)
            whole = left + right
            left, right = left / whole, right / whole
            for h in range(group_size):
                here = slice(h * HEAD, (h + 1) * HEAD)
                out_ref[:, here] = (
                    near_ref[k, :, here].astype(jnp.float32) * left[:, h : h + 1]
                    + got_ref[k, :, here].astype(jnp.float32) * right[:, h : h + 1]
                ).astype(jnp.bfloat16)
            lse = jnp.where(lane < group_size, best + jnp.log(whole), 0.0)
            lse = lse + pltpu.roll(lse, group_size, 1) + pltpu.roll(lse, 2 * group_size, 1)
            out_ref[:, width:] = lse_terms(lse, lane, group_size)

    vmem = pl.BlockSpec(memory_space=pltpu.VMEM)
    return pl.pallas_call(
        kernel,
        out_shape=[jax.ShapeDtypeStruct((own_rows, wide), jnp.bfloat16)] * pair_total,
        in_specs=[vmem, vmem],
        out_specs=[vmem] * pair_total,
        compiler_params=pltpu.CompilerParams(vmem_limit_bytes=SMALL_BYTES),
        cost_estimate=cost(4 * near.size, 6 * near.size, pair_total * own_rows * 2 * HEAD),
        name="merge_pairs",
    )(near, got)


def combine_project(every, weight, row_start, added, place, own_width):
    part_total = len(every)
    own_rows, wide = every[0].shape
    width = wide - HEAD
    group_size = width // HEAD
    block_total = weight.shape[1] // own_width
    last = added is not None or width == weight.shape[0]
    kind = jnp.bfloat16 if last else jnp.float32

    def kernel(place_ref, weight_ref, *refs):
        every_refs, refs = refs[:part_total], refs[part_total:]
        added_refs = refs[:block_total] if added is not None else (None,) * block_total
        attended_ref, *block_refs = refs[len(refs) - 3 - block_total : -2]
        kept, sems = refs[-2:]
        columns = [
            pl.ds(pl.multiple_of((place_ref[0] ^ block) * own_width, HEAD), own_width)
            for block in range(block_total)
        ]
        copies = streamed(
            [
                (weight_ref.at[pl.ds(row_start, width), column], kept.at[block])
                for block, column in enumerate(columns)
            ],
            sems,
        )
        lse = [lse_of(ref[:, width:], group_size) for ref in every_refs]
        best = lse[0]
        for one in lse[1:]:
            best = jnp.maximum(best, one)
        share = [jnp.exp(one - best) for one in lse]
        whole = share[0]
        for one in share[1:]:
            whole = whole + one
        for h in range(group_size):
            summed = jnp.zeros((own_rows, HEAD), jnp.float32)
            for part in range(part_total):
                summed = summed + (
                    every_refs[part][:, h * HEAD : (h + 1) * HEAD].astype(jnp.float32)
                    * share[part][:, h : h + 1]
                )
            attended_ref[:, h * HEAD : (h + 1) * HEAD] = (summed / whole[:, h : h + 1]).astype(
                jnp.bfloat16
            )
        for block in range(block_total):
            copies[block].wait()
            product = jnp.dot(
                attended_ref[...], kept[block], preferred_element_type=jnp.float32
            )
            if added is not None:
                product = product + added_refs[block][...]
            block_refs[block][...] = product.astype(kind)

    vmem = pl.BlockSpec(memory_space=pltpu.VMEM)
    outs = pl.pallas_call(
        kernel,
        out_shape=[jax.ShapeDtypeStruct((own_rows, width), jnp.bfloat16)]
        + [jax.ShapeDtypeStruct((own_rows, own_width), kind)] * block_total,
        in_specs=[pl.BlockSpec(memory_space=pltpu.SMEM), pl.BlockSpec(memory_space=pltpu.HBM)]
        + [vmem] * (part_total + (block_total if added is not None else 0)),
        out_specs=[vmem] * (1 + block_total),
        scratch_shapes=[
            pltpu.VMEM((block_total, width, own_width), jnp.bfloat16),
            pltpu.SemaphoreType.DMA((block_total,)),
        ],
        compiler_params=pltpu.CompilerParams(vmem_limit_bytes=VMEM_BYTES),
        cost_estimate=cost(
            2 * own_rows * width * weight.shape[1],
            2 * width * weight.shape[1],
            part_total * own_rows * HEAD,
        ),
        name="combine_project",
    )(place[None], weight, *every, *(added or ()))
    return outs[0], outs[1:]


def split_terms(value):
    first = value.astype(jnp.bfloat16).astype(jnp.float32)
    second = (value - first).astype(jnp.bfloat16).astype(jnp.float32)
    lane = lax.broadcasted_iota(jnp.int32, value.shape, 1)
    third = jnp.where(lane == 2, value - first - second, 0.0)
    return jnp.where(lane == 0, first, jnp.where(lane == 1, second, third)).astype(jnp.bfloat16)


def gate_up_rows(parts, norm_gain, gate_weight, up_weight, spot, group_total):
    own_rows, features = parts[0].shape
    rows = own_rows * len(parts)
    half = rows // 2
    piece = half // 2
    each = len(parts) // group_total
    units = gate_weight.shape[1]
    tile = units // 2 if (units // 2) % HEAD == 0 else units

    def kernel(spot_ref, gain_ref, gate_ref, up_ref, *refs):
        part_refs = refs[: len(parts)]
        keep_ref, *send_refs, scaled, squares, kept_gate, kept_up, sems = refs[len(parts) :]
        tiles = [
            (ref, kept, base, at)
            for ref, kept, base in ((gate_ref, kept_gate, 0), (up_ref, kept_up, units))
            for at in range(0, units, tile)
        ]
        copies = streamed(
            [
                (ref, kept)
                if tile == units
                else (ref.at[:, pl.ds(at, tile)], kept.at[:, pl.ds(at, tile)])
                for ref, kept, _, at in tiles
            ],
            sems,
        )
        for index, part_ref in enumerate(part_refs):
            at = ((index // each) ^ spot_ref[0]) * each + index % each
            here = pl.ds(pl.multiple_of(at * own_rows, ALIGN), own_rows)
            wide = part_ref[...].astype(jnp.float32)
            scaled[here, :] = (wide * gain_ref[...]).astype(jnp.bfloat16)
            squares[here, :] = jnp.broadcast_to(
                jnp.sum(wide * wide, axis=1, keepdims=True), (own_rows, HEAD)
            )
        for copy, (_, kept, base, at) in zip(copies, tiles):
            copy.wait()
            here = slice(base + at, base + at + tile)
            product = jnp.dot(
                scaled[...], kept[:, at : at + tile], preferred_element_type=jnp.float32
            ).astype(jnp.bfloat16)
            keep_ref[:, here] = product[:half]
            for k, send_ref in enumerate(send_refs):
                send_ref[:, here] = product[half + k * piece : half + (k + 1) * piece]
        terms = split_terms(squares[...])
        keep_ref[:, 2 * units :] = terms[:half]
        for k, send_ref in enumerate(send_refs):
            send_ref[:, 2 * units :] = terms[half + k * piece : half + (k + 1) * piece]

    vmem = pl.BlockSpec(memory_space=pltpu.VMEM)
    keep, *send = pl.pallas_call(
        kernel,
        out_shape=[jax.ShapeDtypeStruct((half, 2 * units + HEAD), jnp.bfloat16)]
        + [jax.ShapeDtypeStruct((piece, 2 * units + HEAD), jnp.bfloat16)] * 2,
        in_specs=[pl.BlockSpec(memory_space=pltpu.SMEM), vmem]
        + [pl.BlockSpec(memory_space=pltpu.HBM)] * 2
        + [vmem] * len(parts),
        out_specs=[vmem] * 3,
        scratch_shapes=[
            pltpu.VMEM((rows, features), jnp.bfloat16),
            pltpu.VMEM((rows, HEAD), jnp.float32),
            pltpu.VMEM((features, units), jnp.bfloat16),
            pltpu.VMEM((features, units), jnp.bfloat16),
            pltpu.SemaphoreType.DMA((2 * units // tile,)),
        ],
        compiler_params=pltpu.CompilerParams(vmem_limit_bytes=VMEM_BYTES),
        cost_estimate=cost(4 * rows * features * units, 4 * features * units, 0),
        name="gate_up",
    )(spot[None], norm_gain[None, :], gate_weight, up_weight, *parts)
    return keep, send


def add_halves(keep, got, units):
    half = keep.shape[0] // 2

    def kernel(keep_ref, low_ref, high_ref, next_ref, send_ref):
        for ref, got_ref, at in ((next_ref, low_ref, 0), (send_ref, high_ref, half)):
            here = pl.ds(at, half)
            ref[:, : 2 * units] = (
                keep_ref[here, : 2 * units].astype(jnp.float32)
                + got_ref[:, : 2 * units].astype(jnp.float32)
            ).astype(jnp.bfloat16)
            terms = keep_ref[here, 2 * units :].astype(jnp.float32)
            terms = terms + got_ref[:, 2 * units :].astype(jnp.float32)
            total = jnp.sum(terms, axis=1, keepdims=True)
            ref[:, 2 * units :] = split_terms(jnp.broadcast_to(total, (half, HEAD)))

    vmem = pl.BlockSpec(memory_space=pltpu.VMEM)
    return pl.pallas_call(
        kernel,
        out_shape=[jax.ShapeDtypeStruct((half, keep.shape[1]), jnp.bfloat16)] * 2,
        in_specs=[vmem] * 3,
        out_specs=[vmem, vmem],
        compiler_params=pltpu.CompilerParams(vmem_limit_bytes=SMALL_BYTES),
        cost_estimate=cost(2 * keep.size, 6 * keep.size, 0),
        name="add_halves",
    )(keep, *got)


def gated(keep, got, units):
    def kernel(keep_ref, got_ref, out_ref):
        summed = keep_ref[...].astype(jnp.float32) + got_ref[...].astype(jnp.float32)
        square = jnp.sum(summed[:, 2 * units :], axis=1, keepdims=True)
        scale = lax.rsqrt(square / D + EPSILON)
        gate = summed[:, :units] * scale
        up = summed[:, units : 2 * units] * scale
        out_ref[...] = (gate / (1.0 + jnp.exp(-gate)) * up).astype(jnp.bfloat16)

    vmem = pl.BlockSpec(memory_space=pltpu.VMEM)
    return pl.pallas_call(
        kernel,
        out_shape=jax.ShapeDtypeStruct((keep.shape[0], units), jnp.bfloat16),
        in_specs=[vmem, vmem],
        out_specs=vmem,
        compiler_params=pltpu.CompilerParams(vmem_limit_bytes=SMALL_BYTES),
        cost_estimate=cost(4 * keep.size, 5 * keep.size, keep.size // 2),
        name="gated",
    )(keep, got)


def down_rows(pieces, down_weight, spot, part_count, own_rows, group_total):
    rows = part_count * own_rows
    each = part_count // group_total
    units, features = down_weight.shape

    def kernel(spot_ref, weight_ref, *refs):
        piece_refs = refs[: len(pieces)]
        out_refs = refs[len(pieces) : len(pieces) + part_count]
        hidden, product = refs[len(pieces) + part_count :]
        at = 0
        for piece_ref in piece_refs:
            hidden[at : at + piece_ref.shape[0], :] = piece_ref[...]
            at += piece_ref.shape[0]
        product[...] = jnp.dot(
            hidden[...], weight_ref[...], preferred_element_type=jnp.float32
        )
        for index, out_ref in enumerate(out_refs):
            at = ((index // each) ^ spot_ref[0]) * each + index % each
            here = pl.ds(pl.multiple_of(at * own_rows, ALIGN), own_rows)
            out_ref[...] = product[here, :].astype(jnp.bfloat16)

    vmem = pl.BlockSpec(memory_space=pltpu.VMEM)
    return pl.pallas_call(
        kernel,
        out_shape=[jax.ShapeDtypeStruct((own_rows, features), jnp.bfloat16)] * part_count,
        in_specs=[pl.BlockSpec(memory_space=pltpu.SMEM)] + [vmem] * (1 + len(pieces)),
        out_specs=[vmem] * part_count,
        scratch_shapes=[
            pltpu.VMEM((rows, units), jnp.bfloat16),
            pltpu.VMEM((rows, features), jnp.float32),
        ],
        compiler_params=pltpu.CompilerParams(vmem_limit_bytes=SMALL_BYTES),
        cost_estimate=cost(2 * rows * features * units, 2 * features * units, 0),
        name="down",
    )(spot[None], down_weight, *pieces)


def swap(value, axis_name, mask):
    axis_total = lax.axis_size(axis_name)
    return lax.ppermute(value, axis_name, [(j, j ^ mask) for j in range(axis_total)])


def after(value, token):
    return lax.optimization_barrier((value, token))[0]


def gather_parts(value, axis_name, token=None):
    parts = [value] * lax.axis_size(axis_name)
    for mask in range(len(parts) - 2, 0, -2):
        parts[mask] = swap(value, axis_name, mask)
    for mask in [0] + list(range(len(parts) - 2, 0, -2)):
        held = parts[mask] if token is None or mask == 0 else after(parts[mask], token)
        parts[mask + 1] = swap(held, axis_name, 1)
    return parts


def shards(
    queries,
    root_cache,
    mid_cache,
    leaf_cache,
    token_leaf,
    leaf_parent,
    mid_parent,
    root_len,
    mid_len,
    leaf_len,
    root_slot,
    mid_slot,
    leaf_slot,
    stream,
    out_weight,
    norm_gain,
    gate_weight,
    up_weight,
    down_weight,
):
    own_rows, width = queries.shape
    owner = lax.axis_index("kv").astype(jnp.int32)
    caches = (root_cache, mid_cache, leaf_cache)
    nodes = own_nodes(
        owner,
        [cache.shape[0] for cache in caches],
        (token_leaf, leaf_parent, mid_parent),
        (root_len, mid_len, leaf_len),
        (root_slot, mid_slot, leaf_slot),
    )
    kv_count = root_cache.shape[2] // (2 * HEAD)
    group_width = width // kv_count
    mlp_total = lax.axis_size("mlp")
    mlp_place = lax.axis_index("mlp").astype(jnp.int32)
    own_width = stream.shape[1]
    query_parts = gather_parts(queries, "kv")
    attended, blocks = [], None
    for k in range(kv_count):
        near, far = tree_attention(query_parts, caches, nodes, owner, k)
        merged = merge_pairs(near, swap(far, "kv", 1))
        every = [swap(one, "kv", 2 * pair) if pair else one for pair, one in enumerate(merged)]
        one, blocks = combine_project(
            every, out_weight, k * group_width, blocks, mlp_place, own_width
        )
        attended.append(one)
    projected = blocks[0].astype(jnp.float32)
    for mask in range(mlp_total - 1, 0, -1):
        projected = projected + swap(blocks[mask], "mlp", mask).astype(jnp.float32)
    residual = (stream.astype(jnp.float32) + projected).astype(jnp.bfloat16)
    steps = [1 << bit for bit in range(mlp_total.bit_length() - 1)]
    spot = jnp.int32(0)
    for step in steps:
        spot = 2 * spot + (mlp_place // step) % 2
    units = gate_weight.shape[1]
    row_parts = gather_parts(residual, "kv")
    first, second = (
        [mask for mask in range(len(row_parts)) if (mask // 2) % 2 == side] for side in range(2)
    )
    row_parts[0] = after(row_parts[0], [row_parts[mask] for mask in second if mask % 2 == 0])

    def multiply(masks):
        parts = [row_parts[mask] for mask in masks]
        return gate_up_rows(parts, norm_gain, gate_weight, up_weight, spot, mlp_total)

    def reduce_once(keep, send, token=None):
        for step in steps[:-1]:
            if step > 1:
                send = jnp.split(send, 2, axis=0)
            got = [swap(piece, "mlp", step) for piece in send]
            if token is not None and step == 1:
                keep = after(keep, token)
            keep, send = add_halves(keep, got, units)
        return keep, send

    def regather(hidden, token):
        pieces = [hidden]
        for step in reversed(steps):
            pieces += [
                swap(piece if k == 0 or step == steps[-1] else after(piece, token), "mlp", step)
                for k, piece in enumerate(pieces)
            ]
        return pieces

    def finish(pieces, masks):
        outs = down_rows(pieces, down_weight, spot, len(masks), own_rows, mlp_total)
        return dict(zip(masks, outs))

    keep, send = reduce_once(*multiply(first))
    row_parts[second[0]] = after(row_parts[second[0]], send)
    later = multiply(second)
    hidden = gated(after(keep, later[0]), swap(send, "mlp", steps[-1]), units)
    keep, send = reduce_once(*later, hidden)
    early = finish(regather(hidden, send), first)
    keep = after(keep, early[0])
    hidden = gated(keep, swap(send, "mlp", steps[-1]), units)
    mixed = early[0].astype(jnp.float32)
    for mask in first[:0:-1]:
        mixed = mixed + swap(early[mask], "kv", mask).astype(jnp.float32)
    late = finish(regather(hidden, mixed), second)
    for mask in sorted(late, reverse=True):
        mixed = mixed + swap(late[mask], "kv", mask).astype(jnp.float32)
    return (jnp.concatenate(attended, axis=1), mixed.astype(jnp.bfloat16))


def solution(mesh):
    in_specs = (
        P("kv", "mlp"),
        P("kv", None, "mlp"),
        P("kv", None, "mlp"),
        P("kv", None, "mlp"),
        P(),
        P(),
        P(),
        P(),
        P(),
        P(),
        P(),
        P(),
        P(),
        P("kv", "mlp"),
        P("mlp", None),
        P("mlp"),
        P("mlp", "kv"),
        P("mlp", "kv"),
        P("kv", "mlp"),
    )
    out_specs = (P("kv", "mlp"), P("kv", "mlp"))
    return jax.shard_map(shards, mesh=mesh, in_specs=in_specs, out_specs=out_specs, check_vma=False)
```

```python
import math

import jax
import jax.numpy as jnp
from jax import lax
from jax.experimental import pallas as pl
from jax.experimental.pallas import tpu as pltpu
from jax.sharding import PartitionSpec as P

D = 4096
HEAD = 128
QLEAF = 16
QMID = 48
QROOT = 144


LOWEST = -1e30
EPSILON = 1e-05
ALIGN = 16
BLOCK = 512
VMEM_BYTES = 50 << 20
SMALL_BYTES = 24 << 20


def cost(flops, moved, exps):
    return pl.CostEstimate(flops=flops, bytes_accessed=moved, transcendentals=exps)


def streamed(pairs, sems):
    copies = [
        pltpu.make_async_copy(source, target, sems.at[k]) for k, (source, target) in enumerate(pairs)
    ]
    for copy in copies:
        copy.start()
    return copies


def own_nodes(owner, local_counts, tree, lengths, slots):
    token_leaf, leaf_parent, mid_parent = tree
    node_total = sum(local_counts)

    def kernel(owner_ref, token_ref, leaf_up, mid_up, *refs):
        len_refs, slot_refs, out_ref = refs[:3], refs[3:6], refs[6]

        def find(slot_ref, len_ref, local):
            base = owner_ref[0] * local

            def step(j, found):
                at, size = slot_ref[j] - base, len_ref[j]
                return tuple(
                    (jnp.where(at == k, j, node), jnp.where(at == k, size, length))
                    for k, (node, length) in enumerate(found)
                )

            zero = jnp.int32(0)
            return lax.fori_loop(0, slot_ref.shape[0], step, ((zero, zero),) * local)

        def below(parent_ref, edges):
            def step(j, counted):
                parent = parent_ref[j]
                return tuple(
                    c + jnp.where(parent < edge, 1, 0) for c, edge in zip(counted, edges)
                )

            return lax.fori_loop(0, parent_ref.shape[0], step, (jnp.int32(0),) * len(edges))

        picked = [find(*level) for level in zip(slot_refs, len_refs, local_counts)]
        edges = ()
        for level, parent_ref in enumerate((mid_up, leaf_up, None)):
            for node, _ in picked[level]:
                edges += (node, node + 1)
            if parent_ref is not None:
                edges = below(parent_ref, edges)
        tokens = token_ref[...]
        sizes = [length for level in picked for _, length in level]
        for k in range(node_total):
            for side in range(2):
                under = jnp.where(tokens < edges[2 * k + side], 1.0, 0.0)
                out_ref[side, k] = jnp.sum(under).astype(jnp.int32)
            out_ref[2, k] = sizes[k]

    smem = pl.BlockSpec(memory_space=pltpu.SMEM)
    vmem = pl.BlockSpec(memory_space=pltpu.VMEM)
    return pl.pallas_call(
        kernel,
        out_shape=jax.ShapeDtypeStruct((3, node_total), jnp.int32),
        in_specs=[smem, vmem] + [smem] * 8,
        out_specs=smem,
        name="own_nodes",
    )(owner[None], token_leaf.reshape(-1, HEAD), leaf_parent, mid_parent, *lengths, *slots)


def tree_attention(query_parts, caches, nodes, owner, kv_head):
    part_total = len(query_parts)
    own_rows = query_parts[0].shape[0]
    total_rows = part_total * own_rows
    width = query_parts[0].shape[1] // (caches[0].shape[2] // (2 * HEAD))
    group_size = width // HEAD
    score_scale = 1.0 / math.sqrt(HEAD)
    levels = []
    for cache, capacity in zip(caches, (QROOT, QMID, QLEAF)):
        levels.append((cache.shape[0], cache.shape[1], min(capacity + ALIGN, total_rows)))

    def kernel(nodes_ref, owner_ref, *refs):
        query_refs = refs[:part_total]
        cache_refs = refs[part_total : part_total + 3]
        near_ref, far_ref, all_rows, run_out, run_lse, acc, peak, total, *rest = refs[
            part_total + 3 :
        ]
        kept_refs, sems = rest[:3], rest[3]
        columns = pl.ds(kv_head * 2 * HEAD, 2 * HEAD)
        starts = [0, levels[0][0], levels[0][0] + levels[1][0]]
        lengths, flag_starts, flag = [], [], 0
        for start, (slot_total, span, _) in zip(starts, levels):
            lengths.append([nodes_ref[2, start + member] for member in range(slot_total)])
            flag_starts.append(flag)
            flag += slot_total * (span // min(BLOCK, span))

        def block_copy(level, member, index):
            span = levels[level][1]
            block = min(BLOCK, span)
            at = index * block
            here = pl.ds(at if isinstance(at, int) else pl.multiple_of(at, block), block)
            return pltpu.make_async_copy(
                cache_refs[level].at[member, here, columns],
                kept_refs[level].at[member, here, :],
                sems.at[flag_starts[level] + member * (span // block) + index],
            )

        steps = []
        for level, (slot_total, span, _) in enumerate(levels):
            block = min(BLOCK, span)
            pair = min(2 * block, span)
            longest = lengths[level][0]
            shortest = lengths[level][0]
            for length in lengths[level][1:]:
                longest, shortest = jnp.maximum(longest, length), jnp.minimum(shortest, length)
            whole, most = lax.div(shortest, pair), lax.div(longest + pair - 1, pair)
            steps.append((block, pair, whole, most))
            for index in range(span // pair):

                @pl.when(index < most)
                def _(level=level, index=index, ratio=pair // block, slot_total=slot_total):
                    for piece in range(ratio):
                        for member in range(slot_total):
                            block_copy(level, member, index * ratio + piece).start()

        me = owner_ref[0]
        for part in range(part_total):
            row = pl.multiple_of((me ^ part) * own_rows, ALIGN)
            all_rows[pl.ds(row, own_rows), :] = query_refs[part][
                :, kv_head * width : (kv_head + 1) * width
            ]
        run_out[...] = jnp.zeros_like(run_out)
        run_lse[...] = jnp.full_like(run_lse, LOWEST)
        offsets = [h * HEAD for h in range(group_size)]
        for level, (slot_total, span, rows) in enumerate(levels):
            block, pair, whole, most = steps[level]
            lanes = rows * group_size
            every = lanes * slot_total
            windows, grouped = [], []
            for member in range(slot_total):
                low = nodes_ref[0, starts[level] + member]
                window = jnp.minimum(low - lax.rem(low, ALIGN), total_rows - rows)
                window = pl.multiple_of(window, ALIGN)
                windows.append(window)
                grouped.append(
                    jnp.concatenate(
                        [all_rows[pl.ds(window, rows), c : c + HEAD] for c in offsets], axis=0
                    )
                )
            lane_of = lax.broadcasted_iota(jnp.int32, (1, every), 1)
            limits = jnp.full((1, every), lengths[level][0], jnp.int32)
            for member in range(1, slot_total):
                limits = jnp.where(lane_of >= member * lanes, lengths[level][member], limits)
            acc[:, :every] = jnp.zeros((HEAD, every), jnp.float32)
            peak[:, :every] = jnp.full((1, every), LOWEST, jnp.float32)
            total[:, :every] = jnp.zeros((1, every), jnp.float32)

            def visit(index, carry, masked):
                ratio = pair // block
                for piece in range(ratio):
                    for member in range(slot_total):
                        block_copy(level, member, index * ratio + piece).wait()
                scores = []
                for piece in range(ratio):
                    at = pl.multiple_of((index * ratio + piece) * block, block)
                    found = [
                        lax.dot_general(
                            kept_refs[level][member, pl.ds(at, block), :HEAD],
                            grouped[member],
                            (((1,), (1,)), ((), ())),
                            preferred_element_type=jnp.float32,
                        )
                        for member in range(slot_total)
                    ]
                    found = found[0] if slot_total == 1 else jnp.concatenate(found, axis=1)
                    if masked:
                        position = lax.broadcasted_iota(jnp.int32, (block, every), 0)
                        found = jnp.where(position < limits - at, found, LOWEST)
                    scores.append((at, found))
                for at, found in scores:
                    old_peak = peak[:, :every]
                    new_peak = jnp.maximum(old_peak, jnp.max(found, axis=0, keepdims=True))
                    weights = jnp.exp((found - new_peak) * score_scale)
                    fade = jnp.exp((old_peak - new_peak) * score_scale)
                    peak[:, :every] = new_peak
                    total[:, :every] = total[:, :every] * fade + jnp.sum(
                        weights, axis=0, keepdims=True
                    )
                    rounded = weights.astype(jnp.bfloat16)
                    for member in range(slot_total):
                        here = slice(member * lanes, (member + 1) * lanes)
                        acc[:, here] = acc[:, here] * fade[:, here] + lax.dot_general(
                            kept_refs[level][member, pl.ds(at, block), HEAD:],
                            rounded[:, here],
                            (((0,), (0,)), ((), ())),
                            preferred_element_type=jnp.float32,
                        )
                return carry

            lax.fori_loop(0, whole, lambda i, c: visit(i, c, False), 0)
            lax.fori_loop(whole, most, lambda i, c: visit(i, c, True), 0)

            weight_sum = total[:, :every]
            part_out = (acc[:, :every] / weight_sum).T
            part_lse = jnp.broadcast_to(
                peak[:, :every] * score_scale + jnp.log(weight_sum), (HEAD, every)
            ).T
            for member, window in enumerate(windows):
                low = nodes_ref[0, starts[level] + member]
                high = nodes_ref[1, starts[level] + member]
                position = window + lax.broadcasted_iota(jnp.int32, (rows, HEAD), 0)
                live = (position >= low) & (position < high)
                for h, c in enumerate(offsets):
                    here = (pl.ds(window, rows), slice(c, c + HEAD))
                    old_lse, old_out = run_lse[here], run_out[here]
                    at = member * lanes + h * rows
                    add_lse = part_lse[at : at + rows]
                    add_out = part_out[at : at + rows]
                    if level == 0:
                        run_out[here] = jnp.where(live, add_out, old_out)
                        run_lse[here] = jnp.where(live, add_lse, old_lse)
                        continue
                    best = jnp.maximum(old_lse, add_lse)
                    old_share = jnp.exp(old_lse - best)
                    add_share = jnp.exp(add_lse - best)
                    share = old_share + add_share
                    run_out[here] = jnp.where(
                        live, (old_out * old_share + add_out * add_share) / share, old_out
                    )
                    run_lse[here] = jnp.where(live, best + jnp.log(share), old_lse)
        lane = lax.broadcasted_iota(jnp.int32, (own_rows, HEAD), 1)
        for part in range(part_total):
            out_ref = far_ref if part % 2 else near_ref
            here = pl.ds(pl.multiple_of((me ^ part) * own_rows, ALIGN), own_rows)
            out_ref[part // 2, :, :width] = run_out[here, :].astype(jnp.bfloat16)
            lse = jnp.zeros((own_rows, HEAD), jnp.float32)
            for h in range(group_size):
                piece = run_lse[here, h * HEAD : (h + 1) * HEAD]
                lse = jnp.where(lax.rem(lane, group_size) == h, piece, lse)
            out_ref[part // 2, :, width:] = lse_terms(lse, lane, group_size)

    block_total = sum(count * (span // min(BLOCK, span)) for count, span, _ in levels)
    most = max(count * rows for count, _, rows in levels) * group_size
    vmem = pl.BlockSpec(memory_space=pltpu.VMEM)
    smem = pl.BlockSpec(memory_space=pltpu.SMEM)
    return pl.pallas_call(
        kernel,
        out_shape=[
            jax.ShapeDtypeStruct((part_total // 2, own_rows, width + HEAD), jnp.bfloat16)
        ]
        * 2,
        in_specs=[smem, smem]
        + [vmem] * part_total
        + [pl.BlockSpec(memory_space=pltpu.HBM)] * 3,
        out_specs=[vmem, vmem],
        scratch_shapes=[
            pltpu.VMEM((total_rows, width), jnp.bfloat16),
            pltpu.VMEM((total_rows, width), jnp.float32),
            pltpu.VMEM((total_rows, width), jnp.float32),
            pltpu.VMEM((HEAD, most), jnp.float32),
            pltpu.VMEM((1, most), jnp.float32),
            pltpu.VMEM((1, most), jnp.float32),
        ]
        + [pltpu.VMEM((count, span, 2 * HEAD), jnp.bfloat16) for count, span, _ in levels]
        + [pltpu.SemaphoreType.DMA((block_total,))],
        compiler_params=pltpu.CompilerParams(vmem_limit_bytes=VMEM_BYTES),
        cost_estimate=cost(
            4 * HEAD * group_size * sum(c * span * rows for c, span, rows in levels),
            2 * 2 * HEAD * sum(count * span for count, span, _ in levels),
            group_size * sum(c * span * rows for c, span, rows in levels),
        ),
        name="tree_attention",
    )(nodes, owner[None], *query_parts, *caches)


def lse_of(packed, group_size):
    terms = packed.astype(jnp.float32)
    return (
        terms
        + pltpu.roll(terms, HEAD - group_size, 1)
        + pltpu.roll(terms, HEAD - 2 * group_size, 1)
    )


def lse_terms(lse, lane, group_size):
    first = lse.astype(jnp.bfloat16).astype(jnp.float32)
    second = (lse - first).astype(jnp.bfloat16).astype(jnp.float32)
    third = lse - first - second
    field = lax.div(lane, group_size)
    packed = jnp.where(field == 2, third, 0.0)
    packed = jnp.where(field == 1, second, packed)
    return jnp.where(field == 0, first, packed).astype(jnp.bfloat16)


def merge_pairs(near, got):
    pair_total, own_rows, wide = near.shape
    width = wide - HEAD
    group_size = width // HEAD

    def kernel(near_ref, got_ref, *out_refs):
        lane = lax.broadcasted_iota(jnp.int32, (own_rows, HEAD), 1)
        for k, out_ref in enumerate(out_refs):
            left = lse_of(near_ref[k, :, width:], group_size)
            right = lse_of(got_ref[k, :, width:], group_size)
            best = jnp.maximum(left, right)
            left, right = jnp.exp(left - best), jnp.exp(right - best)
            whole = left + right
            left, right = left / whole, right / whole
            for h in range(group_size):
                here = slice(h * HEAD, (h + 1) * HEAD)
                out_ref[:, here] = (
                    near_ref[k, :, here].astype(jnp.float32) * left[:, h : h + 1]
                    + got_ref[k, :, here].astype(jnp.float32) * right[:, h : h + 1]
                ).astype(jnp.bfloat16)
            lse = jnp.where(lane < group_size, best + jnp.log(whole), 0.0)
            lse = lse + pltpu.roll(lse, group_size, 1) + pltpu.roll(lse, 2 * group_size, 1)
            out_ref[:, width:] = lse_terms(lse, lane, group_size)

    vmem = pl.BlockSpec(memory_space=pltpu.VMEM)
    return pl.pallas_call(
        kernel,
        out_shape=[jax.ShapeDtypeStruct((own_rows, wide), jnp.bfloat16)] * pair_total,
        in_specs=[vmem, vmem],
        out_specs=[vmem] * pair_total,
        compiler_params=pltpu.CompilerParams(vmem_limit_bytes=SMALL_BYTES),
        cost_estimate=cost(4 * near.size, 6 * near.size, pair_total * own_rows * 2 * HEAD),
        name="merge_pairs",
    )(near, got)


def combine_project(every, weight, row_start, added, place, own_width):
    part_total = len(every)
    own_rows, wide = every[0].shape
    width = wide - HEAD
    group_size = width // HEAD
    block_total = weight.shape[1] // own_width
    last = added is not None or width == weight.shape[0]
    kind = jnp.bfloat16 if last else jnp.float32

    def kernel(place_ref, weight_ref, *refs):
        every_refs, refs = refs[:part_total], refs[part_total:]
        added_refs = refs[:block_total] if added is not None else (None,) * block_total
        attended_ref, *block_refs = refs[len(refs) - 3 - block_total : -2]
        kept, sems = refs[-2:]
        columns = [
            pl.ds(pl.multiple_of((place_ref[0] ^ block) * own_width, HEAD), own_width)
            for block in range(block_total)
        ]
        copies = streamed(
            [
                (weight_ref.at[pl.ds(row_start, width), column], kept.at[block])
                for block, column in enumerate(columns)
            ],
            sems,
        )
        lse = [lse_of(ref[:, width:], group_size) for ref in every_refs]
        best = lse[0]
        for one in lse[1:]:
            best = jnp.maximum(best, one)
        share = [jnp.exp(one - best) for one in lse]
        whole = share[0]
        for one in share[1:]:
            whole = whole + one
        for h in range(group_size):
            summed = jnp.zeros((own_rows, HEAD), jnp.float32)
            for part in range(part_total):
                summed = summed + (
                    every_refs[part][:, h * HEAD : (h + 1) * HEAD].astype(jnp.float32)
                    * share[part][:, h : h + 1]
                )
            attended_ref[:, h * HEAD : (h + 1) * HEAD] = (summed / whole[:, h : h + 1]).astype(
                jnp.bfloat16
            )
        for block in range(block_total):
            copies[block].wait()
            product = jnp.dot(
                attended_ref[...], kept[block], preferred_element_type=jnp.float32
            )
            if added is not None:
                product = product + added_refs[block][...]
            block_refs[block][...] = product.astype(kind)

    vmem = pl.BlockSpec(memory_space=pltpu.VMEM)
    outs = pl.pallas_call(
        kernel,
        out_shape=[jax.ShapeDtypeStruct((own_rows, width), jnp.bfloat16)]
        + [jax.ShapeDtypeStruct((own_rows, own_width), kind)] * block_total,
        in_specs=[pl.BlockSpec(memory_space=pltpu.SMEM), pl.BlockSpec(memory_space=pltpu.HBM)]
        + [vmem] * (part_total + (block_total if added is not None else 0)),
        out_specs=[vmem] * (1 + block_total),
        scratch_shapes=[
            pltpu.VMEM((block_total, width, own_width), jnp.bfloat16),
            pltpu.SemaphoreType.DMA((block_total,)),
        ],
        compiler_params=pltpu.CompilerParams(vmem_limit_bytes=VMEM_BYTES),
        cost_estimate=cost(
            2 * own_rows * width * weight.shape[1],
            2 * width * weight.shape[1],
            part_total * own_rows * HEAD,
        ),
        name="combine_project",
    )(place[None], weight, *every, *(added or ()))
    return outs[0], outs[1:]


def split_terms(value):
    first = value.astype(jnp.bfloat16).astype(jnp.float32)
    second = (value - first).astype(jnp.bfloat16).astype(jnp.float32)
    lane = lax.broadcasted_iota(jnp.int32, value.shape, 1)
    third = jnp.where(lane == 2, value - first - second, 0.0)
    return jnp.where(lane == 0, first, jnp.where(lane == 1, second, third)).astype(jnp.bfloat16)


def gate_up_rows(parts, norm_gain, gate_weight, up_weight, spot, group_total):
    own_rows, features = parts[0].shape
    rows = own_rows * len(parts)
    half = rows // 2
    piece = half // 2
    each = len(parts) // group_total
    units = gate_weight.shape[1]
    tile = units // 2 if (units // 2) % HEAD == 0 else units

    def kernel(spot_ref, gain_ref, gate_ref, up_ref, *refs):
        part_refs = refs[: len(parts)]
        keep_ref, *send_refs, scaled, squares, kept_gate, kept_up, sems = refs[len(parts) :]
        tiles = [
            (ref, kept, base, at)
            for ref, kept, base in ((gate_ref, kept_gate, 0), (up_ref, kept_up, units))
            for at in range(0, units, tile)
        ]
        copies = streamed(
            [
                (ref, kept)
                if tile == units
                else (ref.at[:, pl.ds(at, tile)], kept.at[:, pl.ds(at, tile)])
                for ref, kept, _, at in tiles
            ],
            sems,
        )
        for index, part_ref in enumerate(part_refs):
            at = ((index // each) ^ spot_ref[0]) * each + index % each
            here = pl.ds(pl.multiple_of(at * own_rows, ALIGN), own_rows)
            wide = part_ref[...].astype(jnp.float32)
            scaled[here, :] = (wide * gain_ref[...]).astype(jnp.bfloat16)
            squares[here, :] = jnp.broadcast_to(
                jnp.sum(wide * wide, axis=1, keepdims=True), (own_rows, HEAD)
            )
        for copy, (_, kept, base, at) in zip(copies, tiles):
            copy.wait()
            here = slice(base + at, base + at + tile)
            product = jnp.dot(
                scaled[...], kept[:, at : at + tile], preferred_element_type=jnp.float32
            ).astype(jnp.bfloat16)
            keep_ref[:, here] = product[:half]
            for k, send_ref in enumerate(send_refs):
                send_ref[:, here] = product[half + k * piece : half + (k + 1) * piece]
        terms = split_terms(squares[...])
        keep_ref[:, 2 * units :] = terms[:half]
        for k, send_ref in enumerate(send_refs):
            send_ref[:, 2 * units :] = terms[half + k * piece : half + (k + 1) * piece]

    vmem = pl.BlockSpec(memory_space=pltpu.VMEM)
    keep, *send = pl.pallas_call(
        kernel,
        out_shape=[jax.ShapeDtypeStruct((half, 2 * units + HEAD), jnp.bfloat16)]
        + [jax.ShapeDtypeStruct((piece, 2 * units + HEAD), jnp.bfloat16)] * 2,
        in_specs=[pl.BlockSpec(memory_space=pltpu.SMEM), vmem]
        + [pl.BlockSpec(memory_space=pltpu.HBM)] * 2
        + [vmem] * len(parts),
        out_specs=[vmem] * 3,
        scratch_shapes=[
            pltpu.VMEM((rows, features), jnp.bfloat16),
            pltpu.VMEM((rows, HEAD), jnp.float32),
            pltpu.VMEM((features, units), jnp.bfloat16),
            pltpu.VMEM((features, units), jnp.bfloat16),
            pltpu.SemaphoreType.DMA((2 * units // tile,)),
        ],
        compiler_params=pltpu.CompilerParams(vmem_limit_bytes=VMEM_BYTES),
        cost_estimate=cost(4 * rows * features * units, 4 * features * units, 0),
        name="gate_up",
    )(spot[None], norm_gain[None, :], gate_weight, up_weight, *parts)
    return keep, send


def add_halves(keep, got, units):
    half = keep.shape[0] // 2

    def kernel(keep_ref, low_ref, high_ref, next_ref, send_ref):
        for ref, got_ref, at in ((next_ref, low_ref, 0), (send_ref, high_ref, half)):
            here = pl.ds(at, half)
            ref[:, : 2 * units] = (
                keep_ref[here, : 2 * units].astype(jnp.float32)
                + got_ref[:, : 2 * units].astype(jnp.float32)
            ).astype(jnp.bfloat16)
            terms = keep_ref[here, 2 * units :].astype(jnp.float32)
            terms = terms + got_ref[:, 2 * units :].astype(jnp.float32)
            total = jnp.sum(terms, axis=1, keepdims=True)
            ref[:, 2 * units :] = split_terms(jnp.broadcast_to(total, (half, HEAD)))

    vmem = pl.BlockSpec(memory_space=pltpu.VMEM)
    return pl.pallas_call(
        kernel,
        out_shape=[jax.ShapeDtypeStruct((half, keep.shape[1]), jnp.bfloat16)] * 2,
        in_specs=[vmem] * 3,
        out_specs=[vmem, vmem],
        compiler_params=pltpu.CompilerParams(vmem_limit_bytes=SMALL_BYTES),
        cost_estimate=cost(2 * keep.size, 6 * keep.size, 0),
        name="add_halves",
    )(keep, *got)


def gated(keep, got, units):
    def kernel(keep_ref, got_ref, out_ref):
        summed = keep_ref[...].astype(jnp.float32) + got_ref[...].astype(jnp.float32)
        square = jnp.sum(summed[:, 2 * units :], axis=1, keepdims=True)
        scale = lax.rsqrt(square / D + EPSILON)
        gate = summed[:, :units] * scale
        up = summed[:, units : 2 * units] * scale
        out_ref[...] = (gate / (1.0 + jnp.exp(-gate)) * up).astype(jnp.bfloat16)

    vmem = pl.BlockSpec(memory_space=pltpu.VMEM)
    return pl.pallas_call(
        kernel,
        out_shape=jax.ShapeDtypeStruct((keep.shape[0], units), jnp.bfloat16),
        in_specs=[vmem, vmem],
        out_specs=vmem,
        compiler_params=pltpu.CompilerParams(vmem_limit_bytes=SMALL_BYTES),
        cost_estimate=cost(4 * keep.size, 5 * keep.size, keep.size // 2),
        name="gated",
    )(keep, got)


def down_rows(pieces, down_weight, spot, part_count, own_rows, group_total):
    rows = part_count * own_rows
    each = part_count // group_total
    units, features = down_weight.shape

    def kernel(spot_ref, weight_ref, *refs):
        piece_refs = refs[: len(pieces)]
        out_refs = refs[len(pieces) : len(pieces) + part_count]
        hidden, product = refs[len(pieces) + part_count :]
        at = 0
        for piece_ref in piece_refs:
            hidden[at : at + piece_ref.shape[0], :] = piece_ref[...]
            at += piece_ref.shape[0]
        product[...] = jnp.dot(
            hidden[...], weight_ref[...], preferred_element_type=jnp.float32
        )
        for index, out_ref in enumerate(out_refs):
            at = ((index // each) ^ spot_ref[0]) * each + index % each
            here = pl.ds(pl.multiple_of(at * own_rows, ALIGN), own_rows)
            out_ref[...] = product[here, :].astype(jnp.bfloat16)

    vmem = pl.BlockSpec(memory_space=pltpu.VMEM)
    return pl.pallas_call(
        kernel,
        out_shape=[jax.ShapeDtypeStruct((own_rows, features), jnp.bfloat16)] * part_count,
        in_specs=[pl.BlockSpec(memory_space=pltpu.SMEM)] + [vmem] * (1 + len(pieces)),
        out_specs=[vmem] * part_count,
        scratch_shapes=[
            pltpu.VMEM((rows, units), jnp.bfloat16),
            pltpu.VMEM((rows, features), jnp.float32),
        ],
        compiler_params=pltpu.CompilerParams(vmem_limit_bytes=SMALL_BYTES),
        cost_estimate=cost(2 * rows * features * units, 2 * features * units, 0),
        name="down",
    )(spot[None], down_weight, *pieces)


def swap(value, axis_name, mask):
    axis_total = lax.axis_size(axis_name)
    return lax.ppermute(value, axis_name, [(j, j ^ mask) for j in range(axis_total)])


def after(value, token):
    return lax.optimization_barrier((value, token))[0]


def gather_parts(value, axis_name, token=None):
    parts = [value] * lax.axis_size(axis_name)
    for mask in range(len(parts) - 2, 0, -2):
        parts[mask] = swap(value, axis_name, mask)
    for mask in [0] + list(range(len(parts) - 2, 0, -2)):
        held = parts[mask] if token is None or mask == 0 else after(parts[mask], token)
        parts[mask + 1] = swap(held, axis_name, 1)
    return parts


def shards(
    queries,
    root_cache,
    mid_cache,
    leaf_cache,
    token_leaf,
    leaf_parent,
    mid_parent,
    root_len,
    mid_len,
    leaf_len,
    root_slot,
    mid_slot,
    leaf_slot,
    stream,
    out_weight,
    norm_gain,
    gate_weight,
    up_weight,
    down_weight,
):
    own_rows, width = queries.shape
    owner = lax.axis_index("kv").astype(jnp.int32)
    caches = (root_cache, mid_cache, leaf_cache)
    nodes = own_nodes(
        owner,
        [cache.shape[0] for cache in caches],
        (token_leaf, leaf_parent, mid_parent),
        (root_len, mid_len, leaf_len),
        (root_slot, mid_slot, leaf_slot),
    )
    kv_count = root_cache.shape[2] // (2 * HEAD)
    group_width = width // kv_count
    mlp_total = lax.axis_size("mlp")
    mlp_place = lax.axis_index("mlp").astype(jnp.int32)
    own_width = stream.shape[1]
    query_parts = gather_parts(queries, "kv")
    attended, blocks = [], None
    for k in range(kv_count):
        near, far = tree_attention(query_parts, caches, nodes, owner, k)
        merged = merge_pairs(near, swap(far, "kv", 1))
        every = [swap(one, "kv", 2 * pair) if pair else one for pair, one in enumerate(merged)]
        one, blocks = combine_project(
            every, out_weight, k * group_width, blocks, mlp_place, own_width
        )
        attended.append(one)
    projected = blocks[0].astype(jnp.float32)
    for mask in range(mlp_total - 1, 0, -1):
        projected = projected + swap(blocks[mask], "mlp", mask).astype(jnp.float32)
    residual = (stream.astype(jnp.float32) + projected).astype(jnp.bfloat16)
    steps = [1 << bit for bit in range(mlp_total.bit_length() - 1)]
    spot = jnp.int32(0)
    for step in steps:
        spot = 2 * spot + (mlp_place // step) % 2
    units = gate_weight.shape[1]
    row_parts = gather_parts(residual, "kv")
    first, second = (
        [mask for mask in range(len(row_parts)) if (mask // 2) % 2 == side] for side in range(2)
    )
    row_parts[0] = after(row_parts[0], [row_parts[mask] for mask in second if mask % 2 == 0])

    def multiply(masks):
        parts = [row_parts[mask] for mask in masks]
        return gate_up_rows(parts, norm_gain, gate_weight, up_weight, spot, mlp_total)

    def reduce_once(keep, send, token=None):
        for step in steps[:-1]:
            if step > 1:
                send = jnp.split(send, 2, axis=0)
            got = [swap(piece, "mlp", step) for piece in send]
            if token is not None and step == 1:
                keep = after(keep, token)
            keep, send = add_halves(keep, got, units)
        return keep, send

    def regather(hidden, token):
        pieces = [hidden]
        for step in reversed(steps):
            pieces += [
                swap(piece if k == 0 or step == steps[-1] else after(piece, token), "mlp", step)
                for k, piece in enumerate(pieces)
            ]
        return pieces

    def finish(pieces, masks):
        outs = down_rows(pieces, down_weight, spot, len(masks), own_rows, mlp_total)
        return dict(zip(masks, outs))

    keep, send = reduce_once(*multiply(first))
    row_parts[second[0]] = after(row_parts[second[0]], send)
    later = multiply(second)
    hidden = gated(after(keep, later[0]), swap(send, "mlp", steps[-1]), units)
    keep, send = reduce_once(*later, hidden)
    early = finish(regather(hidden, send), first)
    hidden = gated(keep, swap(send, "mlp", steps[-1]), units)
    mixed = early[0].astype(jnp.float32)
    for mask in first[:0:-1]:
        mixed = mixed + swap(early[mask], "kv", mask).astype(jnp.float32)
    late = finish(regather(hidden, mixed), second)
    for mask in sorted(late, reverse=True):
        mixed = mixed + swap(late[mask], "kv", mask).astype(jnp.float32)
    return (jnp.concatenate(attended, axis=1), mixed.astype(jnp.bfloat16))


def solution(mesh):
    in_specs = (
        P("kv", "mlp"),
        P("kv", None, "mlp"),
        P("kv", None, "mlp"),
        P("kv", None, "mlp"),
        P(),
        P(),
        P(),
        P(),
        P(),
        P(),
        P(),
        P(),
        P(),
        P("kv", "mlp"),
        P("mlp", None),
        P("mlp"),
        P("mlp", "kv"),
        P("mlp", "kv"),
        P("kv", "mlp"),
    )
    out_specs = (P("kv", "mlp"), P("kv", "mlp"))
    return jax.shard_map(shards, mesh=mesh, in_specs=in_specs, out_specs=out_specs, check_vma=False)
```
